32 devices in a mesh: dp: 16 (over z, y, x), tensor: 2 (over core).
Axes of the slice: x: 2, y: 2, z: 4, core: 2. Of those that a mesh axis runs over, the one named last changes fastest.
Arguments:
- tokens: bfloat16 [16384, 768], P(('dp', 'tensor')), may hold values from -6 to 6
- cotangent: bfloat16 [16384, 768], P(('dp', 'tensor')), may hold values from -6 to 6
- prefix: int32 [16], P('dp'), may hold values from 102 to 512, as said below
- routes: int32 [16384, 1], P('dp'), may hold values from 0 to 1; in each aligned block of 1024 rows (0 to 1023, 1024 to 2047, ...) at most 640 rows name the same one
- norm1_gain: float32 [768], P(('dp', 'tensor')), may hold values from 0.5 to 1.5
- norm1_bias: float32 [768], P(('dp', 'tensor')), may hold values from -0.625 to 0.625
- w_query: bfloat16 [768, 768], P('dp', 'tensor'), may hold values from -0.4375 to 0.4375
- w_key: bfloat16 [768, 768], P('dp', 'tensor'), may hold values from -0.21875 to 0.21875
- w_value: bfloat16 [768, 768], P('dp', 'tensor'), may hold values from -0.21875 to 0.21875
- w_out: bfloat16 [768, 768], P('tensor', 'dp'), may hold values from -1.75 to 1.75
- norm2_gain: float32 [768], P(('dp', 'tensor')), may hold values from 0.5 to 1.5
- norm2_bias: float32 [768], P(('dp', 'tensor')), may hold values from -0.625 to 0.625
- centroids: float32 [2, 768], P(None, ('dp', 'tensor')), may hold values from -0.1875 to 0.1875
- expert_in: bfloat16 [2, 768, 3072], P(None, 'dp', 'tensor'), may hold values from -0.21875 to 0.21875
- expert_out: bfloat16 [2, 3072, 768], P(None, 'tensor', 'dp'), may hold values from -0.4375 to 0.4375
Outputs:
- block_out: bfloat16 [16384, 768], P(('dp', 'tensor'))
- grad_tokens: bfloat16 [16384, 768], P(('dp', 'tensor'))
- grad_norm1_gain: float32 [768], P(('dp', 'tensor'))
- grad_norm1_bias: float32 [768], P(('dp', 'tensor'))
- grad_w_query: float32 [768, 768], P('dp', 'tensor')
- grad_w_key: float32 [768, 768], P('dp', 'tensor')
- grad_w_value: float32 [768, 768], P('dp', 'tensor')
- grad_w_out: float32 [768, 768], P('tensor', 'dp')
- grad_norm2_gain: float32 [768], P(('dp', 'tensor'))
- grad_norm2_bias: float32 [768], P(('dp', 'tensor'))
- grad_centroids: float32 [2, 768], P(None, ('dp', 'tensor'))
- grad_expert_in: float32 [2, 768, 3072], P(None, 'dp', 'tensor')
- grad_expert_out: float32 [2, 3072, 768], P(None, 'tensor', 'dp')
The draws below stay inside these ranges and needn't reach their ends.
Inputs may be any that keep to these rules, and one draw needn't show every extreme that they name: Each sequence's first prefix tokens see one another; some sequence's prefix is exactly half of 1024. `routes`: in each aligned block of 1024 rows (the tokens of one index of dp) no expert is named by more than 640 rows; some block names an expert exactly 640 times.
All inputs are finite; a program needn't handle non-finite values.
Results may differ from the reference program's by a relative error of at most 0.02.
Values may be sent and summed in bfloat16 or wider, within the bound.
A program may use at most 192 MiB of HBM per device.

```python
import math
import jax
import jax.numpy as jnp
import numpy as np
from jax import lax

D = 768
HEADS = 12
FF = 3072
EXPERTS = 2
LEN = 1024
ROWS = 1024
CAP = 640
SEQS = 16
TOKENS = 16384


def draw_prefix(key, part):
    first_key, second_key = jax.random.split(key)
    lengths = jax.random.randint(first_key, (SEQS,), LEN // 10, LEN // 2 + 1, dtype=jnp.int32)
    chosen = jax.random.randint(second_key, (), 0, SEQS, dtype=jnp.int32)
    return jnp.where(jnp.arange(SEQS, dtype=jnp.int32) == chosen, LEN // 2, lengths).astype(jnp.int32)


def spiked(values, own_key, source, target, parts, factor):
    def block_of(axis_at):
        return (jnp.arange(values.shape[axis_at]) // (values.shape[axis_at] // parts)).reshape((-1,) + (1,) * (values.ndim - 1 - axis_at))

    near = jax.random.permutation(own_key, parts)[block_of(target)]
    other_side = (block_of(target) + parts // 2) % parts
    return jnp.where((block_of(source) == near) | (block_of(source) == other_side), factor * values, values)


def level_of(key, shape, pieces, smallest, largest):
    level = 1.0
    for axis_at, blocks in pieces:
        steps = jax.random.uniform(jax.random.fold_in(jax.random.fold_in(key, 6), axis_at), (blocks,), jnp.float32, smallest / len(pieces), largest / len(pieces))
        level = level * jnp.repeat(jnp.exp(steps), shape[axis_at] // blocks).reshape((-1,) + (1,) * (len(shape) - 1 - axis_at))
    return level


def routed_block(stream_key, own, number, rows, amount, top, limit, lean):
    order = jax.random.permutation(stream_key, amount)
    packed, usual = load_shares(amount, rows * top, limit, lean, True), load_shares(amount, rows * top, limit, lean, False)
    places = jnp.arange(amount)

    def named(sizes, rotation):
        used = int((sizes > 0).sum())
        fixed = max(1, used // 4)
        passed = fixed + (places - fixed + rotation * (used - fixed)) % max(1, amount - fixed)
        return jnp.zeros((amount,), jnp.int32).at[order[jnp.where(places < fixed, places, passed)]].set(jnp.asarray(sizes, jnp.int32))

    sizes = jnp.where(number % 4 == 0, named(packed, number // 4), named(usual, number - number // 4 - 1))
    mixed = jax.random.permutation(jax.random.fold_in(own, 3), amount)
    source_of, sink = mixed[0:amount // 2 * 2:2], mixed[1:amount // 2 * 2:2]
    room = jnp.minimum(sizes[source_of] - 1, limit - sizes[sink]) // 2
    room = jnp.where((source_of == order[0]) | (sink == order[0]) | (sizes[sink] == 0), 0, jnp.maximum(room, 0))
    passed = jax.random.randint(jax.random.fold_in(own, 4), (amount // 2,), 0, 1 << 20) % (room + 1)
    sizes = sizes.at[source_of].add(-passed).at[sink].add(passed)
    members = jnp.searchsorted(jnp.cumsum(sizes), jnp.arange(rows * top), side="right").astype(jnp.int32)
    listing = members.reshape(top, rows).T
    listing = listing[jax.random.permutation(jax.random.fold_in(own, 1), rows)]
    rotation = jax.random.randint(jax.random.fold_in(own, 2), (rows, 1), 0, top)
    return jnp.take_along_axis(listing, (jnp.arange(top)[None, :] + rotation) % top, axis=1)


def load_shares(amount, total, limit, skew, full):
    portions = [(1 << 20) // math.isqrt(grade ** skew) + 1 for grade in range(1, amount + 1)]
    largest = limit if full else min(limit, max(-(-total // amount), total * portions[0] // sum(portions)))
    least = 1 if total - largest >= amount - 1 else 0
    given, spare = [largest] + [least] * (amount - 1), total - largest - least * (amount - 1)
    while spare > 0:
        movable = [i for i in range(1, amount) if given[i] < largest] or [i for i in range(1, amount) if given[i] < limit]
        pool, budget = sum([portions[i] for i in movable]), spare
        for i in movable:
            addition = min(limit - given[i], max(1, budget * portions[i] // pool), spare)
            given[i] = given[i] + addition
            spare = spare - addition
    return np.array(given)


def centred(own_key, shape, deviation, most, cuts=(), held_as=jnp.bfloat16):
    values = deviation * jax.random.normal(own_key, shape, jnp.float32)
    if cuts:
        values = values * level_of(own_key, shape, cuts, -0.22, 0.18)
    return jnp.clip(values, -most, most).astype(held_as)


def bell_draw_with(rng, shape, deviation, reach, pieces, heavy, kind=jnp.bfloat16):
    result = deviation * jax.random.normal(rng, shape, jnp.float32)
    if pieces:
        result = result * level_of(rng, shape, pieces, -0.22, 0.18)
    return jnp.clip(spiked(result, jax.random.fold_in(rng, 3), *heavy), -reach, reach).astype(kind)


def setup_inputs(seed: int = 0) -> dict:
    keys = jax.random.split(jax.random.key(seed), 16)
    tokens = bell_draw_with(keys[0], (TOKENS, D), 1.0, 6.0, ((0, 32),), (0, 1, 32, 2.75))
    cotangent = bell_draw_with(keys[1], (TOKENS, D), 1.0, 6.0, ((0, 32),), (0, 1, 32, 2.75))
    prefix = draw_prefix(jax.random.fold_in(keys[15], 71), 0)
    routes_keys = jax.random.split(jax.random.fold_in(keys[3], 1), TOKENS // ROWS)
    routes_turns = jax.random.permutation(jax.random.fold_in(keys[3], 3), TOKENS // ROWS)
    routes = jax.vmap(lambda own, number: routed_block(jax.random.fold_in(keys[3], 2), own, number, ROWS, EXPERTS, 1, CAP, 1))(routes_keys, routes_turns).reshape((TOKENS, 1))
    norm1_gain = jnp.clip(1.0 + 0.1 * jax.random.normal(keys[4], (D,), jnp.float32), 0.5, 1.5)
    norm1_bias = centred(keys[5], (D,), 0.1, 0.625, ((0, 32),), jnp.float32)
    w_query = centred(keys[6], (D, D), (D // 4) ** -0.5, 0.4375, ((0, 16), (1, 2)))
    w_key = centred(keys[7], (D, D), D ** -0.5, 0.21875, ((0, 16), (1, 2)))
    w_value = centred(keys[8], (D, D), D ** -0.5, 0.21875, ((0, 16), (1, 2)))
    w_out = centred(keys[9], (D, D), (D // 64) ** -0.5, 1.75, ((0, 2), (1, 16)))
    norm2_gain = jnp.clip(1.0 + 0.1 * jax.random.normal(keys[10], (D,), jnp.float32), 0.5, 1.5)
    norm2_bias = centred(keys[11], (D,), 0.1, 0.625, ((0, 32),), jnp.float32)
    centroids = centred(keys[12], (EXPERTS, D), (0.8 / D ** 0.5), 0.1875, ((1, 32),), jnp.float32)
    expert_in = centred(keys[13], (EXPERTS, D, FF), D ** -0.5, 0.21875, ((1, 16), (2, 2)))
    expert_out = centred(keys[14], (EXPERTS, FF, D), (FF // 16) ** -0.5, 0.4375, ((1, 2), (2, 16)))
    return dict(tokens=tokens, cotangent=cotangent, prefix=prefix, routes=routes, norm1_gain=norm1_gain, norm1_bias=norm1_bias, w_query=w_query, w_key=w_key, w_value=w_value, w_out=w_out, norm2_gain=norm2_gain, norm2_bias=norm2_bias, centroids=centroids, expert_in=expert_in, expert_out=expert_out)


EPS = 1e-05
HIGHEST = lax.Precision.HIGHEST
NEGATIVE = -1e+30

@jax.custom_vjp
def low(v):
    return lax.optimization_barrier(v.astype(jnp.bfloat16)).astype(jnp.float32)

@jax.custom_vjp
def low_back(v):
    return v

def low_keep(v):
    return (low(v), None)

def low_pass(kept, grad):
    return (grad,)

def back_keep(v):
    return (v, None)

def back_low(kept, grad):
    return (low(grad),)
low.defvjp(low_keep, low_pass)
low_back.defvjp(back_keep, back_low)

def norm_rows(features, norm_gain, norm_shift):
    average = lax.optimization_barrier(jnp.mean(features, axis=-1, keepdims=True))
    centered = features - average
    spread = lax.optimization_barrier(jnp.mean(centered * centered, axis=-1, keepdims=True))
    return centered * lax.rsqrt(spread + EPS) * norm_gain + norm_shift

def slot_table(route_rows, experts, capacity):
    row_count = route_rows.shape[0]
    ordering = jnp.argsort(route_rows, stable=True).astype(jnp.int32)
    labels = jnp.arange(experts, dtype=jnp.int32)
    counts = lax.optimization_barrier(jnp.sum((route_rows[:, None] == labels[None, :]).astype(jnp.int32), axis=0)).astype(jnp.int32)
    starts = (jnp.cumsum(counts) - counts).astype(jnp.int32)
    column = jnp.arange(capacity, dtype=jnp.int32)
    places = jnp.minimum(starts[:, None] + column[None, :], row_count - 1).astype(jnp.int32)
    return (ordering[places], column[None, :] < counts[:, None])

def group_forward(features, params, prefix_group, route_group):
    gain_one, bias_one, query_w, key_w, value_w, out_w, gain_two, bias_two, centre_table, in_w, back_w = params
    row_count = features.shape[0]
    seq_count = prefix_group.shape[0]
    length = row_count // seq_count
    head_dim = D // HEADS
    first_rows = low(norm_rows(features, gain_one, bias_one))
    queries = low(low_back(jnp.dot(first_rows, query_w, precision=HIGHEST))).reshape(seq_count, length, HEADS, head_dim)
    keys_all = low(low_back(jnp.dot(first_rows, key_w, precision=HIGHEST))).reshape(seq_count, length, HEADS, head_dim)
    values_all = low(low_back(jnp.dot(first_rows, value_w, precision=HIGHEST))).reshape(seq_count, length, HEADS, head_dim)
    scores = low_back(jnp.einsum('sqhd,skhd->shqk', queries, keys_all, precision=HIGHEST) * head_dim ** (-0.5))
    positions = jnp.arange(length, dtype=jnp.int32)
    allowed = (positions[None, None, :] <= positions[None, :, None]) | (positions[None, None, :] < prefix_group[:, None, None])
    scores = jnp.where(allowed[:, None], scores, NEGATIVE)
    top_score = lax.optimization_barrier(jnp.max(scores, axis=-1, keepdims=True))
    powered = jnp.exp(scores - top_score)
    totals = lax.optimization_barrier(jnp.sum(powered, axis=-1, keepdims=True))
    probabilities = low(powered / totals)
    attended = jnp.einsum('shqk,skhd->sqhd', probabilities, values_all, precision=HIGHEST).reshape(row_count, D)
    attended = low(low_back(attended))
    residual = features + low_back(jnp.dot(attended, out_w, precision=HIGHEST))
    second_rows = low(norm_rows(residual, gain_two, bias_two))
    gate_values = jax.nn.sigmoid(lax.optimization_barrier(jnp.sum(second_rows * centre_table[route_group], axis=-1)))
    slot_index, slot_valid = slot_table(route_group, EXPERTS, CAP)
    picked = second_rows[slot_index]
    up_value = low_back(jnp.einsum('ecd,edf->ecf', picked, in_w, precision=HIGHEST))
    activated = low(jax.nn.gelu(up_value))
    slot_out = jnp.where(slot_valid[:, :, None], jnp.einsum('ecf,efd->ecd', activated, back_w, precision=HIGHEST), 0.0)
    expert_rows = low_back(jnp.zeros_like(features).at[slot_index.reshape(-1)].add(slot_out.reshape(-1, D)))
    return residual + gate_values[:, None] * expert_rows

def reference(tokens, cotangent, prefix, routes, norm1_gain, norm1_bias, w_query, w_key, w_value, w_out, norm2_gain, norm2_bias, centroids, expert_in, expert_out):
    params = tuple((weight.astype(jnp.float32) for weight in (norm1_gain, norm1_bias, w_query, w_key, w_value, w_out, norm2_gain, norm2_bias, centroids, expert_in, expert_out)))
    groups = tokens.shape[0] // ROWS
    inputs = tokens.astype(jnp.float32).reshape(groups, ROWS, D)
    back_rows = cotangent.astype(jnp.float32).reshape(groups, ROWS, D)
    prefix_groups = prefix.reshape(groups, -1)
    route_groups = routes.reshape(groups, ROWS)
    grad_start = jax.tree.map(jnp.zeros_like, params)

    def group_step(grad_total, group_items):
        features, back_group, prefix_group, route_group = group_items

        def forward_of(rows_in, params_in):
            return group_forward(rows_in, params_in, prefix_group, route_group)
        block_out, pullback = jax.vjp(forward_of, features, params)
        back_in, back_params = pullback(back_group)
        return (jax.tree.map(jnp.add, grad_total, back_params), (block_out, back_in))
    grad_total, (outputs, back_inputs) = lax.scan(group_step, grad_start, (inputs, back_rows, prefix_groups, route_groups))
    return (outputs.reshape(-1, D).astype(jnp.bfloat16), back_inputs.reshape(-1, D).astype(jnp.bfloat16), grad_total[0], grad_total[1], grad_total[2], grad_total[3], grad_total[4], grad_total[5], grad_total[6], grad_total[7], grad_total[8], grad_total[9], grad_total[10])
```

```python
import jax
import jax.numpy as jnp
from jax import lax
from jax.sharding import PartitionSpec as P

D = 768
HEADS = 12
CAP = 640
EPS = 1e-05
NEGATIVE = -1e30
BF = jnp.bfloat16
F32 = jnp.float32


def factors_of(count):
    rest, sizes = count // 2, []
    while rest % 4 == 0:
        sizes.append(4)
        rest //= 4
    while rest % 2 == 0 and rest > 1:
        sizes.append(2)
        rest //= 2
    return sizes + ([2] if count > 1 else [])


class Ring:
    def __init__(self, count):
        self.count = count
        self.sizes = factors_of(count)
        self.strides = []
        stride = count
        for size in self.sizes:
            stride //= size
            self.strides.append(stride)
        self.square = len(self.sizes) >= 2 and self.sizes[-1] == 2 and self.sizes[-2] == 2

    def order(self, size):
        return [0, 1, 3, 2] if size == 4 else list(range(size))

    def shift(self, stage, step):
        size, stride = self.sizes[stage], self.strides[stage]
        order = self.order(size)
        pairs = []
        for source in range(self.count):
            digit = source // stride % size
            target = order[(order.index(digit) + step) % size]
            pairs.append((source, source + (target - digit) * stride))
        return pairs

    def move(self, value, stage, step):
        return lax.ppermute(value, "dp", self.shift(stage, step))

    def lead(self, block):
        for stage in range(len(self.sizes) - (2 if self.square else 0)):
            parts = [block] + [self.move(block, stage, s) for s in range(1, self.sizes[stage])]
            block = jnp.concatenate(parts, axis=0)
        return block

    def finish(self, block):
        if not self.square:
            return block
        y, x = len(self.sizes) - 2, len(self.sizes) - 1
        half = block.shape[0] // 2
        from_x, from_y = self.move(block, x, 1), self.move(block, y, 1)
        low, high = self.move(from_y[:half], x, 1), self.move(from_x[half:], y, 1)
        return jnp.concatenate([block, from_y, from_x, low, high], axis=0)

    def gather(self, block):
        return self.finish(self.lead(block))

    def scatter(self, total, kind):
        stages = len(self.sizes)
        if self.square:
            y, x = stages - 2, stages - 1
            quarter = total.shape[0] // 4
            half = quarter // 2
            own, to_y, to_x, far = (total[i * quarter : (i + 1) * quarter] for i in range(4))
            via_x = self.move(far[:half].astype(kind), x, 1)
            via_y = self.move(far[half:].astype(kind), y, 1)
            to_y = jnp.concatenate([to_y[:half].astype(F32) + via_x, to_y[half:].astype(F32)], axis=0)
            to_x = jnp.concatenate([to_x[:half].astype(F32), to_x[half:].astype(F32) + via_y], axis=0)
            from_x = self.move(to_x.astype(kind), x, 1)
            from_y = self.move(to_y.astype(kind), y, 1)
            total = own.astype(F32) + from_x.astype(F32) + from_y.astype(F32)
            stages -= 2
        for stage in reversed(range(stages)):
            size = self.sizes[stage]
            piece = total.shape[0] // size
            parts = [total[i * piece : (i + 1) * piece] for i in range(size)]
            total = parts[0].astype(F32)
            for step in range(1, size):
                total = total + self.move(parts[step].astype(kind), stage, size - step).astype(F32)
        return total

    def width_order(self, width):
        me = lax.axis_index("dp")
        rows = width // self.count
        column = jnp.arange(width, dtype=jnp.int32)
        inner, block = column % rows, column // rows
        found = jnp.zeros_like(column)
        for size, stride in zip(self.sizes, self.strides):
            step, block = block % size, block // size
            digit = me // stride % size
            if size == 4:
                place = jnp.bitwise_xor(digit, digit // 2)
                back = (place - step + size) % size
                source = jnp.bitwise_xor(back, back // 2)
            else:
                source = (digit - step + size) % size
            found = found + source * stride
        return found * rows + inner


def swap(value):
    return lax.ppermute(value, "tensor", [(0, 1), (1, 0)])


def after(value, earlier):
    return lax.optimization_barrier((value, earlier))[0]


def dot(a, b):
    return lax.dot_general(a, b, (((1,), (0,)), ((), ())), preferred_element_type=F32)


def dot_nt(a, b):
    return lax.dot_general(a, b, (((1,), (1,)), ((), ())), preferred_element_type=F32)


def dot_tn(a, b):
    return lax.dot_general(a, b, (((0,), (0,)), ((), ())), preferred_element_type=F32)


def norm_parts(features):
    average = jnp.mean(features, axis=-1, keepdims=True)
    centered = features - average
    spread = jnp.mean(centered * centered, axis=-1, keepdims=True)
    scale = lax.rsqrt(spread + EPS)
    return centered * scale, scale


def norm_back(grad, normed, scale, gain):
    h = grad * gain
    return scale * (
        h - jnp.mean(h, axis=-1, keepdims=True) - normed * jnp.mean(h * normed, axis=-1, keepdims=True)
    )


def allowed_mask(first_query, query_count, key_count, prefix_length):
    query_pos = first_query + jnp.arange(query_count, dtype=jnp.int32)
    key_pos = jnp.arange(key_count, dtype=jnp.int32)
    return (key_pos[None, :] <= query_pos[:, None]) | (key_pos[None, :] < prefix_length)


def block_scores(query_rows, seq_keys, allowed, score_scale):
    scores = (
        jnp.einsum("qhd,khd->hqk", query_rows, seq_keys, preferred_element_type=F32)
        * score_scale
    )
    return jnp.where(allowed[None], scores, NEGATIVE)


def attention_forward(queries, keys_all, values_all, prefix, heads_local, head_dim):
    score_scale = head_dim ** (-0.5)
    length = queries.shape[0]
    block_rows = length // 2
    outputs = []
    logsums = []
    for block_index in range(2):
        first_row = block_index * block_rows
        reach = first_row + block_rows
        seq_keys = keys_all[:reach].reshape(reach, heads_local, head_dim)
        seq_values = values_all[:reach].reshape(reach, heads_local, head_dim)
        query_rows = queries[first_row : first_row + block_rows].reshape(
            block_rows, heads_local, head_dim
        )
        allowed = allowed_mask(first_row, block_rows, reach, prefix[0])
        scores = block_scores(query_rows, seq_keys, allowed, score_scale)
        top_score = jnp.max(scores, axis=-1, keepdims=True)
        powered = jnp.exp(scores - top_score)
        totals = jnp.sum(powered, axis=-1, keepdims=True)
        probabilities = (powered / totals).astype(BF)
        attended = jnp.einsum(
            "hqk,khd->qhd", probabilities, seq_values, preferred_element_type=F32
        )
        outputs.append(attended.reshape(block_rows, heads_local * head_dim).astype(BF))
        logsums.append(top_score + jnp.log(totals))
    return (jnp.concatenate(outputs, axis=0), logsums)


def attention_backward(
    queries, keys_all, values_all, prefix, logsums, back_attended, heads_local, head_dim
):
    score_scale = head_dim ** (-0.5)
    length = queries.shape[0]
    block_rows = length // 2
    back_query_list = []
    back_keys = jnp.zeros((length, heads_local, head_dim), F32)
    back_values = jnp.zeros((length, heads_local, head_dim), F32)
    for block_index in range(2):
        first_row = block_index * block_rows
        reach = first_row + block_rows
        seq_keys = keys_all[:reach].reshape(reach, heads_local, head_dim)
        seq_values = values_all[:reach].reshape(reach, heads_local, head_dim)
        query_rows = queries[first_row:reach].reshape(block_rows, heads_local, head_dim)
        back_rows = back_attended[first_row:reach].reshape(block_rows, heads_local, head_dim)
        allowed = allowed_mask(first_row, block_rows, reach, prefix[0])
        scores = block_scores(query_rows, seq_keys, allowed, score_scale)
        probabilities = jnp.exp(scores - logsums[block_index])
        back_probs = jnp.einsum("qhd,khd->hqk", back_rows, seq_values, preferred_element_type=F32)
        row_dot = jnp.sum(probabilities * back_probs, axis=-1, keepdims=True)
        back_scores = (probabilities * (back_probs - row_dot)).astype(BF)
        back_query = (
            jnp.einsum("hqk,khd->qhd", back_scores, seq_keys, preferred_element_type=F32)
            * score_scale
        )
        back_key_part = (
            jnp.einsum("hqk,qhd->khd", back_scores, query_rows, preferred_element_type=F32)
            * score_scale
        )
        back_value_part = jnp.einsum(
            "hqk,qhd->khd", probabilities.astype(BF), back_rows, preferred_element_type=F32
        )
        back_keys = back_keys.at[:reach].add(back_key_part)
        back_values = back_values.at[:reach].add(back_value_part)
        back_query_list.append(back_query.reshape(block_rows, heads_local * head_dim))
    back_queries = jnp.concatenate(back_query_list, axis=0).astype(BF)
    flat = (length, heads_local * head_dim)
    return jnp.concatenate(
        [back_queries, back_keys.reshape(flat).astype(BF), back_values.reshape(flat).astype(BF)], axis=1
    )


def body(
    ring,
    tokens,
    cotangent,
    prefix,
    routes,
    norm1_gain,
    norm1_bias,
    w_query,
    w_key,
    w_value,
    w_out,
    norm2_gain,
    norm2_bias,
    centroids,
    expert_in,
    expert_out,
):
    side = lax.axis_index("tensor")
    own_rows, width = tokens.shape
    all_rows = 2 * own_rows
    head_dim = width // HEADS
    heads_local = w_query.shape[1] // head_dim
    part = w_query.shape[1]
    rows = w_query.shape[0]
    experts, _, hidden = expert_in.shape
    count = ring.count

    def both(own):
        other = swap(own)
        return jnp.where(
            side == 0, jnp.concatenate([own, other], 0), jnp.concatenate([other, own], 0)
        )

    vectors = jnp.concatenate(
        [
            norm1_gain[None],
            norm1_bias[None],
            norm2_gain[None],
            norm2_bias[None],
            centroids,
        ],
        axis=0,
    )
    small_count = vectors.shape[0]
    other_vectors = swap(vectors)
    vectors = jnp.where(
        side == 0,
        jnp.concatenate([vectors, other_vectors], 1),
        jnp.concatenate([other_vectors, vectors], 1),
    )
    table = ring.gather(vectors.reshape(1, small_count * rows))
    table = table.reshape(count, small_count, rows).transpose(1, 0, 2).reshape(small_count, width)
    gain_one, bias_one, gain_two, bias_two = (table[i : i + 1] for i in range(4))
    centres = table[4:]

    qkv_block = jnp.concatenate([w_query, w_key, w_value], axis=1)
    in_block = jnp.concatenate(
        [w_out.T, expert_in.transpose(1, 0, 2).reshape(rows, experts * hidden)], axis=1
    )
    out_block = expert_out.transpose(2, 0, 1).reshape(rows, experts * hidden)
    qkv_lead = ring.lead(qkv_block)
    qkv_w = ring.finish(qkv_lead)
    in_lead = ring.lead(after(in_block, qkv_lead))
    in_all = ring.finish(after(in_lead, qkv_w))
    out_lead = ring.lead(after(out_block, in_lead))
    back_w = ring.finish(after(out_lead, in_all))
    out_w, in_w = in_all[:, :part], in_all[:, part:]

    found = ring.width_order(width)
    to_order = (jnp.arange(width, dtype=jnp.int32)[:, None] == found[None, :]).astype(BF)
    tokens_all = dot(both(tokens), to_order)
    back_all = dot(both(cotangent), to_order)

    normed_one, scale_one = norm_parts(tokens_all)
    first_rows = (normed_one * gain_one + bias_one).astype(BF)
    qkv = dot(first_rows, qkv_w).astype(BF)
    queries, keys_all, values_all = qkv[:, :part], qkv[:, part : 2 * part], qkv[:, 2 * part :]
    attended, logsums = attention_forward(
        queries, keys_all, values_all, prefix, heads_local, head_dim
    )
    attn_terms = dot_nt(attended, out_w).astype(BF)
    residual = tokens_all + (attn_terms.astype(F32) + swap(attn_terms).astype(F32))
    normed_two, scale_two = norm_parts(residual)
    second_rows = (normed_two * gain_two + bias_two).astype(BF)
    second_wide = second_rows.astype(F32)

    is_last = routes == 1
    ones_before = jnp.tril(jnp.ones((all_rows, all_rows), BF))
    last_before = dot(ones_before, is_last.astype(BF)).astype(jnp.int32)
    position = jnp.arange(all_rows, dtype=jnp.int32)[:, None]
    first_count = all_rows - last_before[all_rows - 1, 0]
    place = jnp.where(is_last, first_count + last_before - 1, position - last_before)
    sort_to = (place == jnp.arange(all_rows, dtype=jnp.int32)[None, :]).astype(BF)
    tail = all_rows - CAP
    in_first = position < first_count

    centre_rows = jnp.where(is_last, centres[1:2], centres[0:1])
    gate = jax.nn.sigmoid(jnp.sum(second_wide * centre_rows, axis=-1, keepdims=True))
    back_branch = (gate * back_all).astype(BF)
    picked = dot_tn(sort_to, second_rows).astype(BF)
    back_slots = dot_tn(sort_to, back_branch).astype(BF)
    windows = (slice(0, CAP), slice(tail, all_rows))
    masks = (in_first[:CAP], ~in_first[tail:])
    slot_out, back_picked, grads_in, grads_out = [], [], [], []
    for e in range(2):
        columns = slice(e * hidden, (e + 1) * hidden)
        rows_in = picked[windows[e]]
        back_rows = jnp.where(masks[e], back_slots[windows[e]], jnp.zeros((), BF))
        up = dot(rows_in, in_w[:, columns])
        activated = jax.nn.gelu(up).astype(BF)
        slot_out.append(dot_nt(activated, back_w[:, columns]).astype(BF))
        grads_out.append(dot_tn(back_rows, activated).astype(BF))
        back_activated = dot(back_rows, back_w[:, columns])
        back_up = jax.vjp(jax.nn.gelu, up)[1](back_activated)[0].astype(BF)
        grads_in.append(dot_tn(rows_in, back_up).astype(BF))
        back_picked.append(dot_nt(back_up, in_w[:, columns]).astype(BF))

    def unsort(pieces):
        joined = jnp.concatenate(
            [
                pieces[0][:tail],
                jnp.where(in_first[tail:CAP], pieces[0][tail:], pieces[1][: CAP - tail]),
                pieces[1][CAP - tail :],
            ],
            axis=0,
        )
        return dot(sort_to, joined).astype(BF)

    row_terms = unsort(slot_out)
    expert_rows = row_terms.astype(F32) + swap(row_terms).astype(F32)
    block_all = (residual + gate * expert_rows).astype(BF)
    first_own = side * own_rows
    block_out = dot_nt(lax.dynamic_slice_in_dim(block_all, first_own, own_rows), to_order).astype(BF)
    back_score = jnp.sum(back_all * expert_rows, axis=-1, keepdims=True) * gate * (1.0 - gate)

    second_terms = unsort(back_picked)
    back_second = second_terms.astype(F32) + swap(second_terms).astype(F32) + back_score * centre_rows
    weighted = back_score * second_wide
    grad_centre = jnp.stack(
        [
            jnp.sum(jnp.where(is_last, 0.0, weighted), axis=0),
            jnp.sum(jnp.where(is_last, weighted, 0.0), axis=0),
        ]
    )
    grad_gain_two = jnp.sum(back_second * normed_two, axis=0)
    grad_bias_two = jnp.sum(back_second, axis=0)
    back_residual = back_all + norm_back(back_second, normed_two, scale_two, gain_two)
    back_out = back_residual.astype(BF)
    back_attended = dot(back_out, out_w).astype(BF)
    grad_out = dot_tn(back_out, attended).astype(BF)
    back_qkv = attention_backward(
        queries, keys_all, values_all, prefix, logsums, back_attended, heads_local, head_dim
    )
    grad_qkv = dot_tn(first_rows, back_qkv).astype(BF)
    first_terms = dot_nt(back_qkv, qkv_w).astype(BF)
    own_terms = lax.dynamic_slice_in_dim(first_terms, first_own, own_rows)
    other_terms = lax.dynamic_slice_in_dim(first_terms, own_rows - first_own, own_rows)
    back_first = own_terms.astype(F32) + swap(other_terms).astype(F32)

    def mine(value):
        return lax.dynamic_slice_in_dim(value, first_own, own_rows)

    normed_own = mine(normed_one)
    back_norm_one = norm_back(back_first, normed_own, mine(scale_one), gain_one)
    grad_tokens = dot_nt(
        (mine(back_residual) + back_norm_one).astype(BF), to_order
    ).astype(BF)
    one_part = jnp.stack([jnp.sum(back_first * normed_own, axis=0), jnp.sum(back_first, axis=0)])
    one_part = one_part + swap(one_part)
    small = jnp.concatenate(
        [one_part, grad_gain_two[None], grad_bias_two[None], grad_centre], axis=0
    )
    small = small.reshape(small_count, count, rows).transpose(1, 0, 2).reshape(count, small_count * rows)

    grads_out = ring.scatter(jnp.concatenate(grads_out, axis=1), BF)
    grads_in = ring.scatter(jnp.concatenate(grads_in, axis=1), BF)
    grad_out = ring.scatter(grad_out, BF)
    grad_qkv = ring.scatter(grad_qkv, BF)
    small = ring.scatter(small, F32).reshape(small_count, rows)
    small = lax.dynamic_slice_in_dim(small, side * (rows // 2), rows // 2, axis=1)
    return (
        block_out,
        grad_tokens,
        small[0],
        small[1],
        grad_qkv[:, :part],
        grad_qkv[:, part : 2 * part],
        grad_qkv[:, 2 * part :],
        grad_out.T,
        small[2],
        small[3],
        small[4:],
        grads_in.reshape(rows, experts, hidden).transpose(1, 0, 2),
        grads_out.reshape(rows, experts, hidden).transpose(1, 2, 0),
    )


def solution(mesh):
    ring = Ring(mesh.shape["dp"])
    both, rows = P(("dp", "tensor")), P(("dp", "tensor"), None)
    columns = P("dp", "tensor")

    def step(*arguments):
        return body(ring, *arguments)

    return jax.shard_map(
        step,
        mesh=mesh,
        in_specs=(
            rows,
            rows,
            P("dp"),
            P("dp", None),
            both,
            both,
            columns,
            columns,
            columns,
            P("tensor", "dp"),
            both,
            both,
            P(None, ("dp", "tensor")),
            P(None, "dp", "tensor"),
            P(None, "tensor", "dp"),
        ),
        out_specs=(
            rows,
            rows,
            both,
            both,
            columns,
            columns,
            columns,
            P("tensor", "dp"),
            both,
            both,
            P(None, ("dp", "tensor")),
            P(None, "dp", "tensor"),
            P(None, "tensor", "dp"),
        ),
        check_vma=False,
    )
```

```python
import jax
import jax.numpy as jnp
from jax import lax
from jax.experimental import pallas as pl
from jax.experimental.pallas import tpu as pltpu
from jax.sharding import PartitionSpec as P

D = 768
HEADS = 12
CAP = 640
EPS = 1e-05
NEGATIVE = -1e30
BF = jnp.bfloat16
F32 = jnp.float32
MESH = pl.DeviceIdType.MESH


def factors_of(count):
    rest, sizes = count // 2, []
    while rest % 4 == 0:
        sizes.append(4)
        rest //= 4
    while rest % 2 == 0 and rest > 1:
        sizes.append(2)
        rest //= 2
    return sizes + ([2] if count > 1 else [])


class Ring:
    def __init__(self, count):
        self.count = count
        self.sizes = factors_of(count)
        self.strides = []
        stride = count
        for size in self.sizes:
            stride //= size
            self.strides.append(stride)
        self.square = len(self.sizes) >= 2 and self.sizes[-1] == 2 and self.sizes[-2] == 2

    def order(self, size):
        return [0, 1, 3, 2] if size == 4 else list(range(size))

    def shift(self, stage, step):
        size, stride = self.sizes[stage], self.strides[stage]
        order = self.order(size)
        pairs = []
        for source in range(self.count):
            digit = source // stride % size
            target = order[(order.index(digit) + step) % size]
            pairs.append((source, source + (target - digit) * stride))
        return pairs

    def move(self, value, stage, step):
        return lax.ppermute(value, "dp", self.shift(stage, step))

    def lead(self, block):
        for stage in range(len(self.sizes) - (2 if self.square else 0)):
            parts = [block] + [self.move(block, stage, s) for s in range(1, self.sizes[stage])]
            block = jnp.concatenate(parts, axis=0)
        return block

    def cross(self, block):
        if not self.square:
            return ()
        y, x = len(self.sizes) - 2, len(self.sizes) - 1
        return self.move(block, x, 1), self.move(block, y, 1)

    def close(self, block, crossed):
        if not self.square:
            return block
        y, x = len(self.sizes) - 2, len(self.sizes) - 1
        half = block.shape[0] // 2
        from_x, from_y = crossed
        low, high = self.move(from_y[:half], x, 1), self.move(from_x[half:], y, 1)
        return jnp.concatenate([block, from_y, from_x, low, high], axis=0)

    def gather(self, block):
        block = self.lead(block)
        return self.close(block, self.cross(block))

    def far(self, total, kind):
        if not self.square:
            return ()
        y, x = len(self.sizes) - 2, len(self.sizes) - 1
        quarter = total.shape[0] // 4
        half = quarter // 2
        far = total[3 * quarter :]
        return self.move(far[:half].astype(kind), x, 1), self.move(far[half:].astype(kind), y, 1)

    def near(self, total, via, kind):
        if not self.square:
            return ()
        y, x = len(self.sizes) - 2, len(self.sizes) - 1
        quarter = total.shape[0] // 4
        half = quarter // 2
        via_x, via_y = via
        to_y, to_x = total[quarter : 2 * quarter], total[2 * quarter : 3 * quarter]
        to_y = jnp.concatenate([(to_y[:half].astype(F32) + via_x).astype(kind), to_y[half:].astype(kind)], axis=0)
        to_x = jnp.concatenate([to_x[:half].astype(kind), (to_x[half:].astype(F32) + via_y).astype(kind)], axis=0)
        return self.move(to_x, x, 1), self.move(to_y, y, 1)

    def last(self, total, crossed, kind):
        stages = len(self.sizes)
        if self.square:
            own = total[: total.shape[0] // 4].astype(F32)
            total = own + crossed[0].astype(F32) + crossed[1].astype(F32)
            stages -= 2
        for stage in reversed(range(stages)):
            size = self.sizes[stage]
            piece = total.shape[0] // size
            parts = [total[i * piece : (i + 1) * piece] for i in range(size)]
            total = parts[0].astype(F32)
            for step in range(1, size):
                total = total + self.move(parts[step].astype(kind), stage, size - step).astype(F32)
        return total

    def scatter(self, total, kind):
        return self.last(total, self.near(total, self.far(total, kind), kind), kind)

    def width_order(self, width):
        me = lax.axis_index("dp")
        rows = width // self.count
        column = jnp.arange(width, dtype=jnp.int32)
        inner, block = column % rows, column // rows
        found = jnp.zeros_like(column)
        for size, stride in zip(self.sizes, self.strides):
            step, block = block % size, block // size
            digit = me // stride % size
            if size == 4:
                place = jnp.bitwise_xor(digit, digit // 2)
                back = (place - step + size) % size
                source = jnp.bitwise_xor(back, back // 2)
            else:
                source = (digit - step + size) % size
            found = found + source * stride
        return found * rows + inner


def ring_place(digit):
    return digit + (digit // 2) * (1 - 2 * (digit % 2))


def partners_of(me):
    digit = me // 4
    place = ring_place(digit)
    along = [me + (ring_place((place + step) % 4) - digit) * 4 for step in range(1, 4)]
    return along, me + 1 - 2 * (me % 2), me + 2 - 4 * ((me // 2) % 2)


def greet(along, x_way, y_way, other):
    barrier = pltpu.get_barrier_semaphore()
    for device in along + [x_way, y_way]:
        pl.semaphore_signal(barrier, inc=1, device_id={"dp": device}, device_id_type=MESH)
    pl.semaphore_signal(barrier, inc=1, device_id={"tensor": other}, device_id_type=MESH)
    pl.semaphore_wait(barrier, 6)


def gather_kernel(vec_ref, qkv_ref, vec_out, qkv_out, vec_other, send, recv, local):
    along, x_way, y_way = partners_of(lax.axis_index("dp"))
    other = 1 - lax.axis_index("tensor")
    greet(along, x_way, y_way, other)
    blocks, outs = (vec_ref, qkv_ref), (vec_out, qkv_out)
    copies = {}

    def start(kind, source, slot, device):
        copy = pltpu.make_async_remote_copy(
            src_ref=source,
            dst_ref=outs[kind].at[slot],
            send_sem=send.at[kind, slot],
            recv_sem=recv.at[kind, slot],
            device_id={"dp": device},
            device_id_type=MESH,
        )
        copy.start()
        copies[kind, slot] = copy

    kept = []
    for kind in range(2):
        for step in range(1, 4):
            start(kind, blocks[kind], step, along[step - 1])
        start(kind, blocks[kind], 4, y_way)
        start(kind, blocks[kind], 8, x_way)
        copy = pltpu.make_async_copy(blocks[kind], outs[kind].at[0], local.at[kind])
        copy.start()
        kept.append(copy)
    for step in range(1, 4):
        for kind in range(2):
            copies[kind, step].wait_recv()
            start(kind, outs[kind].at[step], 4 + step, y_way)
            start(kind, outs[kind].at[step], 8 + step, x_way)
        if step == 1:
            for kind in range(2):
                copies[kind, 4].wait_recv()
                start(kind, outs[kind].at[4], 12, x_way)
    for step in range(1, 4):
        for kind in range(2):
            slot = 4 + step if step < 2 else 8 + step
            copies[kind, slot].wait_recv()
            start(kind, outs[kind].at[slot], 12 + step, x_way if step < 2 else y_way)
    waited = (1, 2, 3, 4, 5, 10, 11)
    rest = [slot for slot in range(4, 16) if slot not in waited]
    for slot in rest:
        copies[0, slot].wait_recv()
    kept[0].wait()
    shared = pltpu.make_async_remote_copy(
        src_ref=vec_out,
        dst_ref=vec_other,
        send_sem=send.at[0, 0],
        recv_sem=recv.at[0, 0],
        device_id={"tensor": other},
        device_id_type=MESH,
    )
    shared.start()
    for slot in rest:
        copies[1, slot].wait_recv()
    kept[1].wait()
    for copy in copies.values():
        copy.wait_send()
    shared.wait()


def gather_first(vectors, qkv):
    anywhere = pl.BlockSpec(memory_space=pl.ANY)
    inside = pl.BlockSpec(memory_space=pltpu.VMEM)
    return pl.pallas_call(
        gather_kernel,
        out_shape=(
            jax.ShapeDtypeStruct((16, *vectors.shape), vectors.dtype),
            jax.ShapeDtypeStruct((16, *qkv.shape), qkv.dtype),
            jax.ShapeDtypeStruct((16, *vectors.shape), vectors.dtype),
        ),
        in_specs=[inside, inside],
        out_specs=(anywhere, anywhere, anywhere),
        scratch_shapes=[
            pltpu.SemaphoreType.DMA((2, 16)),
            pltpu.SemaphoreType.DMA((2, 16)),
            pltpu.SemaphoreType.DMA((2,)),
        ],
        compiler_params=pltpu.CompilerParams(collective_id=0, has_side_effects=True),
        name="gather_first",
    )(vectors, qkv)


def swap(value):
    return lax.ppermute(value, "tensor", [(0, 1), (1, 0)])


def after(value, earlier):
    return lax.optimization_barrier((value, earlier))[0]


def dot(a, b):
    return lax.dot_general(a, b, (((1,), (0,)), ((), ())), preferred_element_type=F32)


def dot_nt(a, b):
    return lax.dot_general(a, b, (((1,), (1,)), ((), ())), preferred_element_type=F32)


def dot_tn(a, b):
    return lax.dot_general(a, b, (((0,), (0,)), ((), ())), preferred_element_type=F32)


def norm_parts(features):
    average = jnp.mean(features, axis=-1, keepdims=True)
    centered = features - average
    spread = jnp.mean(centered * centered, axis=-1, keepdims=True)
    scale = lax.rsqrt(spread + EPS)
    return centered * scale, scale


def norm_back(grad, normed, scale, gain):
    h = grad * gain
    return scale * (
        h - jnp.mean(h, axis=-1, keepdims=True) - normed * jnp.mean(h * normed, axis=-1, keepdims=True)
    )


def allowed_mask(first_query, query_count, key_count, prefix_length):
    query_pos = first_query + jnp.arange(query_count, dtype=jnp.int32)
    key_pos = jnp.arange(key_count, dtype=jnp.int32)
    return (key_pos[None, :] <= query_pos[:, None]) | (key_pos[None, :] < prefix_length)


def block_scores(query_rows, seq_keys, allowed, score_scale):
    scores = (
        jnp.einsum("qhd,khd->hqk", query_rows, seq_keys, preferred_element_type=F32)
        * score_scale
    )
    return jnp.where(allowed[None], scores, NEGATIVE)


def attention_pieces(length, heads_local):
    half, few = length // 2, heads_local // 2
    return [(0, half, 0, heads_local), (half, length, 0, few), (half, length, few, heads_local)]


def head_rows(rows, first_head, end_head, head_dim):
    return rows[:, first_head * head_dim : end_head * head_dim].reshape(
        rows.shape[0], end_head - first_head, head_dim
    )


def attention_forward(queries, keys_all, values_all, prefix, heads_local, head_dim, gates):
    score_scale = head_dim ** (-0.5)
    outputs = []
    logsums = []
    for piece, gate in zip(attention_pieces(queries.shape[0], heads_local), gates):
        first_row, reach, first_head, end_head = piece
        seq_keys = head_rows(keys_all[:reach], first_head, end_head, head_dim)
        seq_values = head_rows(values_all[:reach], first_head, end_head, head_dim)
        query_rows = head_rows(after(queries[first_row:reach], gate), first_head, end_head, head_dim)
        rows = reach - first_row
        allowed = allowed_mask(first_row, rows, reach, prefix[0])
        scores = block_scores(query_rows, seq_keys, allowed, score_scale)
        top_score = jnp.max(scores, axis=-1, keepdims=True)
        powered = jnp.exp(scores - top_score)
        totals = jnp.sum(powered, axis=-1, keepdims=True)
        probabilities = (powered / totals).astype(BF)
        attended = jnp.einsum(
            "hqk,khd->qhd", probabilities, seq_values, preferred_element_type=F32
        )
        outputs.append(attended.reshape(rows, (end_head - first_head) * head_dim).astype(BF))
        logsums.append(top_score + jnp.log(totals))
    lower = jnp.concatenate(outputs[1:], axis=1)
    return (jnp.concatenate([outputs[0], lower], axis=0), [logsums[0], jnp.concatenate(logsums[1:], axis=0)])


def attention_backward(
    queries, keys_all, values_all, prefix, logsums, back_attended, heads_local, head_dim
):
    score_scale = head_dim ** (-0.5)
    length = queries.shape[0]
    block_rows = length // 2
    back_query_list = []
    back_keys = jnp.zeros((length, heads_local, head_dim), F32)
    back_values = jnp.zeros((length, heads_local, head_dim), F32)
    for block_index in range(2):
        first_row = block_index * block_rows
        reach = first_row + block_rows
        seq_keys = keys_all[:reach].reshape(reach, heads_local, head_dim)
        seq_values = values_all[:reach].reshape(reach, heads_local, head_dim)
        query_rows = queries[first_row:reach].reshape(block_rows, heads_local, head_dim)
        back_rows = back_attended[first_row:reach].reshape(block_rows, heads_local, head_dim)
        allowed = allowed_mask(first_row, block_rows, reach, prefix[0])
        scores = block_scores(query_rows, seq_keys, allowed, score_scale)
        probabilities = jnp.exp(scores - logsums[block_index])
        back_probs = jnp.einsum("qhd,khd->hqk", back_rows, seq_values, preferred_element_type=F32)
        row_dot = jnp.sum(probabilities * back_probs, axis=-1, keepdims=True)
        back_scores = (probabilities * (back_probs - row_dot)).astype(BF)
        back_query = (
            jnp.einsum("hqk,khd->qhd", back_scores, seq_keys, preferred_element_type=F32)
            * score_scale
        )
        back_key_part = (
            jnp.einsum("hqk,qhd->khd", back_scores, query_rows, preferred_element_type=F32)
            * score_scale
        )
        back_value_part = jnp.einsum(
            "hqk,qhd->khd", probabilities.astype(BF), back_rows, preferred_element_type=F32
        )
        back_keys = back_keys.at[:reach].add(back_key_part)
        back_values = back_values.at[:reach].add(back_value_part)
        back_query_list.append(back_query.reshape(block_rows, heads_local * head_dim))
    back_queries = jnp.concatenate(back_query_list, axis=0).astype(BF)
    flat = (length, heads_local * head_dim)
    return jnp.concatenate(
        [back_queries, back_keys.reshape(flat).astype(BF), back_values.reshape(flat).astype(BF)], axis=1
    )


def body(
    ring,
    tokens,
    cotangent,
    prefix,
    routes,
    norm1_gain,
    norm1_bias,
    w_query,
    w_key,
    w_value,
    w_out,
    norm2_gain,
    norm2_bias,
    centroids,
    expert_in,
    expert_out,
):
    side = lax.axis_index("tensor")
    own_rows, width = tokens.shape
    all_rows = 2 * own_rows
    head_dim = width // HEADS
    heads_local = w_query.shape[1] // head_dim
    part = w_query.shape[1]
    rows = w_query.shape[0]
    experts, _, hidden = expert_in.shape
    count = ring.count

    def both(own):
        other = swap(own)
        return jnp.where(
            side == 0, jnp.concatenate([own, other], 0), jnp.concatenate([other, own], 0)
        )

    vectors = jnp.concatenate(
        [
            norm1_gain[None],
            norm1_bias[None],
            norm2_gain[None],
            norm2_bias[None],
            centroids,
        ],
        axis=0,
    )
    small_count = vectors.shape[0]
    qkv_block = jnp.concatenate([w_query, w_key, w_value], axis=1)
    in_block = jnp.concatenate(
        [w_out.T, expert_in.transpose(1, 0, 2).reshape(rows, experts * hidden)], axis=1
    )
    out_block = expert_out.transpose(2, 0, 1).reshape(rows, experts * hidden)
    in_lead = ring.lead(in_block)
    if count == 16:
        padded = jnp.pad(vectors, ((0, 8 - small_count), (0, 128 - rows // 2)))
        table, qkv_w, other_table = gather_first(padded, qkv_block)
        table, other_table = (t[:, :small_count, : rows // 2] for t in (table, other_table))
        table = jnp.where(
            side == 0,
            jnp.concatenate([table, other_table], 2),
            jnp.concatenate([other_table, table], 2),
        )
        qkv_w = qkv_w.reshape(width, 3 * part)
    else:
        other_vectors = swap(vectors)
        vectors = jnp.where(
            side == 0,
            jnp.concatenate([vectors, other_vectors], 1),
            jnp.concatenate([other_vectors, vectors], 1),
        )
        table = ring.gather(vectors.reshape(1, small_count * rows)).reshape(count, small_count, rows)
        qkv_w = ring.gather(qkv_block)
    table = table.transpose(1, 0, 2).reshape(small_count, width)
    gain_one, bias_one, gain_two, bias_two = (table[i : i + 1] for i in range(4))
    centres = table[4:]

    in_crossed = ring.cross(after(in_lead, qkv_w))
    out_lead = ring.lead(after(out_block, in_lead))
    in_all = ring.close(in_lead, in_crossed)
    out_lead = after(out_lead, in_crossed)
    out_crossed = ring.cross(after(out_lead, in_all))
    back_w = ring.close(out_lead, out_crossed)
    out_w, in_w = in_all[:, :part], in_all[:, part:]

    found = ring.width_order(width)
    to_order = (jnp.arange(width, dtype=jnp.int32)[:, None] == found[None, :]).astype(BF)
    tokens_all = dot(both(tokens), to_order)
    back_all = dot(both(cotangent), to_order)

    normed_one, scale_one = norm_parts(tokens_all)
    first_rows = (normed_one * gain_one + bias_one).astype(BF)
    qkv = dot(first_rows, qkv_w).astype(BF)
    queries, keys_all, values_all = qkv[:, :part], qkv[:, part : 2 * part], qkv[:, 2 * part :]
    attended, logsums = attention_forward(
        queries, keys_all, values_all, prefix, heads_local, head_dim, [in_lead, in_lead, in_crossed]
    )
    attn_terms = dot_nt(attended, out_w).astype(BF)
    residual = tokens_all + (attn_terms.astype(F32) + swap(attn_terms).astype(F32))
    normed_two, scale_two = norm_parts(residual)
    second_rows = (normed_two * gain_two + bias_two).astype(BF)
    second_wide = second_rows.astype(F32)

    is_last = routes == 1
    ones_before = jnp.tril(jnp.ones((all_rows, all_rows), BF))
    last_before = dot(ones_before, is_last.astype(BF)).astype(jnp.int32)
    position = jnp.arange(all_rows, dtype=jnp.int32)[:, None]
    first_count = all_rows - last_before[all_rows - 1, 0]
    place = jnp.where(is_last, first_count + last_before - 1, position - last_before)
    sort_to = (place == jnp.arange(all_rows, dtype=jnp.int32)[None, :]).astype(BF)
    tail = all_rows - CAP
    in_first = position < first_count

    centre_rows = jnp.where(is_last, centres[1:2], centres[0:1])
    gate = jax.nn.sigmoid(jnp.sum(second_wide * centre_rows, axis=-1, keepdims=True))
    back_branch = (gate * back_all).astype(BF)
    picked = dot_tn(sort_to, second_rows).astype(BF)
    back_slots = dot_tn(sort_to, back_branch).astype(BF)
    windows = (slice(0, CAP), slice(tail, all_rows))
    masks = (in_first[:CAP], ~in_first[tail:])
    slot_out, back_picked, grads_in, grads_out = [], [], [], []
    hidden_of = []
    for e in range(2):
        columns = slice(e * hidden, (e + 1) * hidden)
        rows_in = picked[windows[e]]
        back_rows = jnp.where(masks[e], back_slots[windows[e]], jnp.zeros((), BF))
        up = dot(rows_in, in_w[:, columns])
        activated = jax.nn.gelu(up).astype(BF)
        grads_out.append(dot_tn(back_rows, activated).astype(BF))
        hidden_of.append((columns, rows_in, back_rows, up, activated))
    grads_out = jnp.concatenate(grads_out, axis=1)
    out_via = ring.far(grads_out, BF)
    for e, (columns, rows_in, back_rows, up, activated) in enumerate(hidden_of):
        if e == 1:
            back_rows = after(back_rows, out_via)
        slot_out.append(dot_nt(activated, back_w[:, columns]).astype(BF))
        back_activated = dot(back_rows, back_w[:, columns])
        back_up = jax.vjp(jax.nn.gelu, up)[1](back_activated)[0].astype(BF)
        grads_in.append(dot_tn(rows_in, back_up).astype(BF))
        back_picked.append(dot_nt(back_up, in_w[:, columns]).astype(BF))
    grads_in = jnp.concatenate(grads_in, axis=1)
    out_near = ring.near(grads_out, out_via, BF)
    in_via = ring.far(after(grads_in, out_via), BF)

    def unsort(pieces):
        joined = jnp.concatenate(
            [
                pieces[0][:tail],
                jnp.where(in_first[tail:CAP], pieces[0][tail:], pieces[1][: CAP - tail]),
                pieces[1][CAP - tail :],
            ],
            axis=0,
        )
        return dot(sort_to, joined).astype(BF)

    row_terms = unsort(slot_out)
    expert_rows = row_terms.astype(F32) + swap(row_terms).astype(F32)
    block_all = (residual + gate * expert_rows).astype(BF)
    first_own = side * own_rows
    block_out = dot_nt(lax.dynamic_slice_in_dim(block_all, first_own, own_rows), to_order).astype(BF)
    back_score = jnp.sum(back_all * expert_rows, axis=-1, keepdims=True) * gate * (1.0 - gate)

    second_terms = unsort(back_picked)
    back_second = second_terms.astype(F32) + swap(second_terms).astype(F32) + back_score * centre_rows
    weighted = back_score * second_wide
    grad_centre = jnp.stack(
        [
            jnp.sum(jnp.where(is_last, 0.0, weighted), axis=0),
            jnp.sum(jnp.where(is_last, weighted, 0.0), axis=0),
        ]
    )
    grad_gain_two = jnp.sum(back_second * normed_two, axis=0)
    grad_bias_two = jnp.sum(back_second, axis=0)
    back_residual = back_all + norm_back(back_second, normed_two, scale_two, gain_two)
    back_out = after(back_residual.astype(BF), (out_near, in_via))
    grads_out = ring.last(grads_out, out_near, BF)
    in_near = ring.near(grads_in, in_via, BF)
    back_attended = dot(back_out, out_w).astype(BF)
    grad_out = dot_tn(back_out, attended).astype(BF)
    back_qkv = attention_backward(
        queries, keys_all, values_all, prefix, logsums, back_attended, heads_local, head_dim
    )
    back_qkv = after(back_qkv, in_near)
    grads_in = ring.last(grads_in, in_near, BF)
    grad_qkv = dot_tn(first_rows, back_qkv).astype(BF)
    first_terms = dot_nt(back_qkv, qkv_w).astype(BF)
    own_terms = lax.dynamic_slice_in_dim(first_terms, first_own, own_rows)
    other_terms = lax.dynamic_slice_in_dim(first_terms, own_rows - first_own, own_rows)
    back_first = own_terms.astype(F32) + swap(other_terms).astype(F32)

    def mine(value):
        return lax.dynamic_slice_in_dim(value, first_own, own_rows)

    normed_own = mine(normed_one)
    back_norm_one = norm_back(back_first, normed_own, mine(scale_one), gain_one)
    grad_tokens = dot_nt(
        (mine(back_residual) + back_norm_one).astype(BF), to_order
    ).astype(BF)
    one_part = jnp.stack([jnp.sum(back_first * normed_own, axis=0), jnp.sum(back_first, axis=0)])
    one_part = one_part + swap(one_part)
    small = jnp.concatenate(
        [one_part, grad_gain_two[None], grad_bias_two[None], grad_centre], axis=0
    )
    small = small.reshape(small_count, count, rows).transpose(1, 0, 2).reshape(count, small_count * rows)

    grad_first = ring.scatter(jnp.concatenate([grad_out, grad_qkv], axis=1), BF)
    grad_out, grad_qkv = grad_first[:, :part], grad_first[:, part:]
    small = ring.scatter(small, F32).reshape(small_count, rows)
    small = lax.dynamic_slice_in_dim(small, side * (rows // 2), rows // 2, axis=1)
    return (
        block_out,
        grad_tokens,
        small[0],
        small[1],
        grad_qkv[:, :part],
        grad_qkv[:, part : 2 * part],
        grad_qkv[:, 2 * part :],
        grad_out.T,
        small[2],
        small[3],
        small[4:],
        grads_in.reshape(rows, experts, hidden).transpose(1, 0, 2),
        grads_out.reshape(rows, experts, hidden).transpose(1, 2, 0),
    )


def solution(mesh):
    ring = Ring(mesh.shape["dp"])
    both, rows = P(("dp", "tensor")), P(("dp", "tensor"), None)
    columns = P("dp", "tensor")

    def step(*arguments):
        return body(ring, *arguments)

    return jax.shard_map(
        step,
        mesh=mesh,
        in_specs=(
            rows,
            rows,
            P("dp"),
            P("dp", None),
            both,
            both,
            columns,
            columns,
            columns,
            P("tensor", "dp"),
            both,
            both,
            P(None, ("dp", "tensor")),
            P(None, "dp", "tensor"),
            P(None, "tensor", "dp"),
        ),
        out_specs=(
            rows,
            rows,
            both,
            both,
            columns,
            columns,
            columns,
            P("tensor", "dp"),
            both,
            both,
            P(None, ("dp", "tensor")),
            P(None, "dp", "tensor"),
            P(None, "tensor", "dp"),
        ),
        check_vma=False,
    )
```

```python
import jax
import jax.numpy as jnp
from jax import lax
from jax.experimental import pallas as pl
from jax.experimental.pallas import tpu as pltpu
from jax.sharding import PartitionSpec as P


HEADS = 12
CAP = 640
EPS = 1e-05
NEGATIVE = -1e30
BF = jnp.bfloat16
F32 = jnp.float32
MESH = pl.DeviceIdType.MESH


def factors_of(count):
    rest, sizes = count // 2, []
    while rest % 4 == 0:
        sizes.append(4)
        rest //= 4
    while rest % 2 == 0 and rest > 1:
        sizes.append(2)
        rest //= 2
    return sizes + ([2] if count > 1 else [])


class Ring:
    def __init__(self, count):
        self.count = count
        self.sizes = factors_of(count)
        self.strides = []
        stride = count
        for size in self.sizes:
            stride //= size
            self.strides.append(stride)
        self.square = len(self.sizes) >= 2 and self.sizes[-1] == 2 and self.sizes[-2] == 2

    def order(self, size):
        return [0, 1, 3, 2] if size == 4 else list(range(size))

    def shift(self, stage, step):
        size, stride = self.sizes[stage], self.strides[stage]
        order = self.order(size)
        pairs = []
        for source in range(self.count):
            digit = source // stride % size
            target = order[(order.index(digit) + step) % size]
            pairs.append((source, source + (target - digit) * stride))
        return pairs

    def move(self, value, stage, step):
        return lax.ppermute(value, "dp", self.shift(stage, step))

    def lead(self, block):
        for stage in range(len(self.sizes) - (2 if self.square else 0)):
            parts = [block] + [self.move(block, stage, s) for s in range(1, self.sizes[stage])]
            block = jnp.concatenate(parts, axis=0)
        return block

    def cross(self, block):
        if not self.square:
            return ()
        y, x = len(self.sizes) - 2, len(self.sizes) - 1
        return self.move(block, x, 1), self.move(block, y, 1)

    def close(self, block, crossed):
        if not self.square:
            return block
        y, x = len(self.sizes) - 2, len(self.sizes) - 1
        half = block.shape[0] // 2
        from_x, from_y = crossed
        low, high = self.move(from_y[:half], x, 1), self.move(from_x[half:], y, 1)
        return jnp.concatenate([block, from_y, from_x, low, high], axis=0)

    def gather(self, block):
        block = self.lead(block)
        return self.close(block, self.cross(block))

    def far(self, total, kind):
        if not self.square:
            return ()
        y, x = len(self.sizes) - 2, len(self.sizes) - 1
        quarter = total.shape[0] // 4
        half = quarter // 2
        far = total[3 * quarter :]
        return self.move(far[:half].astype(kind), x, 1), self.move(far[half:].astype(kind), y, 1)

    def near(self, total, via, kind):
        if not self.square:
            return ()
        y, x = len(self.sizes) - 2, len(self.sizes) - 1
        quarter = total.shape[0] // 4
        half = quarter // 2
        via_x, via_y = via
        to_y, to_x = total[quarter : 2 * quarter], total[2 * quarter : 3 * quarter]
        to_y = jnp.concatenate([(to_y[:half].astype(F32) + via_x).astype(kind), to_y[half:].astype(kind)], axis=0)
        to_x = jnp.concatenate([to_x[:half].astype(kind), (to_x[half:].astype(F32) + via_y).astype(kind)], axis=0)
        return self.move(to_x, x, 1), self.move(to_y, y, 1)

    def last(self, total, crossed, kind):
        stages = len(self.sizes)
        if self.square:
            own = total[: total.shape[0] // 4].astype(F32)
            total = own + crossed[0].astype(F32) + crossed[1].astype(F32)
            stages -= 2
        for stage in reversed(range(stages)):
            size = self.sizes[stage]
            piece = total.shape[0] // size
            parts = [total[i * piece : (i + 1) * piece] for i in range(size)]
            total = parts[0].astype(F32)
            for step in range(1, size):
                total = total + self.move(parts[step].astype(kind), stage, size - step).astype(F32)
        return total

    def scatter(self, total, kind):
        return self.last(total, self.near(total, self.far(total, kind), kind), kind)

    def width_order(self, width):
        me = lax.axis_index("dp")
        rows = width // self.count
        column = jnp.arange(width, dtype=jnp.int32)
        inner, block = column % rows, column // rows
        found = jnp.zeros_like(column)
        for size, stride in zip(self.sizes, self.strides):
            step, block = block % size, block // size
            digit = me // stride % size
            if size == 4:
                place = jnp.bitwise_xor(digit, digit // 2)
                back = (place - step + size) % size
                source = jnp.bitwise_xor(back, back // 2)
            else:
                source = (digit - step + size) % size
            found = found + source * stride
        return found * rows + inner


def ring_place(digit):
    return digit + (digit // 2) * (1 - 2 * (digit % 2))


def partners_of(me):
    digit = me // 4
    place = ring_place(digit)
    along = [me + (ring_place((place + step) % 4) - digit) * 4 for step in range(1, 4)]
    return along, me + 1 - 2 * (me % 2), me + 2 - 4 * ((me // 2) % 2)


def greet(along, x_way, y_way, other):
    barrier = pltpu.get_barrier_semaphore()
    for device in along + [x_way, y_way]:
        pl.semaphore_signal(barrier, inc=1, device_id={"dp": device}, device_id_type=MESH)
    pl.semaphore_signal(barrier, inc=1, device_id={"tensor": other}, device_id_type=MESH)
    pl.semaphore_wait(barrier, 6)


def gather_kernel(vec_ref, qkv_ref, vec_out, qkv_out, vec_other, send, recv, local):
    along, x_way, y_way = partners_of(lax.axis_index("dp"))
    other = 1 - lax.axis_index("tensor")
    greet(along, x_way, y_way, other)
    blocks, outs = (vec_ref, qkv_ref), (vec_out, qkv_out)
    copies = {}

    def start(kind, source, slot, device):
        copy = pltpu.make_async_remote_copy(
            src_ref=source,
            dst_ref=outs[kind].at[slot],
            send_sem=send.at[kind, slot],
            recv_sem=recv.at[kind, slot],
            device_id={"dp": device},
            device_id_type=MESH,
        )
        copy.start()
        copies[kind, slot] = copy

    kept = []
    for kind in range(2):
        for step in range(1, 4):
            start(kind, blocks[kind], step, along[step - 1])
        start(kind, blocks[kind], 4, y_way)
        start(kind, blocks[kind], 8, x_way)
        copy = pltpu.make_async_copy(blocks[kind], outs[kind].at[0], local.at[kind])
        copy.start()
        kept.append(copy)
    for step in range(1, 4):
        for kind in range(2):
            copies[kind, step].wait_recv()
            start(kind, outs[kind].at[step], 4 + step, y_way)
            start(kind, outs[kind].at[step], 8 + step, x_way)
        if step == 1:
            for kind in range(2):
                copies[kind, 4].wait_recv()
                start(kind, outs[kind].at[4], 12, x_way)
    for step in range(1, 4):
        for kind in range(2):
            slot = 4 + step if step < 2 else 8 + step
            copies[kind, slot].wait_recv()
            start(kind, outs[kind].at[slot], 12 + step, x_way if step < 2 else y_way)
    waited = (1, 2, 3, 4, 5, 10, 11)
    rest = [slot for slot in range(4, 16) if slot not in waited]
    for slot in rest:
        copies[0, slot].wait_recv()
    kept[0].wait()
    shared = pltpu.make_async_remote_copy(
        src_ref=vec_out,
        dst_ref=vec_other,
        send_sem=send.at[0, 0],
        recv_sem=recv.at[0, 0],
        device_id={"tensor": other},
        device_id_type=MESH,
    )
    shared.start()
    for slot in rest:
        copies[1, slot].wait_recv()
    kept[1].wait()
    for copy in copies.values():
        copy.wait_send()
    shared.wait()


def gather_first(vectors, qkv):
    anywhere = pl.BlockSpec(memory_space=pl.ANY)
    inside = pl.BlockSpec(memory_space=pltpu.VMEM)
    return pl.pallas_call(
        gather_kernel,
        out_shape=(
            jax.ShapeDtypeStruct((16, *vectors.shape), vectors.dtype),
            jax.ShapeDtypeStruct((16, *qkv.shape), qkv.dtype),
            jax.ShapeDtypeStruct((16, *vectors.shape), vectors.dtype),
        ),
        in_specs=[inside, inside],
        out_specs=(anywhere, anywhere, anywhere),
        scratch_shapes=[
            pltpu.SemaphoreType.DMA((2, 16)),
            pltpu.SemaphoreType.DMA((2, 16)),
            pltpu.SemaphoreType.DMA((2,)),
        ],
        compiler_params=pltpu.CompilerParams(collective_id=0, has_side_effects=True),
        name="gather_first",
    )(vectors, qkv)


def scatter_kernel(
    small_ref, grad_ref, small_out, grad_out,
    small_via, small_fold, small_cross, small_sums, small_last,
    grad_via, grad_fold, grad_cross, grad_sums, grad_last,
    send, recv,
):
    along, x_way, y_way = partners_of(lax.axis_index("dp"))
    greet(along, x_way, y_way, 1 - lax.axis_index("tensor"))
    blocks, results = (small_ref, grad_ref), (small_out, grad_out)
    via, fold = (small_via, grad_via), (small_fold, grad_fold)
    cross, sums, last = (small_cross, grad_cross), (small_sums, grad_sums), (small_last, grad_last)
    copies = {}

    def start(kind, source, target, number, device):
        copy = pltpu.make_async_remote_copy(
            src_ref=source,
            dst_ref=target,
            send_sem=send.at[kind, number],
            recv_sem=recv.at[kind, number],
            device_id={"dp": device},
            device_id_type=MESH,
        )
        copy.start()
        copies[kind, number] = copy

    for kind in range(2):
        for step in range(4):
            way = x_way if step < 2 else y_way
            start(kind, blocks[kind].at[12 + step], via[kind].at[step], step, way)
    for kind in range(2):
        for step in range(2):
            start(kind, blocks[kind].at[6 + step], cross[kind].at[2 + step], 6 + step, y_way)
            start(kind, blocks[kind].at[8 + step], cross[kind].at[4 + step], 8 + step, x_way)
    for step in (1, 3, 0, 2):
        for kind in range(2):
            slot = 4 + step if step < 2 else 8 + step
            copies[kind, step].wait_recv()
            folded = blocks[kind][slot].astype(F32) + via[kind][step].astype(F32)
            fold[kind][step] = folded.astype(fold[kind].dtype)
            start(kind, fold[kind].at[step], cross[kind].at[slot - 4], slot, y_way if step < 2 else x_way)
    for step in (3, 1, 2, 0):
        for kind in range(2):
            copies[kind, 4 + step].wait_recv()
            copies[kind, 8 + step].wait_recv()
            total = blocks[kind][step].astype(F32)
            total = total + cross[kind][step].astype(F32) + cross[kind][4 + step].astype(F32)
            if step:
                sums[kind][step] = total.astype(sums[kind].dtype)
                start(kind, sums[kind].at[step], last[kind].at[step], 12 + step, along[3 - step])
            else:
                results[kind][...] = total
    for kind in range(2):
        for step in range(1, 4):
            copies[kind, 12 + step].wait_recv()
            results[kind][...] += last[kind][step].astype(F32)
    for copy in copies.values():
        copy.wait_send()


def scatter_last(small, grads):
    inside = pl.BlockSpec(memory_space=pltpu.VMEM)
    scratch = []
    for value in (small, grads):
        for slots in (4, 4, 8, 4, 4):
            scratch.append(pltpu.VMEM((slots, *value.shape[1:]), value.dtype))
    return pl.pallas_call(
        scatter_kernel,
        out_shape=(
            jax.ShapeDtypeStruct(small.shape[1:], F32),
            jax.ShapeDtypeStruct(grads.shape[1:], F32),
        ),
        in_specs=[inside, inside],
        out_specs=(inside, inside),
        scratch_shapes=scratch
        + [pltpu.SemaphoreType.DMA((2, 16)), pltpu.SemaphoreType.DMA((2, 16))],
        compiler_params=pltpu.CompilerParams(collective_id=1, has_side_effects=True),
        name="scatter_last",
    )(small, grads)


def swap(value):
    return lax.ppermute(value, "tensor", [(0, 1), (1, 0)])


def after(value, earlier):
    return lax.optimization_barrier((value, earlier))[0]


def dot(a, b):
    return lax.dot_general(a, b, (((1,), (0,)), ((), ())), preferred_element_type=F32)


def dot_nt(a, b):
    return lax.dot_general(a, b, (((1,), (1,)), ((), ())), preferred_element_type=F32)


def dot_tn(a, b):
    return lax.dot_general(a, b, (((0,), (0,)), ((), ())), preferred_element_type=F32)


def norm_parts(features):
    average = jnp.mean(features, axis=-1, keepdims=True)
    centered = features - average
    spread = jnp.mean(centered * centered, axis=-1, keepdims=True)
    scale = lax.rsqrt(spread + EPS)
    return centered * scale, scale


def norm_back(grad, normed, scale, gain):
    h = grad * gain
    return scale * (
        h - jnp.mean(h, axis=-1, keepdims=True) - normed * jnp.mean(h * normed, axis=-1, keepdims=True)
    )


def allowed_mask(first_query, query_count, key_count, prefix_length):
    query_pos = first_query + jnp.arange(query_count, dtype=jnp.int32)
    key_pos = jnp.arange(key_count, dtype=jnp.int32)
    return (key_pos[None, :] <= query_pos[:, None]) | (key_pos[None, :] < prefix_length)


def block_scores(query_rows, seq_keys, allowed, score_scale):
    scores = (
        jnp.einsum("qhd,khd->hqk", query_rows, seq_keys, preferred_element_type=F32)
        * score_scale
    )
    return jnp.where(allowed[None], scores, NEGATIVE)


def attention_pieces(length, heads_local):
    half, few = length // 2, heads_local // 2
    return [(0, half, 0, heads_local), (half, length, 0, few), (half, length, few, heads_local)]


def head_rows(rows, first_head, end_head, head_dim):
    return rows[:, first_head * head_dim : end_head * head_dim].reshape(
        rows.shape[0], end_head - first_head, head_dim
    )


def attention_forward(queries, keys_all, values_all, prefix, heads_local, head_dim, gates):
    outputs, logsums = [], []
    for number, piece in enumerate(attention_pieces(queries.shape[0], heads_local)):
        output, logsum = forward_piece(
            piece, after(queries, gates[number]), keys_all, values_all, prefix, head_dim
        )
        outputs.append(output)
        logsums.append(logsum)
    lower = jnp.concatenate(outputs[1:], axis=1)
    return (jnp.concatenate([outputs[0], lower], axis=0), logsums)


def forward_piece(piece, queries, keys_all, values_all, prefix, head_dim):
    first_row, reach, first_head, end_head = piece
    rows = reach - first_row
    seq_keys = head_rows(keys_all[:reach], first_head, end_head, head_dim)
    seq_values = head_rows(values_all[:reach], first_head, end_head, head_dim)
    query_rows = head_rows(queries[first_row:reach], first_head, end_head, head_dim)
    allowed = allowed_mask(first_row, rows, reach, prefix[0])
    scores = block_scores(query_rows, seq_keys, allowed, head_dim ** (-0.5))
    top_score = jnp.max(scores, axis=-1, keepdims=True)
    powered = jnp.exp(scores - top_score)
    totals = jnp.sum(powered, axis=-1, keepdims=True)
    probabilities = (powered / totals).astype(BF)
    attended = jnp.einsum("hqk,khd->qhd", probabilities, seq_values, preferred_element_type=F32)
    return (
        attended.reshape(rows, (end_head - first_head) * head_dim).astype(BF),
        top_score + jnp.log(totals),
    )


def attention_backward(
    queries, keys_all, values_all, prefix, logsums, back_attended, heads_local, head_dim, gates
):
    length = queries.shape[0]
    parts = []
    for number, piece in enumerate(attention_pieces(length, heads_local)):
        parts.append(
            backward_piece(
                piece,
                queries,
                keys_all,
                values_all,
                prefix,
                logsums[number],
                after(back_attended, gates[number]),
                head_dim,
            )
        )
    upper, lower = parts[0], [jnp.concatenate([a, b], axis=1) for a, b in zip(*parts[1:])]
    half = length // 2
    back_queries = jnp.concatenate([upper[0], lower[0]], axis=0)
    back_keys = jnp.concatenate([lower[1][:half] + upper[1], lower[1][half:]], axis=0)
    back_values = jnp.concatenate([lower[2][:half] + upper[2], lower[2][half:]], axis=0)
    return jnp.concatenate([back_queries, back_keys, back_values], axis=1).astype(BF)


def backward_piece(piece, queries, keys_all, values_all, prefix, logsum, back_attended, head_dim):
    score_scale = head_dim ** (-0.5)
    first_row, reach, first_head, end_head = piece
    rows = reach - first_row
    part = (end_head - first_head) * head_dim
    seq_keys = head_rows(keys_all[:reach], first_head, end_head, head_dim)
    seq_values = head_rows(values_all[:reach], first_head, end_head, head_dim)
    query_rows = head_rows(queries[first_row:reach], first_head, end_head, head_dim)
    back_rows = head_rows(back_attended[first_row:reach], first_head, end_head, head_dim)
    allowed = allowed_mask(first_row, rows, reach, prefix[0])
    scores = block_scores(query_rows, seq_keys, allowed, score_scale)
    probabilities = jnp.exp(scores - logsum)
    back_probs = jnp.einsum("qhd,khd->hqk", back_rows, seq_values, preferred_element_type=F32)
    row_dot = jnp.sum(probabilities * back_probs, axis=-1, keepdims=True)
    back_scores = (probabilities * (back_probs - row_dot)).astype(BF)
    back_query = (
        jnp.einsum("hqk,khd->qhd", back_scores, seq_keys, preferred_element_type=F32) * score_scale
    )
    back_key = (
        jnp.einsum("hqk,qhd->khd", back_scores, query_rows, preferred_element_type=F32) * score_scale
    )
    back_value = jnp.einsum(
        "hqk,qhd->khd", probabilities.astype(BF), back_rows, preferred_element_type=F32
    )
    return back_query.reshape(rows, part), back_key.reshape(reach, part), back_value.reshape(reach, part)


def body(
    ring,
    tokens,
    cotangent,
    prefix,
    routes,
    norm1_gain,
    norm1_bias,
    w_query,
    w_key,
    w_value,
    w_out,
    norm2_gain,
    norm2_bias,
    centroids,
    expert_in,
    expert_out,
):
    side = lax.axis_index("tensor")
    own_rows, width = tokens.shape
    all_rows = 2 * own_rows
    head_dim = width // HEADS
    heads_local = w_query.shape[1] // head_dim
    part = w_query.shape[1]
    rows = w_query.shape[0]
    experts, _, hidden = expert_in.shape
    count = ring.count

    def both(own):
        other = swap(own)
        return jnp.where(
            side == 0, jnp.concatenate([own, other], 0), jnp.concatenate([other, own], 0)
        )

    vectors = jnp.concatenate(
        [
            norm1_gain[None],
            norm1_bias[None],
            norm2_gain[None],
            norm2_bias[None],
            centroids,
        ],
        axis=0,
    )
    small_count = vectors.shape[0]
    qkv_block = jnp.concatenate([w_query, w_key, w_value, w_out.T], axis=1)
    in_block = expert_in.transpose(1, 0, 2).reshape(rows, experts * hidden)
    out_block = expert_out.transpose(2, 0, 1).reshape(rows, experts * hidden)
    if count == 16:
        padded = jnp.pad(vectors, ((0, 8 - small_count), (0, 128 - rows // 2)))
        table, qkv_w, other_table = gather_first(padded, qkv_block)
        table, other_table = (t[:, :small_count, : rows // 2] for t in (table, other_table))
        table = jnp.where(
            side == 0,
            jnp.concatenate([table, other_table], 2),
            jnp.concatenate([other_table, table], 2),
        )
        qkv_w = qkv_w.reshape(width, 4 * part)
    else:
        other_vectors = swap(vectors)
        vectors = jnp.where(
            side == 0,
            jnp.concatenate([vectors, other_vectors], 1),
            jnp.concatenate([other_vectors, vectors], 1),
        )
        table = ring.gather(vectors.reshape(1, small_count * rows)).reshape(count, small_count, rows)
        qkv_w = ring.gather(qkv_block)
    table = table.transpose(1, 0, 2).reshape(small_count, width)
    gain_one, bias_one, gain_two, bias_two = (table[i : i + 1] for i in range(4))
    centres = table[4:]

    qkv_w, in_block = lax.optimization_barrier((qkv_w, in_block))
    qkv_w, out_w = qkv_w[:, : 3 * part], qkv_w[:, 3 * part :]
    in_lead = ring.lead(in_block)
    in_crossed = ring.cross(in_lead)
    out_lead = ring.lead(after(out_block, in_lead))
    in_w = ring.close(in_lead, in_crossed)
    out_crossed = ring.cross(after(out_lead, in_w))
    back_w = ring.close(out_lead, out_crossed)

    found = ring.width_order(width)
    to_order = (jnp.arange(width, dtype=jnp.int32)[:, None] == found[None, :]).astype(BF)
    tokens_all = dot(both(tokens), to_order)
    back_all = lax.optimization_barrier(dot(both(cotangent), to_order).astype(BF)).astype(F32)

    normed_one, scale_one = norm_parts(tokens_all)
    first_rows = (normed_one * gain_one + bias_one).astype(BF)
    qkv = dot(first_rows, qkv_w).astype(BF)
    queries, keys_all, values_all = qkv[:, :part], qkv[:, part : 2 * part], qkv[:, 2 * part :]
    attended, logsums = attention_forward(
        queries, keys_all, values_all, prefix, heads_local, head_dim, [(), in_lead, ()]
    )
    attended = after(attended, (in_crossed, out_lead))
    attn_terms = dot_nt(attended, out_w).astype(BF)
    residual = tokens_all + (attn_terms.astype(F32) + swap(attn_terms).astype(F32))
    normed_two, scale_two = norm_parts(residual)
    second_rows = (normed_two * gain_two + bias_two).astype(BF)
    second_wide = second_rows.astype(F32)

    is_last = routes == 1
    ones_before = jnp.tril(jnp.ones((all_rows, all_rows), BF))
    last_before = dot(ones_before, is_last.astype(BF)).astype(jnp.int32)
    position = jnp.arange(all_rows, dtype=jnp.int32)[:, None]
    first_count = all_rows - last_before[all_rows - 1, 0]
    place = jnp.where(is_last, first_count + last_before - 1, position - last_before)
    sort_to = (place == jnp.arange(all_rows, dtype=jnp.int32)[None, :]).astype(BF)
    tail = all_rows - CAP
    in_first = position < first_count

    centre_rows = jnp.where(is_last, centres[1:2], centres[0:1])
    gate = jax.nn.sigmoid(jnp.sum(second_wide * centre_rows, axis=-1, keepdims=True))
    back_branch = (gate * back_all).astype(BF)
    gate, back_branch, sent_rows = lax.optimization_barrier((gate, back_branch, second_rows))
    picked = dot_tn(sort_to, sent_rows).astype(BF)
    back_slots = dot_tn(sort_to, back_branch).astype(BF)
    windows = (slice(0, CAP), slice(tail, all_rows))
    masks = (in_first[:CAP], ~in_first[tail:])
    slot_out, back_picked, grads_in, grads_out = [], [], [], []
    hidden_of = []
    for e in range(2):
        columns = slice(e * hidden, (e + 1) * hidden)
        rows_in = picked[windows[e]]
        back_rows = jnp.where(masks[e], back_slots[windows[e]], jnp.zeros((), BF))
        up = dot(rows_in, in_w[:, columns])
        activated = lax.optimization_barrier(jax.nn.gelu(up).astype(BF))
        grads_out.append(dot_tn(back_rows, activated).astype(BF))
        hidden_of.append((columns, rows_in, back_rows, up, activated))
    grads_out = jnp.concatenate(grads_out, axis=1)
    out_via = ring.far(grads_out, BF)
    for e, (columns, rows_in, back_rows, up, activated) in enumerate(hidden_of):
        if e == 1:
            back_rows = after(back_rows, out_via)
        slot_out.append(dot_nt(activated, back_w[:, columns]).astype(BF))
        back_activated = dot(back_rows, back_w[:, columns])
        back_up = jax.vjp(jax.nn.gelu, up)[1](back_activated)[0].astype(BF)
        grads_in.append(dot_tn(rows_in, back_up).astype(BF))
        back_picked.append(dot_nt(back_up, in_w[:, columns]).astype(BF))
    grads_in = jnp.concatenate(grads_in, axis=1)
    out_near = ring.near(grads_out, out_via, BF)
    in_via = ring.far(after(grads_in, out_via), BF)

    def unsort(pieces):
        joined = jnp.concatenate(
            [
                pieces[0][:tail],
                jnp.where(in_first[tail:CAP], pieces[0][tail:], pieces[1][: CAP - tail]),
                pieces[1][CAP - tail :],
            ],
            axis=0,
        )
        return dot(sort_to, joined).astype(BF)

    row_terms = unsort(slot_out)
    expert_rows = row_terms.astype(F32) + swap(row_terms).astype(F32)
    block_all = (residual + gate * expert_rows).astype(BF)
    first_own = side * own_rows
    block_out = dot_nt(lax.dynamic_slice_in_dim(block_all, first_own, own_rows), to_order).astype(BF)
    back_score = jnp.sum(back_all * expert_rows, axis=-1, keepdims=True) * gate * (1.0 - gate)

    second_terms = unsort(back_picked)
    back_second = second_terms.astype(F32) + swap(second_terms).astype(F32) + back_score * centre_rows
    weighted = back_score * second_wide
    grad_centre = jnp.stack(
        [
            jnp.sum(jnp.where(is_last, 0.0, weighted), axis=0),
            jnp.sum(jnp.where(is_last, weighted, 0.0), axis=0),
        ]
    )
    grad_gain_two = jnp.sum(back_second * normed_two, axis=0)
    grad_bias_two = jnp.sum(back_second, axis=0)
    back_residual = back_all + norm_back(back_second, normed_two, scale_two, gain_two)
    back_out = back_residual.astype(BF)
    grads_out = ring.last(grads_out, out_near, BF)
    in_near = ring.near(grads_in, in_via, BF)
    back_attended = dot(back_out, out_w).astype(BF)
    grad_out = dot_tn(back_out, attended).astype(BF)
    back_qkv = attention_backward(
        queries, keys_all, values_all, prefix, logsums, back_attended, heads_local, head_dim,
        [(), (out_near, in_via), ()],
    )
    back_qkv = after(back_qkv, (in_near, grads_out))
    grads_in = ring.last(grads_in, in_near, BF)
    grad_qkv = dot_tn(first_rows, back_qkv).astype(BF)
    first_terms = dot_nt(back_qkv, qkv_w).astype(BF)
    own_terms = lax.dynamic_slice_in_dim(first_terms, first_own, own_rows)
    other_terms = lax.dynamic_slice_in_dim(first_terms, own_rows - first_own, own_rows)
    back_first = own_terms.astype(F32) + swap(other_terms).astype(F32)

    def mine(value):
        return lax.dynamic_slice_in_dim(value, first_own, own_rows)

    normed_own = mine(normed_one)
    back_norm_one = norm_back(back_first, normed_own, mine(scale_one), gain_one)
    grad_tokens = dot_nt(
        (mine(back_residual) + back_norm_one).astype(BF), to_order
    ).astype(BF)
    one_part = jnp.stack([jnp.sum(back_first * normed_own, axis=0), jnp.sum(back_first, axis=0)])
    one_part = one_part + swap(one_part)
    small = jnp.concatenate(
        [one_part, grad_gain_two[None], grad_bias_two[None], grad_centre], axis=0
    )
    small = small.reshape(small_count, count, rows).transpose(1, 0, 2)
    grad_first = jnp.concatenate([grad_qkv, grad_out], axis=1)
    if count == 16:
        small = jnp.pad(small, ((0, 0), (0, 8 - small_count), (0, 128 - rows)))
        small, grad_first = scatter_last(small, grad_first.reshape(count, rows, 4 * part))
        small = small[:small_count, :rows]
    else:
        grad_first = ring.scatter(grad_first, BF)
        small = ring.scatter(small.reshape(count, small_count * rows), F32).reshape(small_count, rows)
    grad_qkv, grad_out = grad_first[:, : 3 * part], grad_first[:, 3 * part :]
    small = lax.dynamic_slice_in_dim(small, side * (rows // 2), rows // 2, axis=1)
    return (
        block_out,
        grad_tokens,
        small[0],
        small[1],
        grad_qkv[:, :part],
        grad_qkv[:, part : 2 * part],
        grad_qkv[:, 2 * part :],
        grad_out.T,
        small[2],
        small[3],
        small[4:],
        grads_in.reshape(rows, experts, hidden).transpose(1, 0, 2),
        grads_out.reshape(rows, experts, hidden).transpose(1, 2, 0),
    )


def solution(mesh):
    ring = Ring(mesh.shape["dp"])
    both, rows = P(("dp", "tensor")), P(("dp", "tensor"), None)
    columns = P("dp", "tensor")

    def step(*arguments):
        return body(ring, *arguments)

    return jax.shard_map(
        step,
        mesh=mesh,
        in_specs=(
            rows,
            rows,
            P("dp"),
            P("dp", None),
            both,
            both,
            columns,
            columns,
            columns,
            P("tensor", "dp"),
            both,
            both,
            P(None, ("dp", "tensor")),
            P(None, "dp", "tensor"),
            P(None, "tensor", "dp"),
        ),
        out_specs=(
            rows,
            rows,
            both,
            both,
            columns,
            columns,
            columns,
            P("tensor", "dp"),
            both,
            both,
            P(None, ("dp", "tensor")),
            P(None, "dp", "tensor"),
            P(None, "tensor", "dp"),
        ),
        check_vma=False,
    )
```

```python
import functools

import jax
import jax.numpy as jnp
from jax import lax
from jax.experimental import pallas as pl
from jax.experimental.pallas import tpu as pltpu
from jax.sharding import PartitionSpec as P


HEADS = 12
CAP = 640
EPS = 1e-05
NEGATIVE = -1e30
BF = jnp.bfloat16
F32 = jnp.float32
MESH = pl.DeviceIdType.MESH


def factors_of(count):
    rest, sizes = count // 2, []
    while rest % 4 == 0:
        sizes.append(4)
        rest //= 4
    while rest % 2 == 0 and rest > 1:
        sizes.append(2)
        rest //= 2
    return sizes + ([2] if count > 1 else [])


class Ring:
    def __init__(self, count):
        self.count = count
        self.sizes = factors_of(count)
        self.strides = []
        stride = count
        for size in self.sizes:
            stride //= size
            self.strides.append(stride)
        self.square = len(self.sizes) >= 2 and self.sizes[-1] == 2 and self.sizes[-2] == 2

    def order(self, size):
        return [0, 1, 3, 2] if size == 4 else list(range(size))

    def shift(self, stage, step):
        size, stride = self.sizes[stage], self.strides[stage]
        order = self.order(size)
        pairs = []
        for source in range(self.count):
            digit = source // stride % size
            target = order[(order.index(digit) + step) % size]
            pairs.append((source, source + (target - digit) * stride))
        return pairs

    def move(self, value, stage, step):
        return lax.ppermute(value, "dp", self.shift(stage, step))

    def lead(self, block):
        for stage in range(len(self.sizes) - (2 if self.square else 0)):
            parts = [block] + [self.move(block, stage, s) for s in range(1, self.sizes[stage])]
            block = jnp.concatenate(parts, axis=0)
        return lax.optimization_barrier(block)

    def cross(self, block):
        if not self.square:
            return ()
        y, x = len(self.sizes) - 2, len(self.sizes) - 1
        return self.move(block, x, 1), self.move(block, y, 1)

    def close(self, block, crossed):
        if not self.square:
            return block
        y, x = len(self.sizes) - 2, len(self.sizes) - 1
        half = block.shape[0] // 2
        from_x, from_y = crossed
        low, high = self.move(from_y[:half], x, 1), self.move(from_x[half:], y, 1)
        return jnp.concatenate([block, from_y, from_x, low, high], axis=0)

    def gather(self, block):
        block = self.lead(block)
        return self.close(block, self.cross(block))

    def far(self, total, kind):
        if not self.square:
            return ()
        y, x = len(self.sizes) - 2, len(self.sizes) - 1
        quarter = total.shape[0] // 4
        half = quarter // 2
        far = total[3 * quarter :]
        return self.move(far[:half].astype(kind), x, 1), self.move(far[half:].astype(kind), y, 1)

    def near(self, total, via, kind):
        if not self.square:
            return ()
        y, x = len(self.sizes) - 2, len(self.sizes) - 1
        quarter = total.shape[0] // 4
        half = quarter // 2
        via_x, via_y = via
        to_y, to_x = total[quarter : 2 * quarter], total[2 * quarter : 3 * quarter]
        to_y = jnp.concatenate([(to_y[:half].astype(F32) + via_x).astype(kind), to_y[half:].astype(kind)], axis=0)
        to_x = jnp.concatenate([to_x[:half].astype(kind), (to_x[half:].astype(F32) + via_y).astype(kind)], axis=0)
        return self.move(to_x, x, 1), self.move(to_y, y, 1)

    def last(self, total, crossed, kind):
        stages = len(self.sizes)
        if self.square:
            own = total[: total.shape[0] // 4].astype(F32)
            total = own + crossed[0].astype(F32) + crossed[1].astype(F32)
            stages -= 2
        for stage in reversed(range(stages)):
            size = self.sizes[stage]
            piece = total.shape[0] // size
            parts = [total[i * piece : (i + 1) * piece] for i in range(size)]
            total = parts[0].astype(F32)
            for step in range(1, size):
                total = total + self.move(parts[step].astype(kind), stage, size - step).astype(F32)
        return total

    def scatter(self, total, kind):
        return self.last(total, self.near(total, self.far(total, kind), kind), kind)

    def width_order(self, width):
        me = lax.axis_index("dp")
        rows = width // self.count
        column = jnp.arange(width, dtype=jnp.int32)
        inner, block = column % rows, column // rows
        found = jnp.zeros_like(column)
        for size, stride in zip(self.sizes, self.strides):
            step, block = block % size, block // size
            digit = me // stride % size
            if size == 4:
                place = jnp.bitwise_xor(digit, digit // 2)
                back = (place - step + size) % size
                source = jnp.bitwise_xor(back, back // 2)
            else:
                source = (digit - step + size) % size
            found = found + source * stride
        return found * rows + inner


def ring_place(digit):
    return digit + (digit // 2) * (1 - 2 * (digit % 2))


def partners_of(me):
    digit = me // 4
    place = ring_place(digit)
    along = [me + (ring_place((place + step) % 4) - digit) * 4 for step in range(1, 4)]
    return along, me + 1 - 2 * (me % 2), me + 2 - 4 * ((me // 2) % 2)


def greet(along, x_way, y_way, other):
    barrier = pltpu.get_barrier_semaphore()
    for device in along + [x_way, y_way]:
        pl.semaphore_signal(barrier, inc=1, device_id={"dp": device}, device_id_type=MESH)
    pl.semaphore_signal(barrier, inc=1, device_id={"tensor": other}, device_id_type=MESH)
    pl.semaphore_wait(barrier, 6)


def gather_kernel(vec_ref, qkv_ref, vec_out, qkv_out, vec_other, send, recv, local):
    along, x_way, y_way = partners_of(lax.axis_index("dp"))
    other = 1 - lax.axis_index("tensor")
    greet(along, x_way, y_way, other)
    blocks, outs = (vec_ref, qkv_ref), (vec_out, qkv_out)
    copies = {}

    def start(kind, source, slot, device):
        copy = pltpu.make_async_remote_copy(
            src_ref=source,
            dst_ref=outs[kind].at[slot],
            send_sem=send.at[kind, slot],
            recv_sem=recv.at[kind, slot],
            device_id={"dp": device},
            device_id_type=MESH,
        )
        copy.start()
        copies[kind, slot] = copy

    kept = []
    for kind in range(2):
        for step in range(1, 4):
            start(kind, blocks[kind], step, along[step - 1])
        start(kind, blocks[kind], 4, y_way)
        start(kind, blocks[kind], 8, x_way)
        copy = pltpu.make_async_copy(blocks[kind], outs[kind].at[0], local.at[kind])
        copy.start()
        kept.append(copy)
    for step in range(1, 4):
        for kind in range(2):
            copies[kind, step].wait_recv()
            start(kind, outs[kind].at[step], 4 + step, y_way)
            start(kind, outs[kind].at[step], 8 + step, x_way)
        if step == 1:
            for kind in range(2):
                copies[kind, 4].wait_recv()
                start(kind, outs[kind].at[4], 12, x_way)
    for step in range(1, 4):
        for kind in range(2):
            slot = 4 + step if step < 2 else 8 + step
            copies[kind, slot].wait_recv()
            start(kind, outs[kind].at[slot], 12 + step, x_way if step < 2 else y_way)
    waited = (1, 2, 3, 4, 5, 10, 11)
    rest = [slot for slot in range(4, 16) if slot not in waited]
    for slot in rest:
        copies[0, slot].wait_recv()
    kept[0].wait()
    shared = pltpu.make_async_remote_copy(
        src_ref=vec_out,
        dst_ref=vec_other,
        send_sem=send.at[0, 0],
        recv_sem=recv.at[0, 0],
        device_id={"tensor": other},
        device_id_type=MESH,
    )
    shared.start()
    for slot in rest:
        copies[1, slot].wait_recv()
    kept[1].wait()
    for copy in copies.values():
        copy.wait_send()
    shared.wait()


def gather_first(vectors, qkv):
    anywhere = pl.BlockSpec(memory_space=pl.ANY)
    inside = pl.BlockSpec(memory_space=pltpu.VMEM)
    return pl.pallas_call(
        gather_kernel,
        out_shape=(
            jax.ShapeDtypeStruct((16, *vectors.shape), vectors.dtype),
            jax.ShapeDtypeStruct((16, *qkv.shape), qkv.dtype),
            jax.ShapeDtypeStruct((16, *vectors.shape), vectors.dtype),
        ),
        in_specs=[inside, inside],
        out_specs=(anywhere, anywhere, anywhere),
        scratch_shapes=[
            pltpu.SemaphoreType.DMA((2, 16)),
            pltpu.SemaphoreType.DMA((2, 16)),
            pltpu.SemaphoreType.DMA((2,)),
        ],
        compiler_params=pltpu.CompilerParams(collective_id=0, has_side_effects=True),
        name="gather_first",
    )(vectors, qkv)


def scatter_kernel(
    small_ref, grad_ref, small_out, grad_out,
    small_via, small_fold, small_cross, small_sums, small_last,
    grad_via, grad_fold, grad_cross, grad_sums, grad_last,
    send, recv,
):
    along, x_way, y_way = partners_of(lax.axis_index("dp"))
    greet(along, x_way, y_way, 1 - lax.axis_index("tensor"))
    blocks, results = (small_ref, grad_ref), (small_out, grad_out)
    via, fold = (small_via, grad_via), (small_fold, grad_fold)
    cross, sums, last = (small_cross, grad_cross), (small_sums, grad_sums), (small_last, grad_last)
    copies = {}

    def start(kind, source, target, number, device):
        copy = pltpu.make_async_remote_copy(
            src_ref=source,
            dst_ref=target,
            send_sem=send.at[kind, number],
            recv_sem=recv.at[kind, number],
            device_id={"dp": device},
            device_id_type=MESH,
        )
        copy.start()
        copies[kind, number] = copy

    for kind in range(2):
        for step in range(4):
            way = x_way if step < 2 else y_way
            start(kind, blocks[kind].at[12 + step], via[kind].at[step], step, way)
    for kind in range(2):
        for step in range(2):
            start(kind, blocks[kind].at[6 + step], cross[kind].at[2 + step], 6 + step, y_way)
            start(kind, blocks[kind].at[8 + step], cross[kind].at[4 + step], 8 + step, x_way)
    for step in (1, 3, 0, 2):
        for kind in range(2):
            slot = 4 + step if step < 2 else 8 + step
            copies[kind, step].wait_recv()
            folded = blocks[kind][slot].astype(F32) + via[kind][step].astype(F32)
            fold[kind][step] = folded.astype(fold[kind].dtype)
            start(kind, fold[kind].at[step], cross[kind].at[slot - 4], slot, y_way if step < 2 else x_way)
    for step in (3, 1, 2, 0):
        for kind in range(2):
            copies[kind, 4 + step].wait_recv()
            copies[kind, 8 + step].wait_recv()
            total = blocks[kind][step].astype(F32)
            total = total + cross[kind][step].astype(F32) + cross[kind][4 + step].astype(F32)
            if step:
                sums[kind][step] = total.astype(sums[kind].dtype)
                start(kind, sums[kind].at[step], last[kind].at[step], 12 + step, along[3 - step])
            else:
                results[kind][...] = total
    for kind in range(2):
        for step in range(1, 4):
            copies[kind, 12 + step].wait_recv()
            results[kind][...] += last[kind][step].astype(F32)
    for copy in copies.values():
        copy.wait_send()


def scatter_last(small, grads):
    inside = pl.BlockSpec(memory_space=pltpu.VMEM)
    scratch = []
    for value in (small, grads):
        for slots in (4, 4, 8, 4, 4):
            scratch.append(pltpu.VMEM((slots, *value.shape[1:]), value.dtype))
    return pl.pallas_call(
        scatter_kernel,
        out_shape=(
            jax.ShapeDtypeStruct(small.shape[1:], F32),
            jax.ShapeDtypeStruct(grads.shape[1:], F32),
        ),
        in_specs=[inside, inside],
        out_specs=(inside, inside),
        scratch_shapes=scratch
        + [pltpu.SemaphoreType.DMA((2, 16)), pltpu.SemaphoreType.DMA((2, 16))],
        compiler_params=pltpu.CompilerParams(collective_id=1, has_side_effects=True),
        name="scatter_last",
    )(small, grads)


def swap(value):
    return lax.ppermute(value, "tensor", [(0, 1), (1, 0)])


def after(value, earlier):
    return lax.optimization_barrier((value, earlier))[0]


def dot(a, b):
    return lax.dot_general(a, b, (((1,), (0,)), ((), ())), preferred_element_type=F32)


def dot_nt(a, b):
    return lax.dot_general(a, b, (((1,), (1,)), ((), ())), preferred_element_type=F32)


def dot_tn(a, b):
    return lax.dot_general(a, b, (((0,), (0,)), ((), ())), preferred_element_type=F32)


def norm_parts(features):
    average = jnp.mean(features, axis=-1, keepdims=True)
    centered = features - average
    spread = jnp.mean(centered * centered, axis=-1, keepdims=True)
    scale = lax.rsqrt(spread + EPS)
    return centered * scale, scale


def norm_back(grad, normed, scale, gain):
    h = grad * gain
    return scale * (
        h - jnp.mean(h, axis=-1, keepdims=True) - normed * jnp.mean(h * normed, axis=-1, keepdims=True)
    )


STRIP = 256


def strip_scores(keys, queries, first, prefix):
    scores = dot_nt(keys, queries) * (queries.shape[1] ** (-0.5))
    key = lax.broadcasted_iota(jnp.int32, scores.shape, 0)
    query = first + lax.broadcasted_iota(jnp.int32, scores.shape, 1)
    return jnp.where((key <= query) | (key < prefix), scores, NEGATIVE)


def strips(length):
    return [(first, max(length // 2, first + STRIP)) for first in range(0, length, STRIP)]


def attend_kernel(head_dim, prefix_ref, q_ref, k_ref, v_ref, out_ref, lse_ref):
    prefix = prefix_ref[0]
    for head in range(q_ref.shape[1] // head_dim):
        columns = slice(head * head_dim, (head + 1) * head_dim)
        for first, reach in strips(q_ref.shape[0]):
            own = slice(first, first + STRIP)
            scores = strip_scores(k_ref[:reach, columns], q_ref[own, columns], first, prefix)
            top = jnp.max(scores, axis=0, keepdims=True)
            powered = jnp.exp(scores - top)
            total = jnp.sum(powered, axis=0, keepdims=True)
            probabilities = (powered * (1.0 / total)).astype(BF)
            attended = dot_tn(v_ref[:reach, columns], probabilities)
            out_ref[own, columns] = attended.T.astype(BF)
            lse_ref[0, head : head + 1, own] = top + jnp.log(total)


def attend_back_kernel(
    head_dim, prefix_ref, q_ref, k_ref, v_ref, back_ref, lse_ref, out_ref, key_sum, value_sum
):
    prefix = prefix_ref[0]
    score_scale = head_dim ** (-0.5)
    for head in range(q_ref.shape[1] // head_dim):
        columns = slice(head * head_dim, (head + 1) * head_dim)
        for first, reach in reversed(strips(q_ref.shape[0])):
            own = slice(first, first + STRIP)
            keys, queries = k_ref[:reach, columns], q_ref[own, columns]
            back_rows = back_ref[own, columns]
            scores = strip_scores(keys, queries, first, prefix)
            probabilities = jnp.exp(scores - lse_ref[0, head : head + 1, own])
            back_probs = dot_nt(v_ref[:reach, columns], back_rows)
            row_dot = jnp.sum(probabilities * back_probs, axis=0, keepdims=True)
            back_scores = (probabilities * (back_probs - row_dot)).astype(BF)
            out_ref[0, own, columns] = (dot_tn(keys, back_scores) * score_scale).T.astype(BF)
            back_key = dot(back_scores, queries)
            back_value = dot(probabilities.astype(BF), back_rows)
            if reach == q_ref.shape[0]:
                key_sum[...] = back_key
                value_sum[...] = back_value
            else:
                key_sum[:reach, :] += back_key
                value_sum[:reach, :] += back_value
        out_ref[1, :, columns] = (key_sum[...] * score_scale).astype(BF)
        out_ref[2, :, columns] = value_sum[...].astype(BF)


def attend_specs(length, groups):
    joint = [
        pl.BlockSpec((length, 128), lambda i, kind=kind: (0, kind * groups + i)) for kind in range(3)
    ]
    rows = pl.BlockSpec((length, 128), lambda i: (0, i))
    sums = pl.BlockSpec((1, 8, length), lambda i: (i, 0, 0))
    return [pl.BlockSpec(memory_space=pltpu.SMEM)] + joint, rows, sums


def attend(qkv, prefix, head_dim):
    length, part = qkv.shape[0], qkv.shape[1] // 3
    groups = part // 128
    inputs, rows, sums = attend_specs(length, groups)
    work = length * length * part
    return pl.pallas_call(
        functools.partial(attend_kernel, head_dim),
        grid=(groups,),
        out_shape=(
            jax.ShapeDtypeStruct((length, part), BF),
            jax.ShapeDtypeStruct((groups, 8, length), F32),
        ),
        in_specs=inputs,
        out_specs=(rows, sums),
        cost_estimate=pl.CostEstimate(
            flops=4 * work, bytes_accessed=8 * length * part, transcendentals=work // head_dim
        ),
        name="attend",
    )(prefix, qkv, qkv, qkv)


def attend_back(qkv, prefix, back_attended, lse, head_dim):
    length, part = back_attended.shape
    groups = part // 128
    inputs, rows, sums = attend_specs(length, groups)
    work = length * length * part
    return pl.pallas_call(
        functools.partial(attend_back_kernel, head_dim),
        grid=(groups,),
        out_shape=jax.ShapeDtypeStruct((3, length, part), BF),
        in_specs=inputs + [rows, sums],
        out_specs=pl.BlockSpec((3, length, 128), lambda i: (0, 0, i)),
        scratch_shapes=[pltpu.VMEM((length, head_dim), F32), pltpu.VMEM((length, head_dim), F32)],
        cost_estimate=pl.CostEstimate(
            flops=10 * work, bytes_accessed=14 * length * part, transcendentals=work // head_dim
        ),
        name="attend_back",
    )(prefix, qkv, qkv, qkv, back_attended, lse)


def body(
    ring,
    tokens,
    cotangent,
    prefix,
    routes,
    norm1_gain,
    norm1_bias,
    w_query,
    w_key,
    w_value,
    w_out,
    norm2_gain,
    norm2_bias,
    centroids,
    expert_in,
    expert_out,
):
    side = lax.axis_index("tensor")
    own_rows, width = tokens.shape
    all_rows = 2 * own_rows
    head_dim = width // HEADS
    part = w_query.shape[1]
    rows = w_query.shape[0]
    experts, _, hidden = expert_in.shape
    count = ring.count

    def both(own):
        other = swap(own)
        return jnp.where(
            side == 0, jnp.concatenate([own, other], 0), jnp.concatenate([other, own], 0)
        )

    vectors = jnp.concatenate(
        [
            norm1_gain[None],
            norm1_bias[None],
            norm2_gain[None],
            norm2_bias[None],
            centroids,
        ],
        axis=0,
    )
    small_count = vectors.shape[0]
    qkv_block = jnp.concatenate([w_query, w_key, w_value, w_out.T], axis=1)
    in_block = expert_in.transpose(1, 0, 2).reshape(rows, experts * hidden)
    out_block = expert_out.transpose(2, 0, 1).reshape(rows, experts * hidden)
    if count == 16:
        padded = jnp.pad(vectors, ((0, 8 - small_count), (0, 128 - rows // 2)))
        table, qkv_w, other_table = gather_first(padded, qkv_block)
        table, other_table = (t[:, :small_count, : rows // 2] for t in (table, other_table))
        table = jnp.where(
            side == 0,
            jnp.concatenate([table, other_table], 2),
            jnp.concatenate([other_table, table], 2),
        )
        qkv_w = qkv_w.reshape(width, 4 * part)
    else:
        other_vectors = swap(vectors)
        vectors = jnp.where(
            side == 0,
            jnp.concatenate([vectors, other_vectors], 1),
            jnp.concatenate([other_vectors, vectors], 1),
        )
        table = ring.gather(vectors.reshape(1, small_count * rows)).reshape(count, small_count, rows)
        qkv_w = ring.gather(qkv_block)
    table = table.transpose(1, 0, 2).reshape(small_count, width)
    gain_one, bias_one, gain_two, bias_two = (table[i : i + 1] for i in range(4))
    centres = table[4:]

    qkv_w, in_block = lax.optimization_barrier((qkv_w, in_block))
    qkv_w, out_w = qkv_w[:, : 3 * part], qkv_w[:, 3 * part :]
    in_lead = ring.lead(in_block)
    in_crossed = ring.cross(in_lead)
    out_lead = ring.lead(after(out_block, in_lead))
    in_w = ring.close(in_lead, in_crossed)
    out_crossed = ring.cross(after(out_lead, in_w))
    back_w = ring.close(out_lead, out_crossed)

    found = ring.width_order(width)
    to_order = (jnp.arange(width, dtype=jnp.int32)[:, None] == found[None, :]).astype(BF)
    tokens_all = dot(both(tokens), to_order)
    back_all = lax.optimization_barrier(dot(both(cotangent), to_order).astype(BF)).astype(F32)

    normed_one, scale_one = norm_parts(tokens_all)
    first_rows = (normed_one * gain_one + bias_one).astype(BF)
    qkv = dot(first_rows, qkv_w).astype(BF)
    attended, lse = attend(qkv, prefix, head_dim)
    attended = after(attended, in_lead)

    attn_terms = dot_nt(attended, out_w).astype(BF)
    residual = tokens_all + (attn_terms.astype(F32) + swap(attn_terms).astype(F32))
    normed_two, scale_two = norm_parts(residual)
    second_rows = (normed_two * gain_two + bias_two).astype(BF)
    second_wide = second_rows.astype(F32)

    is_last = routes == 1
    ones_before = jnp.tril(jnp.ones((all_rows, all_rows), BF))
    last_before = dot(ones_before, is_last.astype(BF)).astype(jnp.int32)
    position = jnp.arange(all_rows, dtype=jnp.int32)[:, None]
    first_count = all_rows - last_before[all_rows - 1, 0]
    place = jnp.where(is_last, first_count + last_before - 1, position - last_before)
    sort_to = (place == jnp.arange(all_rows, dtype=jnp.int32)[None, :]).astype(BF)
    tail = all_rows - CAP
    in_first = position < first_count

    centre_rows = jnp.where(is_last, centres[1:2], centres[0:1])
    gate = jax.nn.sigmoid(jnp.sum(second_wide * centre_rows, axis=-1, keepdims=True))
    back_branch = (gate * back_all).astype(BF)
    gate, back_branch, sent_rows = lax.optimization_barrier((gate, back_branch, second_rows))
    picked = dot_tn(sort_to, sent_rows).astype(BF)
    back_slots = dot_tn(sort_to, back_branch).astype(BF)
    windows = (slice(0, CAP), slice(tail, all_rows))
    masks = (in_first[:CAP], ~in_first[tail:])
    slot_out, back_picked, grads_in, grads_out = [], [], [], []
    hidden_of = []
    for e in range(2):
        columns = slice(e * hidden, (e + 1) * hidden)
        rows_in = picked[windows[e]]
        back_rows = jnp.where(masks[e], back_slots[windows[e]], jnp.zeros((), BF))
        up = dot(rows_in, in_w[:, columns])
        activated = lax.optimization_barrier(jax.nn.gelu(up).astype(BF))
        grads_out.append(dot_tn(back_rows, activated).astype(BF))
        hidden_of.append((columns, rows_in, back_rows, up, activated))
    grads_out = jnp.concatenate(grads_out, axis=1)
    out_via = ring.far(grads_out, BF)
    for e, (columns, rows_in, back_rows, up, activated) in enumerate(hidden_of):
        if e == 1:
            back_rows = after(back_rows, out_via)
        slot_out.append(dot_nt(activated, back_w[:, columns]).astype(BF))
        back_activated = dot(back_rows, back_w[:, columns])
        back_up = jax.vjp(jax.nn.gelu, up)[1](back_activated)[0].astype(BF)
        grads_in.append(dot_tn(rows_in, back_up).astype(BF))
        back_picked.append(dot_nt(back_up, in_w[:, columns]).astype(BF))
    grads_in = jnp.concatenate(grads_in, axis=1)
    out_near = ring.near(grads_out, out_via, BF)
    in_via = ring.far(after(grads_in, out_via), BF)

    def unsort(pieces):
        joined = jnp.concatenate(
            [
                pieces[0][:tail],
                jnp.where(in_first[tail:CAP], pieces[0][tail:], pieces[1][: CAP - tail]),
                pieces[1][CAP - tail :],
            ],
            axis=0,
        )
        return dot(sort_to, joined).astype(BF)

    row_terms = unsort(slot_out)
    expert_rows = row_terms.astype(F32) + swap(row_terms).astype(F32)
    block_all = (residual + gate * expert_rows).astype(BF)
    first_own = side * own_rows
    block_out = dot_nt(lax.dynamic_slice_in_dim(block_all, first_own, own_rows), to_order).astype(BF)
    back_score = jnp.sum(back_all * expert_rows, axis=-1, keepdims=True) * gate * (1.0 - gate)

    second_terms = unsort(back_picked)
    back_second = second_terms.astype(F32) + swap(second_terms).astype(F32) + back_score * centre_rows
    weighted = back_score * second_wide
    grad_centre = jnp.stack(
        [
            jnp.sum(jnp.where(is_last, 0.0, weighted), axis=0),
            jnp.sum(jnp.where(is_last, weighted, 0.0), axis=0),
        ]
    )
    grad_gain_two = jnp.sum(back_second * normed_two, axis=0)
    grad_bias_two = jnp.sum(back_second, axis=0)
    back_residual = back_all + norm_back(back_second, normed_two, scale_two, gain_two)
    back_out = back_residual.astype(BF)
    grads_out = ring.last(grads_out, out_near, BF)
    in_near = ring.near(grads_in, in_via, BF)
    back_attended = dot(back_out, out_w).astype(BF)
    grad_out = dot_tn(back_out, attended).astype(BF)
    back_qkv = attend_back(qkv, prefix, back_attended, lse, head_dim)
    back_qkv = after(back_qkv, (in_near, grads_out))
    grads_in = ring.last(grads_in, in_near, BF)
    grad_qkv = jnp.concatenate([dot_tn(first_rows, back_qkv[i]).astype(BF) for i in range(3)], axis=1)
    first_terms = sum(dot_nt(back_qkv[i], qkv_w[:, i * part : (i + 1) * part]) for i in range(3))
    first_terms = first_terms.astype(BF)
    own_terms = lax.dynamic_slice_in_dim(first_terms, first_own, own_rows)
    other_terms = lax.dynamic_slice_in_dim(first_terms, own_rows - first_own, own_rows)
    back_first = own_terms.astype(F32) + swap(other_terms).astype(F32)

    def mine(value):
        return lax.dynamic_slice_in_dim(value, first_own, own_rows)

    normed_own = mine(normed_one)
    back_norm_one = norm_back(back_first, normed_own, mine(scale_one), gain_one)
    grad_tokens = dot_nt(
        (mine(back_residual) + back_norm_one).astype(BF), to_order
    ).astype(BF)
    one_part = jnp.stack([jnp.sum(back_first * normed_own, axis=0), jnp.sum(back_first, axis=0)])
    one_part = one_part + swap(one_part)
    small = jnp.concatenate(
        [one_part, grad_gain_two[None], grad_bias_two[None], grad_centre], axis=0
    )
    small = small.reshape(small_count, count, rows).transpose(1, 0, 2)
    grad_first = jnp.concatenate([grad_qkv, grad_out], axis=1)
    if count == 16:
        small = jnp.pad(small, ((0, 0), (0, 8 - small_count), (0, 128 - rows)))
        small, grad_first = scatter_last(small, grad_first.reshape(count, rows, 4 * part))
        small = small[:small_count, :rows]
    else:
        grad_first = ring.scatter(grad_first, BF)
        small = ring.scatter(small.reshape(count, small_count * rows), F32).reshape(small_count, rows)
    grad_qkv, grad_out = grad_first[:, : 3 * part], grad_first[:, 3 * part :]
    small = lax.dynamic_slice_in_dim(small, side * (rows // 2), rows // 2, axis=1)
    return (
        block_out,
        grad_tokens,
        small[0],
        small[1],
        grad_qkv[:, :part],
        grad_qkv[:, part : 2 * part],
        grad_qkv[:, 2 * part :],
        grad_out.T,
        small[2],
        small[3],
        small[4:],
        grads_in.reshape(rows, experts, hidden).transpose(1, 0, 2),
        grads_out.reshape(rows, experts, hidden).transpose(1, 2, 0),
    )


def solution(mesh):
    ring = Ring(mesh.shape["dp"])
    both, rows = P(("dp", "tensor")), P(("dp", "tensor"), None)
    columns = P("dp", "tensor")

    def step(*arguments):
        return body(ring, *arguments)

    return jax.shard_map(
        step,
        mesh=mesh,
        in_specs=(
            rows,
            rows,
            P("dp"),
            P("dp", None),
            both,
            both,
            columns,
            columns,
            columns,
            P("tensor", "dp"),
            both,
            both,
            P(None, ("dp", "tensor")),
            P(None, "dp", "tensor"),
            P(None, "tensor", "dp"),
        ),
        out_specs=(
            rows,
            rows,
            both,
            both,
            columns,
            columns,
            columns,
            P("tensor", "dp"),
            both,
            both,
            P(None, ("dp", "tensor")),
            P(None, "dp", "tensor"),
            P(None, "tensor", "dp"),
        ),
        check_vma=False,
    )
```

```python
import functools

import jax
import jax.numpy as jnp
from jax import lax
from jax.experimental import pallas as pl
from jax.experimental.pallas import tpu as pltpu
from jax.sharding import PartitionSpec as P


HEADS = 12
CAP = 640
EPS = 1e-05
NEGATIVE = -1e30
BF = jnp.bfloat16
F32 = jnp.float32
MESH = pl.DeviceIdType.MESH


def factors_of(count):
    rest, sizes = count // 2, []
    while rest % 4 == 0:
        sizes.append(4)
        rest //= 4
    while rest % 2 == 0 and rest > 1:
        sizes.append(2)
        rest //= 2
    return sizes + ([2] if count > 1 else [])


class Ring:
    def __init__(self, count):
        self.count = count
        self.sizes = factors_of(count)
        self.strides = []
        stride = count
        for size in self.sizes:
            stride //= size
            self.strides.append(stride)
        self.square = len(self.sizes) >= 2 and self.sizes[-1] == 2 and self.sizes[-2] == 2

    def order(self, size):
        return [0, 1, 3, 2] if size == 4 else list(range(size))

    def shift(self, stage, step):
        size, stride = self.sizes[stage], self.strides[stage]
        order = self.order(size)
        pairs = []
        for source in range(self.count):
            digit = source // stride % size
            target = order[(order.index(digit) + step) % size]
            pairs.append((source, source + (target - digit) * stride))
        return pairs

    def move(self, value, stage, step):
        return lax.ppermute(value, "dp", self.shift(stage, step))

    def lead(self, block):
        for stage in range(len(self.sizes) - (2 if self.square else 0)):
            parts = [block] + [self.move(block, stage, s) for s in range(1, self.sizes[stage])]
            block = jnp.concatenate(parts, axis=0)
        return lax.optimization_barrier(block)

    def cross(self, block):
        if not self.square:
            return ()
        y, x = len(self.sizes) - 2, len(self.sizes) - 1
        return self.move(block, x, 1), self.move(block, y, 1)

    def close(self, block, crossed):
        if not self.square:
            return block
        y, x = len(self.sizes) - 2, len(self.sizes) - 1
        half = block.shape[0] // 2
        from_x, from_y = crossed
        low, high = self.move(from_y[:half], x, 1), self.move(from_x[half:], y, 1)
        return jnp.concatenate([block, from_y, from_x, low, high], axis=0)

    def along(self, blocks):
        steps = [blocks] + [self.move(blocks, 0, step) for step in range(1, 4)]
        rows, width = blocks.shape
        joined = jnp.stack([step.reshape(4, rows // 4, width) for step in steps], axis=1)
        return joined.reshape(4 * rows, width)

    def gather(self, block):
        block = self.lead(block)
        return self.close(block, self.cross(block))

    def far(self, total, kind):
        if not self.square:
            return ()
        y, x = len(self.sizes) - 2, len(self.sizes) - 1
        quarter = total.shape[0] // 4
        half = quarter // 2
        far = total[3 * quarter :]
        return self.move(far[:half].astype(kind), x, 1), self.move(far[half:].astype(kind), y, 1)

    def near(self, total, via, kind):
        if not self.square:
            return ()
        y, x = len(self.sizes) - 2, len(self.sizes) - 1
        quarter = total.shape[0] // 4
        half = quarter // 2
        via_x, via_y = via
        to_y, to_x = total[quarter : 2 * quarter], total[2 * quarter : 3 * quarter]
        to_y = jnp.concatenate([(to_y[:half].astype(F32) + via_x).astype(kind), to_y[half:].astype(kind)], axis=0)
        to_x = jnp.concatenate([to_x[:half].astype(kind), (to_x[half:].astype(F32) + via_y).astype(kind)], axis=0)
        return self.move(to_x, x, 1), self.move(to_y, y, 1)

    def last(self, total, crossed, kind):
        stages = len(self.sizes)
        if self.square:
            own = total[: total.shape[0] // 4].astype(F32)
            total = own + crossed[0].astype(F32) + crossed[1].astype(F32)
            stages -= 2
        for stage in reversed(range(stages)):
            size = self.sizes[stage]
            piece = total.shape[0] // size
            parts = [total[i * piece : (i + 1) * piece] for i in range(size)]
            total = parts[0].astype(F32)
            for step in range(1, size):
                total = total + self.move(parts[step].astype(kind), stage, size - step).astype(F32)
        return total

    def scatter(self, total, kind):
        return self.last(total, self.near(total, self.far(total, kind), kind), kind)

    def width_order(self, width):
        me = lax.axis_index("dp")
        rows = width // self.count
        column = jnp.arange(width, dtype=jnp.int32)
        inner, block = column % rows, column // rows
        found = jnp.zeros_like(column)
        for size, stride in zip(self.sizes, self.strides):
            step, block = block % size, block // size
            digit = me // stride % size
            if size == 4:
                place = jnp.bitwise_xor(digit, digit // 2)
                back = (place - step + size) % size
                source = jnp.bitwise_xor(back, back // 2)
            else:
                source = (digit - step + size) % size
            found = found + source * stride
        return found * rows + inner


def ring_place(digit):
    return digit + (digit // 2) * (1 - 2 * (digit % 2))


def partners_of(me):
    digit = me // 4
    place = ring_place(digit)
    along = [me + (ring_place((place + step) % 4) - digit) * 4 for step in range(1, 4)]
    return along, me + 1 - 2 * (me % 2), me + 2 - 4 * ((me // 2) % 2)


def greet(along, x_way, y_way):
    barrier = pltpu.get_barrier_semaphore()
    for device in along + [x_way, y_way]:
        pl.semaphore_signal(barrier, inc=1, device_id={"dp": device}, device_id_type=MESH)
    pl.semaphore_wait(barrier, 5)


CHUNK = 16


def gather_kernel(block_ref, out_ref, send, recv, local):
    along, x_way, y_way = partners_of(lax.axis_index("dp"))
    greet(along, x_way, y_way)
    chunks = block_ref.shape[0] // CHUNK
    copies = {}

    def own(chunk):
        return block_ref.at[pl.ds(chunk * CHUNK, CHUNK)]

    def slot_of(chunk, slot):
        return out_ref.at[slot, pl.ds(chunk * CHUNK, CHUNK)]

    def start(chunk, source, slot, device):
        copy = pltpu.make_async_remote_copy(
            src_ref=source,
            dst_ref=slot_of(chunk, slot),
            send_sem=send.at[chunk, slot],
            recv_sem=recv.at[chunk, slot],
            device_id={"dp": device},
            device_id_type=MESH,
        )
        copy.start()
        copies[chunk, slot] = copy

    def pass_far(chunk):
        for step in range(4):
            slot = 4 + step if step < 2 else 8 + step
            copies[chunk, slot].wait_recv()
            start(chunk, slot_of(chunk, slot), 12 + step, x_way if step < 2 else y_way)

    for chunk in range(chunks):
        for step in range(1, 4):
            start(chunk, own(chunk), step, along[step - 1])
        start(chunk, own(chunk), 4, y_way)
        start(chunk, own(chunk), 8, x_way)
    kept = pltpu.make_async_copy(block_ref, out_ref.at[0], local)
    kept.start()
    for chunk in range(chunks):
        for step in range(1, 4):
            copies[chunk, step].wait_recv()
            start(chunk, slot_of(chunk, step), 4 + step, y_way)
            start(chunk, slot_of(chunk, step), 8 + step, x_way)
        if chunk:
            pass_far(chunk - 1)
    pass_far(chunks - 1)
    for chunk in range(chunks):
        for slot in (6, 7, 8, 9, 12, 13, 14, 15):
            copies[chunk, slot].wait_recv()
    kept.wait()
    for copy in copies.values():
        copy.wait_send()


def gather_first(block):
    chunks = block.shape[0] // CHUNK
    return pl.pallas_call(
        gather_kernel,
        out_shape=jax.ShapeDtypeStruct((16, *block.shape), block.dtype),
        in_specs=[pl.BlockSpec(memory_space=pltpu.VMEM)],
        out_specs=pl.BlockSpec(memory_space=pl.ANY),
        scratch_shapes=[
            pltpu.SemaphoreType.DMA((chunks, 16)),
            pltpu.SemaphoreType.DMA((chunks, 16)),
            pltpu.SemaphoreType.DMA,
        ],
        compiler_params=pltpu.CompilerParams(collective_id=0, has_side_effects=True),
        name="gather_first",
    )(block)


def three_parts(values):
    parts = []
    for _ in range(3):
        part = lax.reduce_precision(values, 8, 7)
        parts.append(part.astype(BF))
        values = values - part
    return jnp.stack(parts)


def scatter_kernel(blocks, out_ref, via, fold, cross, sums, last, send, recv):
    along, x_way, y_way = partners_of(lax.axis_index("dp"))
    greet(along, x_way, y_way)
    chunks = out_ref.shape[0] // CHUNK
    copies = {}

    def at(buffer, chunk, slot):
        return buffer.at[slot, pl.ds(chunk * CHUNK, CHUNK)]

    def wide(buffer, chunk, slot):
        return at(buffer, chunk, slot)[...].astype(F32)

    def result(chunk):
        return out_ref.at[pl.ds(chunk * CHUNK, CHUNK)]

    def start(chunk, source, target, number, device):
        copy = pltpu.make_async_remote_copy(
            src_ref=source,
            dst_ref=target,
            send_sem=send.at[chunk, number],
            recv_sem=recv.at[chunk, number],
            device_id={"dp": device},
            device_id_type=MESH,
        )
        copy.start()
        copies[chunk, number] = copy

    def close(chunk):
        for step in (3, 1, 2, 0):
            copies[chunk, 4 + step].wait_recv()
            copies[chunk, 8 + step].wait_recv()
            total = wide(blocks, chunk, step) + wide(cross, chunk, step) + wide(cross, chunk, 4 + step)
            if step:
                source = at(sums, chunk, step)
                source[...] = total.astype(source.dtype)
                start(chunk, source, at(last, chunk, step), 12 + step, along[3 - step])
            else:
                result(chunk)[...] = total

    for chunk in range(chunks):
        for step in range(4):
            way = x_way if step < 2 else y_way
            start(chunk, at(blocks, chunk, 12 + step), at(via, chunk, step), step, way)
        for step in range(2):
            start(chunk, at(blocks, chunk, 6 + step), at(cross, chunk, 2 + step), 6 + step, y_way)
            start(chunk, at(blocks, chunk, 8 + step), at(cross, chunk, 4 + step), 8 + step, x_way)
    for chunk in range(chunks):
        for step in (1, 3, 0, 2):
            slot = 4 + step if step < 2 else 8 + step
            copies[chunk, step].wait_recv()
            source = at(fold, chunk, step)
            source[...] = (wide(blocks, chunk, slot) + wide(via, chunk, step)).astype(source.dtype)
            start(chunk, source, at(cross, chunk, slot - 4), slot, y_way if step < 2 else x_way)
        if chunk:
            close(chunk - 1)
    close(chunks - 1)
    for chunk in range(chunks):
        for step in range(1, 4):
            copies[chunk, 12 + step].wait_recv()
            result(chunk)[...] += wide(last, chunk, step)
    for copy in copies.values():
        copy.wait_send()


def scatter_last(grads):
    inside = pl.BlockSpec(memory_space=pltpu.VMEM)
    return pl.pallas_call(
        scatter_kernel,
        out_shape=jax.ShapeDtypeStruct(grads.shape[1:], F32),
        in_specs=[inside],
        out_specs=inside,
        scratch_shapes=[pltpu.VMEM((slots, *grads.shape[1:]), grads.dtype) for slots in (4, 4, 8, 4, 4)]
        + [pltpu.SemaphoreType.DMA((grads.shape[1] // CHUNK, 16))] * 2,
        compiler_params=pltpu.CompilerParams(collective_id=1, has_side_effects=True),
        name="scatter_last",
    )(grads)


def swap(value):
    return lax.ppermute(value, "tensor", [(0, 1), (1, 0)])


def after(value, earlier):
    return lax.optimization_barrier((value, earlier))[0]


def dot(a, b):
    return lax.dot_general(a, b, (((1,), (0,)), ((), ())), preferred_element_type=F32)


def dot_nt(a, b):
    return lax.dot_general(a, b, (((1,), (1,)), ((), ())), preferred_element_type=F32)


def dot_tn(a, b):
    return lax.dot_general(a, b, (((0,), (0,)), ((), ())), preferred_element_type=F32)


def norm_parts(features):
    average = jnp.mean(features, axis=-1, keepdims=True)
    centered = features - average
    spread = jnp.mean(centered * centered, axis=-1, keepdims=True)
    scale = lax.rsqrt(spread + EPS)
    return centered * scale, scale


def norm_back(grad, normed, scale, gain):
    h = grad * gain
    return scale * (
        h - jnp.mean(h, axis=-1, keepdims=True) - normed * jnp.mean(h * normed, axis=-1, keepdims=True)
    )


STRIP = 256


def strip_scores(keys, queries, first, prefix):
    scores = dot_nt(keys, queries) * (queries.shape[1] ** (-0.5))
    key = lax.broadcasted_iota(jnp.int32, scores.shape, 0)
    query = first + lax.broadcasted_iota(jnp.int32, scores.shape, 1)
    return jnp.where((key <= query) | (key < prefix), scores, NEGATIVE)


def strips(length):
    return [(first, max(length // 2, first + STRIP)) for first in range(0, length, STRIP)]


def attend_kernel(head_dim, prefix_ref, q_ref, k_ref, v_ref, out_ref, lse_ref):
    prefix = prefix_ref[0]
    for head in range(q_ref.shape[1] // head_dim):
        columns = slice(head * head_dim, (head + 1) * head_dim)
        for first, reach in strips(q_ref.shape[0]):
            own = slice(first, first + STRIP)
            scores = strip_scores(k_ref[:reach, columns], q_ref[own, columns], first, prefix)
            top = jnp.max(scores, axis=0, keepdims=True)
            powered = jnp.exp(scores - top)
            total = jnp.sum(powered, axis=0, keepdims=True)
            probabilities = (powered * (1.0 / total)).astype(BF)
            attended = dot_tn(v_ref[:reach, columns], probabilities)
            out_ref[own, columns] = attended.T.astype(BF)
            lse_ref[0, head : head + 1, own] = top + jnp.log(total)


def attend_back_kernel(
    head_dim, prefix_ref, q_ref, k_ref, v_ref, back_ref, lse_ref, out_ref, key_sum, value_sum
):
    prefix = prefix_ref[0]
    score_scale = head_dim ** (-0.5)
    for head in range(q_ref.shape[1] // head_dim):
        columns = slice(head * head_dim, (head + 1) * head_dim)
        for first, reach in reversed(strips(q_ref.shape[0])):
            own = slice(first, first + STRIP)
            keys, queries = k_ref[:reach, columns], q_ref[own, columns]
            back_rows = back_ref[own, columns]
            scores = strip_scores(keys, queries, first, prefix)
            probabilities = jnp.exp(scores - lse_ref[0, head : head + 1, own])
            back_probs = dot_nt(v_ref[:reach, columns], back_rows)
            row_dot = jnp.sum(probabilities * back_probs, axis=0, keepdims=True)
            back_scores = (probabilities * (back_probs - row_dot)).astype(BF)
            out_ref[0, own, columns] = (dot_tn(keys, back_scores) * score_scale).T.astype(BF)
            back_key = dot(back_scores, queries)
            back_value = dot(probabilities.astype(BF), back_rows)
            if reach == q_ref.shape[0]:
                key_sum[...] = back_key
                value_sum[...] = back_value
            else:
                key_sum[:reach, :] += back_key
                value_sum[:reach, :] += back_value
        out_ref[1, :, columns] = (key_sum[...] * score_scale).astype(BF)
        out_ref[2, :, columns] = value_sum[...].astype(BF)


def attend_specs(length, groups):
    joint = [
        pl.BlockSpec((length, 128), lambda i, kind=kind: (0, kind * groups + i)) for kind in range(3)
    ]
    rows = pl.BlockSpec((length, 128), lambda i: (0, i))
    sums = pl.BlockSpec((1, 8, length), lambda i: (i, 0, 0))
    return [pl.BlockSpec(memory_space=pltpu.SMEM)] + joint, rows, sums


def attend(qkv, prefix, head_dim):
    length, part = qkv.shape[0], qkv.shape[1] // 3
    groups = part // 128
    inputs, rows, sums = attend_specs(length, groups)
    work = length * length * part
    return pl.pallas_call(
        functools.partial(attend_kernel, head_dim),
        grid=(groups,),
        out_shape=(
            jax.ShapeDtypeStruct((length, part), BF),
            jax.ShapeDtypeStruct((groups, 8, length), F32),
        ),
        in_specs=inputs,
        out_specs=(rows, sums),
        cost_estimate=pl.CostEstimate(
            flops=4 * work, bytes_accessed=8 * length * part, transcendentals=work // head_dim
        ),
        name="attend",
    )(prefix, qkv, qkv, qkv)


def attend_back(qkv, prefix, back_attended, lse, head_dim):
    length, part = back_attended.shape
    groups = part // 128
    inputs, rows, sums = attend_specs(length, groups)
    work = length * length * part
    return pl.pallas_call(
        functools.partial(attend_back_kernel, head_dim),
        grid=(groups,),
        out_shape=jax.ShapeDtypeStruct((3, length, part), BF),
        in_specs=inputs + [rows, sums],
        out_specs=pl.BlockSpec((3, length, 128), lambda i: (0, 0, i)),
        scratch_shapes=[pltpu.VMEM((length, head_dim), F32), pltpu.VMEM((length, head_dim), F32)],
        cost_estimate=pl.CostEstimate(
            flops=10 * work, bytes_accessed=14 * length * part, transcendentals=work // head_dim
        ),
        name="attend_back",
    )(prefix, qkv, qkv, qkv, back_attended, lse)


def body(
    ring,
    tokens,
    cotangent,
    prefix,
    routes,
    norm1_gain,
    norm1_bias,
    w_query,
    w_key,
    w_value,
    w_out,
    norm2_gain,
    norm2_bias,
    centroids,
    expert_in,
    expert_out,
):
    side = lax.axis_index("tensor")
    own_rows, width = tokens.shape
    all_rows = 2 * own_rows
    head_dim = width // HEADS
    part = w_query.shape[1]
    rows = w_query.shape[0]
    experts, _, hidden = expert_in.shape
    count = ring.count

    def both(own):
        other = swap(own)
        return jnp.where(
            side == 0, jnp.concatenate([own, other], 0), jnp.concatenate([other, own], 0)
        )

    vectors = jnp.concatenate(
        [
            norm1_gain[None],
            norm1_bias[None],
            norm2_gain[None],
            norm2_bias[None],
            centroids,
        ],
        axis=0,
    )
    small_count = vectors.shape[0]
    qkv_block = jnp.concatenate([w_query, w_key, w_value, w_out.T], axis=1)
    in_block = expert_in.transpose(1, 0, 2).reshape(rows, experts * hidden)
    out_blocks = expert_out.transpose(2, 0, 1)
    out_block, turned_block = out_blocks[:, 0], out_blocks[:, 1]
    if count == 16:
        small_width = 3 * small_count * (rows // 2) // rows
        extra = three_parts(vectors).reshape(rows, small_width)
        extra = jnp.pad(extra, ((0, 0), (0, 128 - small_width)))
        gathered = gather_first(jnp.concatenate([qkv_block, extra], axis=1))
        parts = gathered[:, :, 4 * part : 4 * part + small_width].astype(F32)
        parts = parts.reshape(count, 3, small_count, rows // 2)
        table = (parts[:, 0] + parts[:, 1]) + parts[:, 2]
        other_table = swap(table.reshape(count, -1)).reshape(table.shape)
        table = jnp.where(
            side == 0,
            jnp.concatenate([table, other_table], 2),
            jnp.concatenate([other_table, table], 2),
        )
        qkv_w = gathered.reshape(width, 4 * part + 128)
    else:
        other_vectors = swap(vectors)
        vectors = jnp.where(
            side == 0,
            jnp.concatenate([vectors, other_vectors], 1),
            jnp.concatenate([other_vectors, vectors], 1),
        )
        table = ring.gather(vectors.reshape(1, small_count * rows)).reshape(count, small_count, rows)
        qkv_w = ring.gather(qkv_block)
    table = table.transpose(1, 0, 2).reshape(small_count, width)
    gain_one, bias_one, gain_two, bias_two = (table[i : i + 1] for i in range(4))
    centres = table[4:]

    qkv_w, in_block, turned_block = lax.optimization_barrier((qkv_w, in_block, turned_block))
    qkv_w, out_w = qkv_w[:, : 3 * part], qkv_w[:, 3 * part : 4 * part]
    in_lead = ring.lead(in_block)
    if count == 16:
        turned_crossed = ring.cross(turned_block)
        turned_square = ring.close(turned_block, turned_crossed)
        in_lead, turned_square = lax.optimization_barrier((in_lead, turned_square))
        turned_w = ring.along(turned_square)
    else:
        turned_w = ring.gather(turned_block)
    in_crossed = ring.cross(in_lead)
    out_lead = ring.lead(after(out_block, in_lead))
    in_w = ring.close(in_lead, in_crossed)
    out_crossed = ring.cross(after(out_lead, in_w))
    back_ws = (ring.close(out_lead, out_crossed), turned_w)

    found = ring.width_order(width)
    to_order = (jnp.arange(width, dtype=jnp.int32)[:, None] == found[None, :]).astype(BF)
    tokens_all = dot(both(tokens), to_order)
    back_all = lax.optimization_barrier(dot(both(cotangent), to_order).astype(BF)).astype(F32)

    normed_one, scale_one = norm_parts(tokens_all)
    first_rows = (normed_one * gain_one + bias_one).astype(BF)
    qkv = dot(first_rows, qkv_w).astype(BF)
    attended, lse = attend(qkv, prefix, head_dim)
    attended = after(attended, in_lead)

    attn_terms = dot_nt(attended, out_w).astype(BF)
    residual = tokens_all + (attn_terms.astype(F32) + swap(attn_terms).astype(F32))
    normed_two, scale_two = norm_parts(residual)
    second_rows = (normed_two * gain_two + bias_two).astype(BF)
    second_wide = second_rows.astype(F32)

    is_last = routes == 1
    ones_before = jnp.tril(jnp.ones((all_rows, all_rows), BF))
    last_before = dot(ones_before, is_last.astype(BF)).astype(jnp.int32)
    position = jnp.arange(all_rows, dtype=jnp.int32)[:, None]
    first_count = all_rows - last_before[all_rows - 1, 0]
    place = jnp.where(is_last, first_count + last_before - 1, position - last_before)
    sort_to = (place == jnp.arange(all_rows, dtype=jnp.int32)[None, :]).astype(BF)
    tail = all_rows - CAP
    in_first = position < first_count

    centre_rows = jnp.where(is_last, centres[1:2], centres[0:1])
    gate = jax.nn.sigmoid(jnp.sum(second_wide * centre_rows, axis=-1, keepdims=True))
    back_branch = (gate * back_all).astype(BF)
    gate, back_branch, sent_rows = lax.optimization_barrier((gate, back_branch, second_rows))
    picked = dot_tn(sort_to, sent_rows).astype(BF)
    back_slots = dot_tn(sort_to, back_branch).astype(BF)
    windows = (slice(0, CAP), slice(tail, all_rows))
    masks = (in_first[:CAP], ~in_first[tail:])
    slot_out, back_picked, grads_in, grads_out = [], [], [], []
    hidden_of = []
    for e in range(2):
        columns = slice(e * hidden, (e + 1) * hidden)
        rows_in = picked[windows[e]]
        back_rows = jnp.where(masks[e], back_slots[windows[e]], jnp.zeros((), BF))
        up = dot(rows_in, in_w[:, columns])
        activated = lax.optimization_barrier(jax.nn.gelu(up).astype(BF))
        grads_out.append(dot_tn(back_rows, activated).astype(BF))
        hidden_of.append((columns, rows_in, back_rows, up, activated))
    grads_out = jnp.concatenate(grads_out, axis=1)
    out_via = ring.far(grads_out, BF)
    for e, (columns, rows_in, back_rows, up, activated) in enumerate(hidden_of):
        if e == 1:
            back_rows = after(back_rows, out_via)
        slot_out.append(dot_nt(activated, back_ws[e]).astype(BF))
        back_activated = dot(back_rows, back_ws[e])
        back_up = jax.vjp(jax.nn.gelu, up)[1](back_activated)[0].astype(BF)
        grads_in.append(dot_tn(rows_in, back_up).astype(BF))
        back_picked.append(dot_nt(back_up, in_w[:, columns]).astype(BF))
    grads_in = jnp.concatenate(grads_in, axis=1)
    out_near = ring.near(grads_out, out_via, BF)
    in_via = ring.far(after(grads_in, out_via), BF)

    def unsort(pieces):
        joined = jnp.concatenate(
            [
                pieces[0][:tail],
                jnp.where(in_first[tail:CAP], pieces[0][tail:], pieces[1][: CAP - tail]),
                pieces[1][CAP - tail :],
            ],
            axis=0,
        )
        return dot(sort_to, joined).astype(BF)

    row_terms = unsort(slot_out)
    expert_rows = row_terms.astype(F32) + swap(row_terms).astype(F32)
    block_all = (residual + gate * expert_rows).astype(BF)
    first_own = side * own_rows
    block_out = dot_nt(lax.dynamic_slice_in_dim(block_all, first_own, own_rows), to_order).astype(BF)
    back_score = jnp.sum(back_all * expert_rows, axis=-1, keepdims=True) * gate * (1.0 - gate)

    second_terms = unsort(back_picked)
    back_second = second_terms.astype(F32) + swap(second_terms).astype(F32) + back_score * centre_rows
    weighted = back_score * second_wide
    grad_centre = jnp.stack(
        [
            jnp.sum(jnp.where(is_last, 0.0, weighted), axis=0),
            jnp.sum(jnp.where(is_last, weighted, 0.0), axis=0),
        ]
    )
    grad_gain_two = jnp.sum(back_second * normed_two, axis=0)
    grad_bias_two = jnp.sum(back_second, axis=0)
    back_residual = back_all + norm_back(back_second, normed_two, scale_two, gain_two)
    back_out = back_residual.astype(BF)
    grads_out = ring.last(grads_out, out_near, BF)
    in_near = ring.near(grads_in, in_via, BF)
    back_attended = dot(back_out, out_w).astype(BF)
    grad_out = dot_tn(back_out, attended).astype(BF)
    back_qkv = attend_back(qkv, prefix, back_attended, lse, head_dim)
    back_qkv = after(back_qkv, (in_near, grads_out))
    grads_in = ring.last(grads_in, in_near, BF)
    grad_qkv = jnp.concatenate([dot_tn(first_rows, back_qkv[i]).astype(BF) for i in range(3)], axis=1)
    first_terms = sum(dot_nt(back_qkv[i], qkv_w[:, i * part : (i + 1) * part]) for i in range(3))
    first_terms = first_terms.astype(BF)
    own_terms = lax.dynamic_slice_in_dim(first_terms, first_own, own_rows)
    other_terms = lax.dynamic_slice_in_dim(first_terms, own_rows - first_own, own_rows)
    back_first = own_terms.astype(F32) + swap(other_terms).astype(F32)

    def mine(value):
        return lax.dynamic_slice_in_dim(value, first_own, own_rows)

    normed_own = mine(normed_one)
    back_norm_one = norm_back(back_first, normed_own, mine(scale_one), gain_one)
    grad_tokens = dot_nt(
        (mine(back_residual) + back_norm_one).astype(BF), to_order
    ).astype(BF)
    one_part = jnp.stack([jnp.sum(back_first * normed_own, axis=0), jnp.sum(back_first, axis=0)])
    one_part = one_part + swap(one_part)
    small = jnp.concatenate(
        [one_part, grad_gain_two[None], grad_bias_two[None], grad_centre], axis=0
    )
    if count == 16:
        extra = jnp.pad(small.T.astype(BF), ((0, 0), (0, 128 - small_count)))
        grad_first = jnp.concatenate([grad_qkv, grad_out, extra], axis=1)
        grad_first = scatter_last(grad_first.reshape(count, rows, 4 * part + 128))
        small = grad_first[:, 4 * part : 4 * part + small_count].T
        grad_first = grad_first[:, : 4 * part]
    else:
        small = small.reshape(small_count, count, rows).transpose(1, 0, 2)
        grad_first = ring.scatter(jnp.concatenate([grad_qkv, grad_out], axis=1), BF)
        small = ring.scatter(small.reshape(count, small_count * rows), F32).reshape(small_count, rows)
    grad_qkv, grad_out = grad_first[:, : 3 * part], grad_first[:, 3 * part :]
    small = lax.dynamic_slice_in_dim(small, side * (rows // 2), rows // 2, axis=1)
    return (
        block_out,
        grad_tokens,
        small[0],
        small[1],
        grad_qkv[:, :part],
        grad_qkv[:, part : 2 * part],
        grad_qkv[:, 2 * part :],
        grad_out.T,
        small[2],
        small[3],
        small[4:],
        grads_in.reshape(rows, experts, hidden).transpose(1, 0, 2),
        grads_out.reshape(rows, experts, hidden).transpose(1, 2, 0),
    )


def solution(mesh):
    ring = Ring(mesh.shape["dp"])
    both, rows = P(("dp", "tensor")), P(("dp", "tensor"), None)
    columns = P("dp", "tensor")

    def step(*arguments):
        return body(ring, *arguments)

    return jax.shard_map(
        step,
        mesh=mesh,
        in_specs=(
            rows,
            rows,
            P("dp"),
            P("dp", None),
            both,
            both,
            columns,
            columns,
            columns,
            P("tensor", "dp"),
            both,
            both,
            P(None, ("dp", "tensor")),
            P(None, "dp", "tensor"),
            P(None, "tensor", "dp"),
        ),
        out_specs=(
            rows,
            rows,
            both,
            both,
            columns,
            columns,
            columns,
            P("tensor", "dp"),
            both,
            both,
            P(None, ("dp", "tensor")),
            P(None, "dp", "tensor"),
            P(None, "tensor", "dp"),
        ),
        check_vma=False,
    )
```

```python
import functools

import jax
import jax.numpy as jnp
from jax import lax
from jax.experimental import pallas as pl
from jax.experimental.pallas import tpu as pltpu
from jax.sharding import PartitionSpec as P


HEADS = 12
CAP = 640
EPS = 1e-05
NEGATIVE = -1e30
BF = jnp.bfloat16
F32 = jnp.float32
MESH = pl.DeviceIdType.MESH


def factors_of(count):
    rest, sizes = count // 2, []
    while rest % 4 == 0:
        sizes.append(4)
        rest //= 4
    while rest % 2 == 0 and rest > 1:
        sizes.append(2)
        rest //= 2
    return sizes + ([2] if count > 1 else [])


class Ring:
    def __init__(self, count):
        self.count = count
        self.sizes = factors_of(count)
        self.strides = []
        stride = count
        for size in self.sizes:
            stride //= size
            self.strides.append(stride)
        self.square = len(self.sizes) >= 2 and self.sizes[-1] == 2 and self.sizes[-2] == 2

    def order(self, size):
        return [0, 1, 3, 2] if size == 4 else list(range(size))

    def shift(self, stage, step):
        size, stride = self.sizes[stage], self.strides[stage]
        order = self.order(size)
        pairs = []
        for source in range(self.count):
            digit = source // stride % size
            target = order[(order.index(digit) + step) % size]
            pairs.append((source, source + (target - digit) * stride))
        return pairs

    def move(self, value, stage, step):
        return lax.ppermute(value, "dp", self.shift(stage, step))

    def lead(self, block):
        for stage in range(len(self.sizes) - (2 if self.square else 0)):
            parts = [block] + [self.move(block, stage, s) for s in range(1, self.sizes[stage])]
            block = jnp.concatenate(parts, axis=0)
        return lax.optimization_barrier(block)

    def cross(self, block):
        if not self.square:
            return ()
        y, x = len(self.sizes) - 2, len(self.sizes) - 1
        return self.move(block, x, 1), self.move(block, y, 1)

    def close(self, block, crossed):
        if not self.square:
            return block
        y, x = len(self.sizes) - 2, len(self.sizes) - 1
        half = block.shape[0] // 2
        from_x, from_y = crossed
        low, high = self.move(from_y[:half], x, 1), self.move(from_x[half:], y, 1)
        return jnp.concatenate([block, from_y, from_x, low, high], axis=0)

    def along(self, blocks):
        steps = [blocks] + [self.move(blocks, 0, step) for step in range(1, 4)]
        rows, width = blocks.shape
        joined = jnp.stack([step.reshape(4, rows // 4, width) for step in steps], axis=1)
        return joined.reshape(4 * rows, width)

    def gather(self, block):
        block = self.lead(block)
        return self.close(block, self.cross(block))

    def far(self, total, kind):
        if not self.square:
            return ()
        y, x = len(self.sizes) - 2, len(self.sizes) - 1
        quarter = total.shape[0] // 4
        half = quarter // 2
        far = total[3 * quarter :]
        return self.move(far[:half].astype(kind), x, 1), self.move(far[half:].astype(kind), y, 1)

    def near(self, total, via, kind):
        if not self.square:
            return ()
        y, x = len(self.sizes) - 2, len(self.sizes) - 1
        quarter = total.shape[0] // 4
        half = quarter // 2
        via_x, via_y = via
        to_y, to_x = total[quarter : 2 * quarter], total[2 * quarter : 3 * quarter]
        to_y = jnp.concatenate([(to_y[:half].astype(F32) + via_x).astype(kind), to_y[half:].astype(kind)], axis=0)
        to_x = jnp.concatenate([to_x[:half].astype(kind), (to_x[half:].astype(F32) + via_y).astype(kind)], axis=0)
        return self.move(to_x, x, 1), self.move(to_y, y, 1)

    def last(self, total, crossed, kind):
        stages = len(self.sizes)
        if self.square:
            own = total[: total.shape[0] // 4].astype(F32)
            total = own + crossed[0].astype(F32) + crossed[1].astype(F32)
            stages -= 2
        for stage in reversed(range(stages)):
            size = self.sizes[stage]
            piece = total.shape[0] // size
            parts = [total[i * piece : (i + 1) * piece] for i in range(size)]
            total = parts[0].astype(F32)
            for step in range(1, size):
                total = total + self.move(parts[step].astype(kind), stage, size - step).astype(F32)
        return total

    def scatter(self, total, kind):
        return self.last(total, self.near(total, self.far(total, kind), kind), kind)

    def width_order(self, width):
        me = lax.axis_index("dp")
        rows = width // self.count
        column = jnp.arange(width, dtype=jnp.int32)
        inner, block = column % rows, column // rows
        found = jnp.zeros_like(column)
        for size, stride in zip(self.sizes, self.strides):
            step, block = block % size, block // size
            digit = me // stride % size
            if size == 4:
                place = jnp.bitwise_xor(digit, digit // 2)
                back = (place - step + size) % size
                source = jnp.bitwise_xor(back, back // 2)
            else:
                source = (digit - step + size) % size
            found = found + source * stride
        return found * rows + inner


def ring_place(digit):
    return digit + (digit // 2) * (1 - 2 * (digit % 2))


def partners_of(me):
    digit = me // 4
    place = ring_place(digit)
    along = [me + (ring_place((place + step) % 4) - digit) * 4 for step in range(1, 4)]
    return along, me + 1 - 2 * (me % 2), me + 2 - 4 * ((me // 2) % 2)


def greet(along, x_way, y_way, other):
    barrier = pltpu.get_barrier_semaphore()
    for device in along + [x_way, y_way]:
        pl.semaphore_signal(barrier, inc=1, device_id={"dp": device}, device_id_type=MESH)
    pl.semaphore_signal(barrier, inc=1, device_id={"tensor": other}, device_id_type=MESH)
    pl.semaphore_wait(barrier, 6)


CHUNK = 16


def gather_kernel(vec_ref, qkv_ref, vec_out, qkv_out, vec_other, send, recv, local):
    along, x_way, y_way = partners_of(lax.axis_index("dp"))
    other = 1 - lax.axis_index("tensor")
    greet(along, x_way, y_way, other)
    kinds = 1 + qkv_ref.shape[0] // CHUNK
    copies = {}

    def own(kind):
        return qkv_ref.at[pl.ds((kind - 1) * CHUNK, CHUNK)] if kind else vec_ref

    def slot_of(kind, slot):
        return qkv_out.at[slot, pl.ds((kind - 1) * CHUNK, CHUNK)] if kind else vec_out.at[slot]

    def start(kind, source, slot, device):
        copy = pltpu.make_async_remote_copy(
            src_ref=source,
            dst_ref=slot_of(kind, slot),
            send_sem=send.at[kind, slot],
            recv_sem=recv.at[kind, slot],
            device_id={"dp": device},
            device_id_type=MESH,
        )
        copy.start()
        copies[kind, slot] = copy

    def pass_far(kind):
        for step in range(4):
            slot = 4 + step if step < 2 else 8 + step
            copies[kind, slot].wait_recv()
            start(kind, slot_of(kind, slot), 12 + step, x_way if step < 2 else y_way)

    kept = []
    for kind in range(kinds):
        for step in range(1, 4):
            start(kind, own(kind), step, along[step - 1])
        start(kind, own(kind), 4, y_way)
        start(kind, own(kind), 8, x_way)
        copy = pltpu.make_async_copy(own(kind), slot_of(kind, 0), local.at[kind])
        copy.start()
        kept.append(copy)
    for kind in range(kinds):
        for step in range(1, 4):
            copies[kind, step].wait_recv()
            start(kind, slot_of(kind, step), 4 + step, y_way)
            start(kind, slot_of(kind, step), 8 + step, x_way)
        if kind:
            pass_far(kind - 1)
    pass_far(kinds - 1)
    rest = (6, 7, 8, 9, 12, 13, 14, 15)
    for slot in rest:
        copies[0, slot].wait_recv()
    kept[0].wait()
    shared = pltpu.make_async_remote_copy(
        src_ref=vec_out,
        dst_ref=vec_other,
        send_sem=send.at[0, 0],
        recv_sem=recv.at[0, 0],
        device_id={"tensor": other},
        device_id_type=MESH,
    )
    shared.start()
    for kind in range(1, kinds):
        for slot in rest:
            copies[kind, slot].wait_recv()
        kept[kind].wait()
    for copy in copies.values():
        copy.wait_send()
    shared.wait()


def gather_first(vectors, qkv):
    anywhere = pl.BlockSpec(memory_space=pl.ANY)
    inside = pl.BlockSpec(memory_space=pltpu.VMEM)
    kinds = 1 + qkv.shape[0] // CHUNK
    return pl.pallas_call(
        gather_kernel,
        out_shape=(
            jax.ShapeDtypeStruct((16, *vectors.shape), vectors.dtype),
            jax.ShapeDtypeStruct((16, *qkv.shape), qkv.dtype),
            jax.ShapeDtypeStruct((16, *vectors.shape), vectors.dtype),
        ),
        in_specs=[inside, inside],
        out_specs=(anywhere, anywhere, anywhere),
        scratch_shapes=[
            pltpu.SemaphoreType.DMA((kinds, 16)),
            pltpu.SemaphoreType.DMA((kinds, 16)),
            pltpu.SemaphoreType.DMA((kinds,)),
        ],
        compiler_params=pltpu.CompilerParams(collective_id=0, has_side_effects=True),
        name="gather_first",
    )(vectors, qkv)


def scatter_kernel(
    small_ref, grad_ref, small_out, grad_out,
    small_via, small_fold, small_cross, small_sums, small_last,
    grad_via, grad_fold, grad_cross, grad_sums, grad_last,
    send, recv,
):
    along, x_way, y_way = partners_of(lax.axis_index("dp"))
    greet(along, x_way, y_way, 1 - lax.axis_index("tensor"))
    kinds = 1 + grad_out.shape[0] // CHUNK
    copies = {}

    def at(pair, kind, slot):
        return pair[1].at[slot, pl.ds((kind - 1) * CHUNK, CHUNK)] if kind else pair[0].at[slot]

    blocks = (small_ref, grad_ref)
    via, fold = (small_via, grad_via), (small_fold, grad_fold)
    cross, sums, last = (small_cross, grad_cross), (small_sums, grad_sums), (small_last, grad_last)

    def wide(pair, kind, slot):
        return at(pair, kind, slot)[...].astype(F32)

    def start(kind, source, target, number, device):
        copy = pltpu.make_async_remote_copy(
            src_ref=source,
            dst_ref=target,
            send_sem=send.at[kind, number],
            recv_sem=recv.at[kind, number],
            device_id={"dp": device},
            device_id_type=MESH,
        )
        copy.start()
        copies[kind, number] = copy

    def result(kind):
        return grad_out.at[pl.ds((kind - 1) * CHUNK, CHUNK)] if kind else small_out

    def close(kind):
        for step in (3, 1, 2, 0):
            copies[kind, 4 + step].wait_recv()
            copies[kind, 8 + step].wait_recv()
            total = wide(blocks, kind, step) + wide(cross, kind, step) + wide(cross, kind, 4 + step)
            if step:
                source = at(sums, kind, step)
                source[...] = total.astype(source.dtype)
                start(kind, source, at(last, kind, step), 12 + step, along[3 - step])
            else:
                result(kind)[...] = total

    for kind in range(kinds):
        for step in range(4):
            way = x_way if step < 2 else y_way
            start(kind, at(blocks, kind, 12 + step), at(via, kind, step), step, way)
        for step in range(2):
            start(kind, at(blocks, kind, 6 + step), at(cross, kind, 2 + step), 6 + step, y_way)
            start(kind, at(blocks, kind, 8 + step), at(cross, kind, 4 + step), 8 + step, x_way)
    for kind in range(kinds):
        for step in (1, 3, 0, 2):
            slot = 4 + step if step < 2 else 8 + step
            copies[kind, step].wait_recv()
            source = at(fold, kind, step)
            source[...] = (wide(blocks, kind, slot) + wide(via, kind, step)).astype(source.dtype)
            start(kind, source, at(cross, kind, slot - 4), slot, y_way if step < 2 else x_way)
        if kind:
            close(kind - 1)
    close(kinds - 1)
    for kind in range(kinds):
        for step in range(1, 4):
            copies[kind, 12 + step].wait_recv()
            result(kind)[...] += wide(last, kind, step)
    for copy in copies.values():
        copy.wait_send()


def scatter_last(small, grads):
    inside = pl.BlockSpec(memory_space=pltpu.VMEM)
    scratch = []
    for value in (small, grads):
        for slots in (4, 4, 8, 4, 4):
            scratch.append(pltpu.VMEM((slots, *value.shape[1:]), value.dtype))
    return pl.pallas_call(
        scatter_kernel,
        out_shape=(
            jax.ShapeDtypeStruct(small.shape[1:], F32),
            jax.ShapeDtypeStruct(grads.shape[1:], F32),
        ),
        in_specs=[inside, inside],
        out_specs=(inside, inside),
        scratch_shapes=scratch
        + [pltpu.SemaphoreType.DMA((1 + grads.shape[1] // CHUNK, 16))] * 2,
        compiler_params=pltpu.CompilerParams(collective_id=1, has_side_effects=True),
        name="scatter_last",
    )(small, grads)


def swap(value):
    return lax.ppermute(value, "tensor", [(0, 1), (1, 0)])


def after(value, earlier):
    return lax.optimization_barrier((value, earlier))[0]


def dot(a, b):
    return lax.dot_general(a, b, (((1,), (0,)), ((), ())), preferred_element_type=F32)


def dot_nt(a, b):
    return lax.dot_general(a, b, (((1,), (1,)), ((), ())), preferred_element_type=F32)


def dot_tn(a, b):
    return lax.dot_general(a, b, (((0,), (0,)), ((), ())), preferred_element_type=F32)


def norm_parts(features):
    average = jnp.mean(features, axis=-1, keepdims=True)
    centered = features - average
    spread = jnp.mean(centered * centered, axis=-1, keepdims=True)
    scale = lax.rsqrt(spread + EPS)
    return centered * scale, scale


def norm_back(grad, normed, scale, gain):
    h = grad * gain
    return scale * (
        h - jnp.mean(h, axis=-1, keepdims=True) - normed * jnp.mean(h * normed, axis=-1, keepdims=True)
    )


STRIP = 256


def strip_scores(keys, queries, first, prefix):
    scores = dot_nt(keys, queries) * (queries.shape[1] ** (-0.5))
    key = lax.broadcasted_iota(jnp.int32, scores.shape, 0)
    query = first + lax.broadcasted_iota(jnp.int32, scores.shape, 1)
    return jnp.where((key <= query) | (key < prefix), scores, NEGATIVE)


def strips(length):
    return [(first, max(length // 2, first + STRIP)) for first in range(0, length, STRIP)]


def attend_kernel(head_dim, prefix_ref, q_ref, k_ref, v_ref, out_ref, lse_ref):
    prefix = prefix_ref[0]
    for head in range(q_ref.shape[1] // head_dim):
        columns = slice(head * head_dim, (head + 1) * head_dim)
        for first, reach in strips(q_ref.shape[0]):
            own = slice(first, first + STRIP)
            scores = strip_scores(k_ref[:reach, columns], q_ref[own, columns], first, prefix)
            top = jnp.max(scores, axis=0, keepdims=True)
            powered = jnp.exp(scores - top)
            total = jnp.sum(powered, axis=0, keepdims=True)
            probabilities = (powered * (1.0 / total)).astype(BF)
            attended = dot_tn(v_ref[:reach, columns], probabilities)
            out_ref[own, columns] = attended.T.astype(BF)
            lse_ref[0, head : head + 1, own] = top + jnp.log(total)


def attend_back_kernel(
    head_dim, prefix_ref, q_ref, k_ref, v_ref, back_ref, lse_ref, out_ref, key_sum, value_sum
):
    prefix = prefix_ref[0]
    score_scale = head_dim ** (-0.5)
    for head in range(q_ref.shape[1] // head_dim):
        columns = slice(head * head_dim, (head + 1) * head_dim)
        for first, reach in reversed(strips(q_ref.shape[0])):
            own = slice(first, first + STRIP)
            keys, queries = k_ref[:reach, columns], q_ref[own, columns]
            back_rows = back_ref[own, columns]
            scores = strip_scores(keys, queries, first, prefix)
            probabilities = jnp.exp(scores - lse_ref[0, head : head + 1, own])
            back_probs = dot_nt(v_ref[:reach, columns], back_rows)
            row_dot = jnp.sum(probabilities * back_probs, axis=0, keepdims=True)
            back_scores = (probabilities * (back_probs - row_dot)).astype(BF)
            out_ref[0, own, columns] = (dot_tn(keys, back_scores) * score_scale).T.astype(BF)
            back_key = dot(back_scores, queries)
            back_value = dot(probabilities.astype(BF), back_rows)
            if reach == q_ref.shape[0]:
                key_sum[...] = back_key
                value_sum[...] = back_value
            else:
                key_sum[:reach, :] += back_key
                value_sum[:reach, :] += back_value
        out_ref[1, :, columns] = (key_sum[...] * score_scale).astype(BF)
        out_ref[2, :, columns] = value_sum[...].astype(BF)


def attend_specs(length, groups):
    joint = [
        pl.BlockSpec((length, 128), lambda i, kind=kind: (0, kind * groups + i)) for kind in range(3)
    ]
    rows = pl.BlockSpec((length, 128), lambda i: (0, i))
    sums = pl.BlockSpec((1, 8, length), lambda i: (i, 0, 0))
    return [pl.BlockSpec(memory_space=pltpu.SMEM)] + joint, rows, sums


def attend(qkv, prefix, head_dim):
    length, part = qkv.shape[0], qkv.shape[1] // 3
    groups = part // 128
    inputs, rows, sums = attend_specs(length, groups)
    work = length * length * part
    return pl.pallas_call(
        functools.partial(attend_kernel, head_dim),
        grid=(groups,),
        out_shape=(
            jax.ShapeDtypeStruct((length, part), BF),
            jax.ShapeDtypeStruct((groups, 8, length), F32),
        ),
        in_specs=inputs,
        out_specs=(rows, sums),
        cost_estimate=pl.CostEstimate(
            flops=4 * work, bytes_accessed=8 * length * part, transcendentals=work // head_dim
        ),
        name="attend",
    )(prefix, qkv, qkv, qkv)


def attend_back(qkv, prefix, back_attended, lse, head_dim):
    length, part = back_attended.shape
    groups = part // 128
    inputs, rows, sums = attend_specs(length, groups)
    work = length * length * part
    return pl.pallas_call(
        functools.partial(attend_back_kernel, head_dim),
        grid=(groups,),
        out_shape=jax.ShapeDtypeStruct((3, length, part), BF),
        in_specs=inputs + [rows, sums],
        out_specs=pl.BlockSpec((3, length, 128), lambda i: (0, 0, i)),
        scratch_shapes=[pltpu.VMEM((length, head_dim), F32), pltpu.VMEM((length, head_dim), F32)],
        cost_estimate=pl.CostEstimate(
            flops=10 * work, bytes_accessed=14 * length * part, transcendentals=work // head_dim
        ),
        name="attend_back",
    )(prefix, qkv, qkv, qkv, back_attended, lse)


def body(
    ring,
    tokens,
    cotangent,
    prefix,
    routes,
    norm1_gain,
    norm1_bias,
    w_query,
    w_key,
    w_value,
    w_out,
    norm2_gain,
    norm2_bias,
    centroids,
    expert_in,
    expert_out,
):
    side = lax.axis_index("tensor")
    own_rows, width = tokens.shape
    all_rows = 2 * own_rows
    head_dim = width // HEADS
    part = w_query.shape[1]
    rows = w_query.shape[0]
    experts, _, hidden = expert_in.shape
    count = ring.count

    def both(own):
        other = swap(own)
        return jnp.where(
            side == 0, jnp.concatenate([own, other], 0), jnp.concatenate([other, own], 0)
        )

    vectors = jnp.concatenate(
        [
            norm1_gain[None],
            norm1_bias[None],
            norm2_gain[None],
            norm2_bias[None],
            centroids,
        ],
        axis=0,
    )
    small_count = vectors.shape[0]
    qkv_block = jnp.concatenate([w_query, w_key, w_value, w_out.T], axis=1)
    in_block = expert_in.transpose(1, 0, 2).reshape(rows, experts * hidden)
    out_blocks = expert_out.transpose(2, 0, 1)
    out_block, turned_block = out_blocks[:, 0], out_blocks[:, 1]
    if count == 16:
        padded = jnp.pad(vectors, ((0, 8 - small_count), (0, 128 - rows // 2)))
        table, qkv_w, other_table = gather_first(padded, qkv_block)
        table, other_table = (t[:, :small_count, : rows // 2] for t in (table, other_table))
        table = jnp.where(
            side == 0,
            jnp.concatenate([table, other_table], 2),
            jnp.concatenate([other_table, table], 2),
        )
        qkv_w = qkv_w.reshape(width, 4 * part)
    else:
        other_vectors = swap(vectors)
        vectors = jnp.where(
            side == 0,
            jnp.concatenate([vectors, other_vectors], 1),
            jnp.concatenate([other_vectors, vectors], 1),
        )
        table = ring.gather(vectors.reshape(1, small_count * rows)).reshape(count, small_count, rows)
        qkv_w = ring.gather(qkv_block)
    table = table.transpose(1, 0, 2).reshape(small_count, width)
    gain_one, bias_one, gain_two, bias_two = (table[i : i + 1] for i in range(4))
    centres = table[4:]

    qkv_w, in_block, turned_block = lax.optimization_barrier((qkv_w, in_block, turned_block))
    qkv_w, out_w = qkv_w[:, : 3 * part], qkv_w[:, 3 * part :]
    in_lead = ring.lead(in_block)
    if count == 16:
        turned_crossed = ring.cross(turned_block)
        turned_square = ring.close(turned_block, turned_crossed)
        in_lead, turned_square = lax.optimization_barrier((in_lead, turned_square))
        turned_w = ring.along(turned_square)
    else:
        turned_w = ring.gather(turned_block)
    in_crossed = ring.cross(in_lead)
    out_lead = ring.lead(after(out_block, in_lead))
    in_w = ring.close(in_lead, in_crossed)
    out_crossed = ring.cross(after(out_lead, in_w))
    back_ws = (ring.close(out_lead, out_crossed), turned_w)

    found = ring.width_order(width)
    to_order = (jnp.arange(width, dtype=jnp.int32)[:, None] == found[None, :]).astype(BF)
    tokens_all = dot(both(tokens), to_order)
    back_all = lax.optimization_barrier(dot(both(cotangent), to_order).astype(BF)).astype(F32)

    normed_one, scale_one = norm_parts(tokens_all)
    first_rows = (normed_one * gain_one + bias_one).astype(BF)
    qkv = dot(first_rows, qkv_w).astype(BF)
    attended, lse = attend(qkv, prefix, head_dim)
    attended = after(attended, in_lead)

    attn_terms = dot_nt(attended, out_w).astype(BF)
    residual = tokens_all + (attn_terms.astype(F32) + swap(attn_terms).astype(F32))
    normed_two, scale_two = norm_parts(residual)
    second_rows = (normed_two * gain_two + bias_two).astype(BF)
    second_wide = second_rows.astype(F32)

    is_last = routes == 1
    ones_before = jnp.tril(jnp.ones((all_rows, all_rows), BF))
    last_before = dot(ones_before, is_last.astype(BF)).astype(jnp.int32)
    position = jnp.arange(all_rows, dtype=jnp.int32)[:, None]
    first_count = all_rows - last_before[all_rows - 1, 0]
    place = jnp.where(is_last, first_count + last_before - 1, position - last_before)
    sort_to = (place == jnp.arange(all_rows, dtype=jnp.int32)[None, :]).astype(BF)
    tail = all_rows - CAP
    in_first = position < first_count

    centre_rows = jnp.where(is_last, centres[1:2], centres[0:1])
    gate = jax.nn.sigmoid(jnp.sum(second_wide * centre_rows, axis=-1, keepdims=True))
    back_branch = (gate * back_all).astype(BF)
    gate, back_branch, sent_rows = lax.optimization_barrier((gate, back_branch, second_rows))
    picked = dot_tn(sort_to, sent_rows).astype(BF)
    back_slots = dot_tn(sort_to, back_branch).astype(BF)
    windows = (slice(0, CAP), slice(tail, all_rows))
    masks = (in_first[:CAP], ~in_first[tail:])
    slot_out, back_picked, grads_in, grads_out = [], [], [], []
    hidden_of = []
    for e in range(2):
        columns = slice(e * hidden, (e + 1) * hidden)
        rows_in = picked[windows[e]]
        back_rows = jnp.where(masks[e], back_slots[windows[e]], jnp.zeros((), BF))
        up = dot(rows_in, in_w[:, columns])
        activated = lax.optimization_barrier(jax.nn.gelu(up).astype(BF))
        grads_out.append(dot_tn(back_rows, activated).astype(BF))
        hidden_of.append((columns, rows_in, back_rows, up, activated))
    grads_out = jnp.concatenate(grads_out, axis=1)
    out_via = ring.far(grads_out, BF)
    for e, (columns, rows_in, back_rows, up, activated) in enumerate(hidden_of):
        if e == 1:
            back_rows = after(back_rows, out_via)
        slot_out.append(dot_nt(activated, back_ws[e]).astype(BF))
        back_activated = dot(back_rows, back_ws[e])
        back_up = jax.vjp(jax.nn.gelu, up)[1](back_activated)[0].astype(BF)
        grads_in.append(dot_tn(rows_in, back_up).astype(BF))
        back_picked.append(dot_nt(back_up, in_w[:, columns]).astype(BF))
    grads_in = jnp.concatenate(grads_in, axis=1)
    out_near = ring.near(grads_out, out_via, BF)
    in_via = ring.far(after(grads_in, out_via), BF)

    def unsort(pieces):
        joined = jnp.concatenate(
            [
                pieces[0][:tail],
                jnp.where(in_first[tail:CAP], pieces[0][tail:], pieces[1][: CAP - tail]),
                pieces[1][CAP - tail :],
            ],
            axis=0,
        )
        return dot(sort_to, joined).astype(BF)

    row_terms = unsort(slot_out)
    expert_rows = row_terms.astype(F32) + swap(row_terms).astype(F32)
    block_all = (residual + gate * expert_rows).astype(BF)
    first_own = side * own_rows
    block_out = dot_nt(lax.dynamic_slice_in_dim(block_all, first_own, own_rows), to_order).astype(BF)
    back_score = jnp.sum(back_all * expert_rows, axis=-1, keepdims=True) * gate * (1.0 - gate)

    second_terms = unsort(back_picked)
    back_second = second_terms.astype(F32) + swap(second_terms).astype(F32) + back_score * centre_rows
    weighted = back_score * second_wide
    grad_centre = jnp.stack(
        [
            jnp.sum(jnp.where(is_last, 0.0, weighted), axis=0),
            jnp.sum(jnp.where(is_last, weighted, 0.0), axis=0),
        ]
    )
    grad_gain_two = jnp.sum(back_second * normed_two, axis=0)
    grad_bias_two = jnp.sum(back_second, axis=0)
    back_residual = back_all + norm_back(back_second, normed_two, scale_two, gain_two)
    back_out = back_residual.astype(BF)
    grads_out = ring.last(grads_out, out_near, BF)
    in_near = ring.near(grads_in, in_via, BF)
    back_attended = dot(back_out, out_w).astype(BF)
    grad_out = dot_tn(back_out, attended).astype(BF)
    back_qkv = attend_back(qkv, prefix, back_attended, lse, head_dim)
    back_qkv = after(back_qkv, (in_near, grads_out))
    grads_in = ring.last(grads_in, in_near, BF)
    grad_qkv = jnp.concatenate([dot_tn(first_rows, back_qkv[i]).astype(BF) for i in range(3)], axis=1)
    first_terms = sum(dot_nt(back_qkv[i], qkv_w[:, i * part : (i + 1) * part]) for i in range(3))
    first_terms = first_terms.astype(BF)
    own_terms = lax.dynamic_slice_in_dim(first_terms, first_own, own_rows)
    other_terms = lax.dynamic_slice_in_dim(first_terms, own_rows - first_own, own_rows)
    back_first = own_terms.astype(F32) + swap(other_terms).astype(F32)

    def mine(value):
        return lax.dynamic_slice_in_dim(value, first_own, own_rows)

    normed_own = mine(normed_one)
    back_norm_one = norm_back(back_first, normed_own, mine(scale_one), gain_one)
    grad_tokens = dot_nt(
        (mine(back_residual) + back_norm_one).astype(BF), to_order
    ).astype(BF)
    one_part = jnp.stack([jnp.sum(back_first * normed_own, axis=0), jnp.sum(back_first, axis=0)])
    one_part = one_part + swap(one_part)
    small = jnp.concatenate(
        [one_part, grad_gain_two[None], grad_bias_two[None], grad_centre], axis=0
    )
    small = small.reshape(small_count, count, rows).transpose(1, 0, 2)
    grad_first = jnp.concatenate([grad_qkv, grad_out], axis=1)
    if count == 16:
        small = jnp.pad(small, ((0, 0), (0, 8 - small_count), (0, 128 - rows)))
        small, grad_first = scatter_last(small, grad_first.reshape(count, rows, 4 * part))
        small = small[:small_count, :rows]
    else:
        grad_first = ring.scatter(grad_first, BF)
        small = ring.scatter(small.reshape(count, small_count * rows), F32).reshape(small_count, rows)
    grad_qkv, grad_out = grad_first[:, : 3 * part], grad_first[:, 3 * part :]
    small = lax.dynamic_slice_in_dim(small, side * (rows // 2), rows // 2, axis=1)
    return (
        block_out,
        grad_tokens,
        small[0],
        small[1],
        grad_qkv[:, :part],
        grad_qkv[:, part : 2 * part],
        grad_qkv[:, 2 * part :],
        grad_out.T,
        small[2],
        small[3],
        small[4:],
        grads_in.reshape(rows, experts, hidden).transpose(1, 0, 2),
        grads_out.reshape(rows, experts, hidden).transpose(1, 2, 0),
    )


def solution(mesh):
    ring = Ring(mesh.shape["dp"])
    both, rows = P(("dp", "tensor")), P(("dp", "tensor"), None)
    columns = P("dp", "tensor")

    def step(*arguments):
        return body(ring, *arguments)

    return jax.shard_map(
        step,
        mesh=mesh,
        in_specs=(
            rows,
            rows,
            P("dp"),
            P("dp", None),
            both,
            both,
            columns,
            columns,
            columns,
            P("tensor", "dp"),
            both,
            both,
            P(None, ("dp", "tensor")),
            P(None, "dp", "tensor"),
            P(None, "tensor", "dp"),
        ),
        out_specs=(
            rows,
            rows,
            both,
            both,
            columns,
            columns,
            columns,
            P("tensor", "dp"),
            both,
            both,
            P(None, ("dp", "tensor")),
            P(None, "dp", "tensor"),
            P(None, "tensor", "dp"),
        ),
        check_vma=False,
    )
```

```python
import functools

import jax
import jax.numpy as jnp
from jax import lax
from jax.experimental import pallas as pl
from jax.experimental.pallas import tpu as pltpu
from jax.sharding import PartitionSpec as P


HEADS = 12
CAP = 640
EPS = 1e-05
NEGATIVE = -1e30
BF = jnp.bfloat16
F32 = jnp.float32
MESH = pl.DeviceIdType.MESH


def factors_of(count):
    rest, sizes = count // 2, []
    while rest % 4 == 0:
        sizes.append(4)
        rest //= 4
    while rest % 2 == 0 and rest > 1:
        sizes.append(2)
        rest //= 2
    return sizes + ([2] if count > 1 else [])


class Ring:
    def __init__(self, count):
        self.count = count
        self.sizes = factors_of(count)
        self.strides = []
        stride = count
        for size in self.sizes:
            stride //= size
            self.strides.append(stride)
        self.square = len(self.sizes) >= 2 and self.sizes[-1] == 2 and self.sizes[-2] == 2

    def order(self, size):
        return [0, 1, 3, 2] if size == 4 else list(range(size))

    def shift(self, stage, step):
        size, stride = self.sizes[stage], self.strides[stage]
        order = self.order(size)
        pairs = []
        for source in range(self.count):
            digit = source // stride % size
            target = order[(order.index(digit) + step) % size]
            pairs.append((source, source + (target - digit) * stride))
        return pairs

    def move(self, value, stage, step):
        return lax.ppermute(value, "dp", self.shift(stage, step))

    def lead(self, block):
        for stage in range(len(self.sizes) - (2 if self.square else 0)):
            parts = [block] + [self.move(block, stage, s) for s in range(1, self.sizes[stage])]
            block = jnp.concatenate(parts, axis=0)
        return lax.optimization_barrier(block)

    def cross(self, block):
        if not self.square:
            return ()
        y, x = len(self.sizes) - 2, len(self.sizes) - 1
        return self.move(block, x, 1), self.move(block, y, 1)

    def close(self, block, crossed):
        if not self.square:
            return block
        y, x = len(self.sizes) - 2, len(self.sizes) - 1
        half = block.shape[0] // 2
        from_x, from_y = crossed
        low, high = self.move(from_y[:half], x, 1), self.move(from_x[half:], y, 1)
        return jnp.concatenate([block, from_y, from_x, low, high], axis=0)

    def along(self, blocks):
        steps = [blocks] + [self.move(blocks, 0, step) for step in range(1, 4)]
        rows, width = blocks.shape
        joined = jnp.stack([step.reshape(4, rows // 4, width) for step in steps], axis=1)
        return joined.reshape(4 * rows, width)

    def gather(self, block):
        block = self.lead(block)
        return self.close(block, self.cross(block))

    def far(self, total, kind):
        if not self.square:
            return ()
        y, x = len(self.sizes) - 2, len(self.sizes) - 1
        quarter = total.shape[0] // 4
        half = quarter // 2
        far = total[3 * quarter :]
        return self.move(far[:half].astype(kind), x, 1), self.move(far[half:].astype(kind), y, 1)

    def near(self, total, via, kind):
        if not self.square:
            return ()
        y, x = len(self.sizes) - 2, len(self.sizes) - 1
        quarter = total.shape[0] // 4
        half = quarter // 2
        via_x, via_y = via
        to_y, to_x = total[quarter : 2 * quarter], total[2 * quarter : 3 * quarter]
        to_y = jnp.concatenate([(to_y[:half].astype(F32) + via_x).astype(kind), to_y[half:].astype(kind)], axis=0)
        to_x = jnp.concatenate([to_x[:half].astype(kind), (to_x[half:].astype(F32) + via_y).astype(kind)], axis=0)
        return self.move(to_x, x, 1), self.move(to_y, y, 1)

    def last(self, total, crossed, kind):
        stages = len(self.sizes)
        if self.square:
            own = total[: total.shape[0] // 4].astype(F32)
            total = own + crossed[0].astype(F32) + crossed[1].astype(F32)
            stages -= 2
        for stage in reversed(range(stages)):
            size = self.sizes[stage]
            piece = total.shape[0] // size
            parts = [total[i * piece : (i + 1) * piece] for i in range(size)]
            total = parts[0].astype(F32)
            for step in range(1, size):
                total = total + self.move(parts[step].astype(kind), stage, size - step).astype(F32)
        return total

    def scatter(self, total, kind):
        return self.last(total, self.near(total, self.far(total, kind), kind), kind)

    def width_order(self, width):
        me = lax.axis_index("dp")
        rows = width // self.count
        column = jnp.arange(width, dtype=jnp.int32)
        inner, block = column % rows, column // rows
        found = jnp.zeros_like(column)
        for size, stride in zip(self.sizes, self.strides):
            step, block = block % size, block // size
            digit = me // stride % size
            if size == 4:
                place = jnp.bitwise_xor(digit, digit // 2)
                back = (place - step + size) % size
                source = jnp.bitwise_xor(back, back // 2)
            else:
                source = (digit - step + size) % size
            found = found + source * stride
        return found * rows + inner


def ring_place(digit):
    return digit + (digit // 2) * (1 - 2 * (digit % 2))


def partners_of(me):
    digit = me // 4
    place = ring_place(digit)
    along = [me + (ring_place((place + step) % 4) - digit) * 4 for step in range(1, 4)]
    return along, me + 1 - 2 * (me % 2), me + 2 - 4 * ((me // 2) % 2)


def greet(along, x_way, y_way, other):
    barrier = pltpu.get_barrier_semaphore()
    for device in along + [x_way, y_way]:
        pl.semaphore_signal(barrier, inc=1, device_id={"dp": device}, device_id_type=MESH)
    pl.semaphore_signal(barrier, inc=1, device_id={"tensor": other}, device_id_type=MESH)
    pl.semaphore_wait(barrier, 6)


CHUNK = 16


def gather_kernel(vec_ref, qkv_ref, vec_out, qkv_out, vec_other, send, recv, local):
    along, x_way, y_way = partners_of(lax.axis_index("dp"))
    other = 1 - lax.axis_index("tensor")
    greet(along, x_way, y_way, other)
    kinds = 1 + qkv_ref.shape[0] // CHUNK
    copies = {}

    def own(kind):
        return qkv_ref.at[pl.ds((kind - 1) * CHUNK, CHUNK)] if kind else vec_ref

    def slot_of(kind, slot):
        return qkv_out.at[slot, pl.ds((kind - 1) * CHUNK, CHUNK)] if kind else vec_out.at[slot]

    def start(kind, source, slot, device):
        copy = pltpu.make_async_remote_copy(
            src_ref=source,
            dst_ref=slot_of(kind, slot),
            send_sem=send.at[kind, slot],
            recv_sem=recv.at[kind, slot],
            device_id={"dp": device},
            device_id_type=MESH,
        )
        copy.start()
        copies[kind, slot] = copy

    def pass_far(kind):
        for step in range(4):
            slot = 4 + step if step < 2 else 8 + step
            copies[kind, slot].wait_recv()
            start(kind, slot_of(kind, slot), 12 + step, x_way if step < 2 else y_way)

    kept = []
    for kind in range(kinds):
        for step in range(1, 4):
            start(kind, own(kind), step, along[step - 1])
        start(kind, own(kind), 4, y_way)
        start(kind, own(kind), 8, x_way)
        copy = pltpu.make_async_copy(own(kind), slot_of(kind, 0), local.at[kind])
        copy.start()
        kept.append(copy)
    for kind in range(kinds):
        for step in range(1, 4):
            copies[kind, step].wait_recv()
            start(kind, slot_of(kind, step), 4 + step, y_way)
            start(kind, slot_of(kind, step), 8 + step, x_way)
        if kind:
            pass_far(kind - 1)
    pass_far(kinds - 1)
    rest = (6, 7, 8, 9, 12, 13, 14, 15)
    for slot in rest:
        copies[0, slot].wait_recv()
    kept[0].wait()
    shared = pltpu.make_async_remote_copy(
        src_ref=vec_out,
        dst_ref=vec_other,
        send_sem=send.at[0, 0],
        recv_sem=recv.at[0, 0],
        device_id={"tensor": other},
        device_id_type=MESH,
    )
    shared.start()
    for kind in range(1, kinds):
        for slot in rest:
            copies[kind, slot].wait_recv()
        kept[kind].wait()
    for copy in copies.values():
        copy.wait_send()
    shared.wait()


def gather_first(vectors, qkv):
    anywhere = pl.BlockSpec(memory_space=pl.ANY)
    inside = pl.BlockSpec(memory_space=pltpu.VMEM)
    kinds = 1 + qkv.shape[0] // CHUNK
    return pl.pallas_call(
        gather_kernel,
        out_shape=(
            jax.ShapeDtypeStruct((16, *vectors.shape), vectors.dtype),
            jax.ShapeDtypeStruct((16, *qkv.shape), qkv.dtype),
            jax.ShapeDtypeStruct((16, *vectors.shape), vectors.dtype),
        ),
        in_specs=[inside, inside],
        out_specs=(anywhere, anywhere, anywhere),
        scratch_shapes=[
            pltpu.SemaphoreType.DMA((kinds, 16)),
            pltpu.SemaphoreType.DMA((kinds, 16)),
            pltpu.SemaphoreType.DMA((kinds,)),
        ],
        compiler_params=pltpu.CompilerParams(collective_id=0, has_side_effects=True),
        name="gather_first",
    )(vectors, qkv)


def scatter_kernel(
    small_ref, grad_ref, small_out, grad_out,
    small_via, small_fold, small_cross, small_sums, small_last,
    grad_via, grad_fold, grad_cross, grad_sums, grad_last,
    send, recv,
):
    along, x_way, y_way = partners_of(lax.axis_index("dp"))
    greet(along, x_way, y_way, 1 - lax.axis_index("tensor"))
    kinds = 1 + grad_out.shape[0] // CHUNK
    copies = {}

    def at(pair, kind, slot):
        return pair[1].at[slot, pl.ds((kind - 1) * CHUNK, CHUNK)] if kind else pair[0].at[slot]

    blocks = (small_ref, grad_ref)
    via, fold = (small_via, grad_via), (small_fold, grad_fold)
    cross, sums, last = (small_cross, grad_cross), (small_sums, grad_sums), (small_last, grad_last)

    def wide(pair, kind, slot):
        return at(pair, kind, slot)[...].astype(F32)

    def start(kind, source, target, number, device):
        copy = pltpu.make_async_remote_copy(
            src_ref=source,
            dst_ref=target,
            send_sem=send.at[kind, number],
            recv_sem=recv.at[kind, number],
            device_id={"dp": device},
            device_id_type=MESH,
        )
        copy.start()
        copies[kind, number] = copy

    def result(kind):
        return grad_out.at[pl.ds((kind - 1) * CHUNK, CHUNK)] if kind else small_out

    def close(kind):
        for step in (3, 1, 2, 0):
            copies[kind, 4 + step].wait_recv()
            copies[kind, 8 + step].wait_recv()
            total = wide(blocks, kind, step) + wide(cross, kind, step) + wide(cross, kind, 4 + step)
            if step:
                source = at(sums, kind, step)
                source[...] = total.astype(source.dtype)
                start(kind, source, at(last, kind, step), 12 + step, along[3 - step])
            else:
                result(kind)[...] = total

    for kind in range(kinds):
        for step in range(4):
            way = x_way if step < 2 else y_way
            start(kind, at(blocks, kind, 12 + step), at(via, kind, step), step, way)
        for step in range(2):
            start(kind, at(blocks, kind, 6 + step), at(cross, kind, 2 + step), 6 + step, y_way)
            start(kind, at(blocks, kind, 8 + step), at(cross, kind, 4 + step), 8 + step, x_way)
    for kind in range(kinds):
        for step in (1, 3, 0, 2):
            slot = 4 + step if step < 2 else 8 + step
            copies[kind, step].wait_recv()
            source = at(fold, kind, step)
            source[...] = (wide(blocks, kind, slot) + wide(via, kind, step)).astype(source.dtype)
            start(kind, source, at(cross, kind, slot - 4), slot, y_way if step < 2 else x_way)
        if kind:
            close(kind - 1)
    close(kinds - 1)
    for kind in range(kinds):
        for step in range(1, 4):
            copies[kind, 12 + step].wait_recv()
            result(kind)[...] += wide(last, kind, step)
    for copy in copies.values():
        copy.wait_send()


def scatter_last(small, grads):
    inside = pl.BlockSpec(memory_space=pltpu.VMEM)
    scratch = []
    for value in (small, grads):
        for slots in (4, 4, 8, 4, 4):
            scratch.append(pltpu.VMEM((slots, *value.shape[1:]), value.dtype))
    return pl.pallas_call(
        scatter_kernel,
        out_shape=(
            jax.ShapeDtypeStruct(small.shape[1:], F32),
            jax.ShapeDtypeStruct(grads.shape[1:], F32),
        ),
        in_specs=[inside, inside],
        out_specs=(inside, inside),
        scratch_shapes=scratch
        + [pltpu.SemaphoreType.DMA((1 + grads.shape[1] // CHUNK, 16))] * 2,
        compiler_params=pltpu.CompilerParams(collective_id=1, has_side_effects=True),
        name="scatter_last",
    )(small, grads)


def swap(value):
    return lax.ppermute(value, "tensor", [(0, 1), (1, 0)])


def after(value, earlier):
    return lax.optimization_barrier((value, earlier))[0]


def dot(a, b):
    return lax.dot_general(a, b, (((1,), (0,)), ((), ())), preferred_element_type=F32)


def dot_nt(a, b):
    return lax.dot_general(a, b, (((1,), (1,)), ((), ())), preferred_element_type=F32)


def dot_tn(a, b):
    return lax.dot_general(a, b, (((0,), (0,)), ((), ())), preferred_element_type=F32)


def norm_parts(features):
    average = jnp.mean(features, axis=-1, keepdims=True)
    centered = features - average
    spread = jnp.mean(centered * centered, axis=-1, keepdims=True)
    scale = lax.rsqrt(spread + EPS)
    return centered * scale, scale


def norm_back(grad, normed, scale, gain):
    h = grad * gain
    return scale * (
        h - jnp.mean(h, axis=-1, keepdims=True) - normed * jnp.mean(h * normed, axis=-1, keepdims=True)
    )


STRIP = 256


def strip_scores(keys, queries, first, prefix):
    scores = dot_nt(keys, queries) * (queries.shape[1] ** (-0.5))
    key = lax.broadcasted_iota(jnp.int32, scores.shape, 0)
    query = first + lax.broadcasted_iota(jnp.int32, scores.shape, 1)
    return jnp.where((key <= query) | (key < prefix), scores, NEGATIVE)


def strips(length):
    return [(first, max(length // 2, first + STRIP)) for first in range(0, length, STRIP)]


def attend_kernel(head_dim, prefix_ref, q_ref, k_ref, v_ref, out_ref, lse_ref):
    prefix = prefix_ref[0]
    for head in range(q_ref.shape[1] // head_dim):
        columns = slice(head * head_dim, (head + 1) * head_dim)
        for first, reach in strips(q_ref.shape[0]):
            own = slice(first, first + STRIP)
            scores = strip_scores(k_ref[:reach, columns], q_ref[own, columns], first, prefix)
            top = jnp.max(scores, axis=0, keepdims=True)
            powered = jnp.exp(scores - top)
            total = jnp.sum(powered, axis=0, keepdims=True)
            probabilities = (powered * (1.0 / total)).astype(BF)
            attended = dot_tn(v_ref[:reach, columns], probabilities)
            out_ref[own, columns] = attended.T.astype(BF)
            lse_ref[0, head : head + 1, own] = top + jnp.log(total)


def attend_back_kernel(
    head_dim, prefix_ref, q_ref, k_ref, v_ref, back_ref, lse_ref, out_ref, key_sum, value_sum
):
    prefix = prefix_ref[0]
    score_scale = head_dim ** (-0.5)
    for head in range(q_ref.shape[1] // head_dim):
        columns = slice(head * head_dim, (head + 1) * head_dim)
        for first, reach in reversed(strips(q_ref.shape[0])):
            own = slice(first, first + STRIP)
            keys, queries = k_ref[:reach, columns], q_ref[own, columns]
            back_rows = back_ref[own, columns]
            scores = strip_scores(keys, queries, first, prefix)
            probabilities = jnp.exp(scores - lse_ref[0, head : head + 1, own])
            back_probs = dot_nt(v_ref[:reach, columns], back_rows)
            row_dot = jnp.sum(probabilities * back_probs, axis=0, keepdims=True)
            back_scores = (probabilities * (back_probs - row_dot)).astype(BF)
            out_ref[0, own, columns] = (dot_tn(keys, back_scores) * score_scale).T.astype(BF)
            back_key = dot(back_scores, queries)
            back_value = dot(probabilities.astype(BF), back_rows)
            if reach == q_ref.shape[0]:
                key_sum[...] = back_key
                value_sum[...] = back_value
            else:
                key_sum[:reach, :] += back_key
                value_sum[:reach, :] += back_value
        out_ref[1, :, columns] = (key_sum[...] * score_scale).astype(BF)
        out_ref[2, :, columns] = value_sum[...].astype(BF)


def attend_specs(length, groups):
    joint = [
        pl.BlockSpec((length, 128), lambda i, kind=kind: (0, kind * groups + i)) for kind in range(3)
    ]
    rows = pl.BlockSpec((length, 128), lambda i: (0, i))
    sums = pl.BlockSpec((1, 8, length), lambda i: (i, 0, 0))
    return [pl.BlockSpec(memory_space=pltpu.SMEM)] + joint, rows, sums


def attend(qkv, prefix, head_dim):
    length, part = qkv.shape[0], qkv.shape[1] // 3
    groups = part // 128
    inputs, rows, sums = attend_specs(length, groups)
    work = length * length * part
    return pl.pallas_call(
        functools.partial(attend_kernel, head_dim),
        grid=(groups,),
        out_shape=(
            jax.ShapeDtypeStruct((length, part), BF),
            jax.ShapeDtypeStruct((groups, 8, length), F32),
        ),
        in_specs=inputs,
        out_specs=(rows, sums),
        cost_estimate=pl.CostEstimate(
            flops=4 * work, bytes_accessed=8 * length * part, transcendentals=work // head_dim
        ),
        name="attend",
    )(prefix, qkv, qkv, qkv)


def attend_back(qkv, prefix, back_attended, lse, head_dim):
    length, part = back_attended.shape
    groups = part // 128
    inputs, rows, sums = attend_specs(length, groups)
    work = length * length * part
    return pl.pallas_call(
        functools.partial(attend_back_kernel, head_dim),
        grid=(groups,),
        out_shape=jax.ShapeDtypeStruct((3, length, part), BF),
        in_specs=inputs + [rows, sums],
        out_specs=pl.BlockSpec((3, length, 128), lambda i: (0, 0, i)),
        scratch_shapes=[pltpu.VMEM((length, head_dim), F32), pltpu.VMEM((length, head_dim), F32)],
        cost_estimate=pl.CostEstimate(
            flops=10 * work, bytes_accessed=14 * length * part, transcendentals=work // head_dim
        ),
        name="attend_back",
    )(prefix, qkv, qkv, qkv, back_attended, lse)


def body(
    ring,
    tokens,
    cotangent,
    prefix,
    routes,
    norm1_gain,
    norm1_bias,
    w_query,
    w_key,
    w_value,
    w_out,
    norm2_gain,
    norm2_bias,
    centroids,
    expert_in,
    expert_out,
):
    side = lax.axis_index("tensor")
    own_rows, width = tokens.shape
    all_rows = 2 * own_rows
    head_dim = width // HEADS
    part = w_query.shape[1]
    rows = w_query.shape[0]
    experts, _, hidden = expert_in.shape
    count = ring.count

    def both(own):
        other = swap(own)
        return jnp.where(
            side == 0, jnp.concatenate([own, other], 0), jnp.concatenate([other, own], 0)
        )

    vectors = jnp.concatenate(
        [
            norm1_gain[None],
            norm1_bias[None],
            norm2_gain[None],
            norm2_bias[None],
            centroids,
        ],
        axis=0,
    )
    small_count = vectors.shape[0]
    qkv_block = jnp.concatenate([w_query, w_key, w_value, w_out.T], axis=1)
    in_block = expert_in.transpose(1, 0, 2).reshape(rows, experts * hidden)
    out_blocks = expert_out.transpose(2, 0, 1)
    out_block, turned_block = out_blocks[:, 0], out_blocks[:, 1]
    if count == 16:
        padded = jnp.pad(vectors, ((0, 8 - small_count), (0, 128 - rows // 2)))
        table, qkv_w, other_table = gather_first(padded, qkv_block)
        table, other_table = (t[:, :small_count, : rows // 2] for t in (table, other_table))
        table = jnp.where(
            side == 0,
            jnp.concatenate([table, other_table], 2),
            jnp.concatenate([other_table, table], 2),
        )
        qkv_w = qkv_w.reshape(width, 4 * part)
    else:
        other_vectors = swap(vectors)
        vectors = jnp.where(
            side == 0,
            jnp.concatenate([vectors, other_vectors], 1),
            jnp.concatenate([other_vectors, vectors], 1),
        )
        table = ring.gather(vectors.reshape(1, small_count * rows)).reshape(count, small_count, rows)
        qkv_w = ring.gather(qkv_block)
    table = table.transpose(1, 0, 2).reshape(small_count, width)
    gain_one, bias_one, gain_two, bias_two = (table[i : i + 1] for i in range(4))
    centres = table[4:]

    qkv_w, in_block, out_block, turned_block = lax.optimization_barrier(
        (qkv_w, in_block, out_block, turned_block)
    )
    qkv_w, out_w = qkv_w[:, : 3 * part], qkv_w[:, 3 * part :]
    if count == 16:
        joint = jnp.concatenate([in_block, out_block], axis=1)
        leads = [joint] + [ring.move(joint, 0, step) for step in range(1, 4)]
        wide = in_block.shape[1]
        in_lead = jnp.concatenate([lead[:, :wide] for lead in leads], axis=0)
        out_lead = jnp.concatenate([lead[:, wide:] for lead in leads], axis=0)
        turned_crossed = ring.cross(turned_block)
        turned_square = ring.close(turned_block, turned_crossed)
        in_lead, out_lead, turned_square = lax.optimization_barrier((in_lead, out_lead, turned_square))
        turned_w = ring.along(turned_square)
    else:
        in_lead, out_lead = ring.lead(in_block), ring.lead(out_block)
        turned_w = ring.gather(turned_block)
    in_crossed = ring.cross(in_lead)
    in_w = ring.close(in_lead, in_crossed)
    out_crossed = ring.cross(after(out_lead, in_w))
    back_ws = (ring.close(out_lead, out_crossed), turned_w)

    found = ring.width_order(width)
    to_order = (jnp.arange(width, dtype=jnp.int32)[:, None] == found[None, :]).astype(BF)
    tokens_all = dot(both(tokens), to_order)
    back_all = lax.optimization_barrier(dot(both(cotangent), to_order).astype(BF)).astype(F32)

    normed_one, scale_one = norm_parts(tokens_all)
    first_rows = (normed_one * gain_one + bias_one).astype(BF)
    qkv = dot(first_rows, qkv_w).astype(BF)
    attended, lse = attend(qkv, prefix, head_dim)
    attended = after(attended, in_lead)

    attn_terms = dot_nt(attended, out_w).astype(BF)
    residual = tokens_all + (attn_terms.astype(F32) + swap(attn_terms).astype(F32))
    normed_two, scale_two = norm_parts(residual)
    second_rows = (normed_two * gain_two + bias_two).astype(BF)
    second_wide = second_rows.astype(F32)

    is_last = routes == 1
    ones_before = jnp.tril(jnp.ones((all_rows, all_rows), BF))
    last_before = dot(ones_before, is_last.astype(BF)).astype(jnp.int32)
    position = jnp.arange(all_rows, dtype=jnp.int32)[:, None]
    first_count = all_rows - last_before[all_rows - 1, 0]
    place = jnp.where(is_last, first_count + last_before - 1, position - last_before)
    sort_to = (place == jnp.arange(all_rows, dtype=jnp.int32)[None, :]).astype(BF)
    tail = all_rows - CAP
    in_first = position < first_count

    centre_rows = jnp.where(is_last, centres[1:2], centres[0:1])
    gate = jax.nn.sigmoid(jnp.sum(second_wide * centre_rows, axis=-1, keepdims=True))
    back_branch = (gate * back_all).astype(BF)
    gate, back_branch, sent_rows = lax.optimization_barrier((gate, back_branch, second_rows))
    picked = dot_tn(sort_to, sent_rows).astype(BF)
    back_slots = dot_tn(sort_to, back_branch).astype(BF)
    windows = (slice(0, CAP), slice(tail, all_rows))
    masks = (in_first[:CAP], ~in_first[tail:])
    slot_out, back_picked, grads_in, grads_out = [], [], [], []
    hidden_of = []
    for e in range(2):
        columns = slice(e * hidden, (e + 1) * hidden)
        rows_in = picked[windows[e]]
        back_rows = jnp.where(masks[e], back_slots[windows[e]], jnp.zeros((), BF))
        up = dot(rows_in, in_w[:, columns])
        activated = lax.optimization_barrier(jax.nn.gelu(up).astype(BF))
        grads_out.append(dot_tn(back_rows, activated).astype(BF))
        hidden_of.append((columns, rows_in, back_rows, up, activated))
    grads_out = jnp.concatenate(grads_out, axis=1)
    out_via = ring.far(grads_out, BF)
    for e, (columns, rows_in, back_rows, up, activated) in enumerate(hidden_of):
        if e == 1:
            back_rows = after(back_rows, out_via)
        slot_out.append(dot_nt(activated, back_ws[e]).astype(BF))
        back_activated = dot(back_rows, back_ws[e])
        back_up = jax.vjp(jax.nn.gelu, up)[1](back_activated)[0].astype(BF)
        grads_in.append(dot_tn(rows_in, back_up).astype(BF))
        back_picked.append(dot_nt(back_up, in_w[:, columns]).astype(BF))
    grads_in = jnp.concatenate(grads_in, axis=1)
    out_near = ring.near(grads_out, out_via, BF)
    in_via = ring.far(after(grads_in, out_via), BF)

    def unsort(pieces):
        joined = jnp.concatenate(
            [
                pieces[0][:tail],
                jnp.where(in_first[tail:CAP], pieces[0][tail:], pieces[1][: CAP - tail]),
                pieces[1][CAP - tail :],
            ],
            axis=0,
        )
        return dot(sort_to, joined).astype(BF)

    row_terms = unsort(slot_out)
    expert_rows = row_terms.astype(F32) + swap(row_terms).astype(F32)
    block_all = (residual + gate * expert_rows).astype(BF)
    first_own = side * own_rows
    block_out = dot_nt(lax.dynamic_slice_in_dim(block_all, first_own, own_rows), to_order).astype(BF)
    back_score = jnp.sum(back_all * expert_rows, axis=-1, keepdims=True) * gate * (1.0 - gate)

    second_terms = unsort(back_picked)
    back_second = second_terms.astype(F32) + swap(second_terms).astype(F32) + back_score * centre_rows
    weighted = back_score * second_wide
    grad_centre = jnp.stack(
        [
            jnp.sum(jnp.where(is_last, 0.0, weighted), axis=0),
            jnp.sum(jnp.where(is_last, weighted, 0.0), axis=0),
        ]
    )
    grad_gain_two = jnp.sum(back_second * normed_two, axis=0)
    grad_bias_two = jnp.sum(back_second, axis=0)
    back_residual = back_all + norm_back(back_second, normed_two, scale_two, gain_two)
    back_out = back_residual.astype(BF)
    grads_out = ring.last(grads_out, out_near, BF)
    in_near = ring.near(grads_in, in_via, BF)
    back_attended = dot(back_out, out_w).astype(BF)
    grad_out = dot_tn(back_out, attended).astype(BF)
    back_qkv = attend_back(qkv, prefix, back_attended, lse, head_dim)
    back_qkv = after(back_qkv, (in_near, grads_out))
    grads_in = ring.last(grads_in, in_near, BF)
    grad_qkv = jnp.concatenate([dot_tn(first_rows, back_qkv[i]).astype(BF) for i in range(3)], axis=1)
    first_terms = sum(dot_nt(back_qkv[i], qkv_w[:, i * part : (i + 1) * part]) for i in range(3))
    first_terms = first_terms.astype(BF)
    own_terms = lax.dynamic_slice_in_dim(first_terms, first_own, own_rows)
    other_terms = lax.dynamic_slice_in_dim(first_terms, own_rows - first_own, own_rows)
    back_first = own_terms.astype(F32) + swap(other_terms).astype(F32)

    def mine(value):
        return lax.dynamic_slice_in_dim(value, first_own, own_rows)

    normed_own = mine(normed_one)
    back_norm_one = norm_back(back_first, normed_own, mine(scale_one), gain_one)
    grad_tokens = dot_nt(
        (mine(back_residual) + back_norm_one).astype(BF), to_order
    ).astype(BF)
    one_part = jnp.stack([jnp.sum(back_first * normed_own, axis=0), jnp.sum(back_first, axis=0)])
    one_part = one_part + swap(one_part)
    small = jnp.concatenate(
        [one_part, grad_gain_two[None], grad_bias_two[None], grad_centre], axis=0
    )
    small = small.reshape(small_count, count, rows).transpose(1, 0, 2)
    grad_first = jnp.concatenate([grad_qkv, grad_out], axis=1)
    if count == 16:
        small = jnp.pad(small, ((0, 0), (0, 8 - small_count), (0, 128 - rows)))
        small, grad_first = scatter_last(small, grad_first.reshape(count, rows, 4 * part))
        small = small[:small_count, :rows]
    else:
        grad_first = ring.scatter(grad_first, BF)
        small = ring.scatter(small.reshape(count, small_count * rows), F32).reshape(small_count, rows)
    grad_qkv, grad_out = grad_first[:, : 3 * part], grad_first[:, 3 * part :]
    small = lax.dynamic_slice_in_dim(small, side * (rows // 2), rows // 2, axis=1)
    return (
        block_out,
        grad_tokens,
        small[0],
        small[1],
        grad_qkv[:, :part],
        grad_qkv[:, part : 2 * part],
        grad_qkv[:, 2 * part :],
        grad_out.T,
        small[2],
        small[3],
        small[4:],
        grads_in.reshape(rows, experts, hidden).transpose(1, 0, 2),
        grads_out.reshape(rows, experts, hidden).transpose(1, 2, 0),
    )


def solution(mesh):
    ring = Ring(mesh.shape["dp"])
    both, rows = P(("dp", "tensor")), P(("dp", "tensor"), None)
    columns = P("dp", "tensor")

    def step(*arguments):
        return body(ring, *arguments)

    return jax.shard_map(
        step,
        mesh=mesh,
        in_specs=(
            rows,
            rows,
            P("dp"),
            P("dp", None),
            both,
            both,
            columns,
            columns,
            columns,
            P("tensor", "dp"),
            both,
            both,
            P(None, ("dp", "tensor")),
            P(None, "dp", "tensor"),
            P(None, "tensor", "dp"),
        ),
        out_specs=(
            rows,
            rows,
            both,
            both,
            columns,
            columns,
            columns,
            P("tensor", "dp"),
            both,
            both,
            P(None, ("dp", "tensor")),
            P(None, "dp", "tensor"),
            P(None, "tensor", "dp"),
        ),
        check_vma=False,
    )
```
